8 devices in a mesh: row: 4 (over z, y, x), col: 2 (over core).
Axes of the slice: x: 2, y: 2, z: 1, core: 2. Of those that a mesh axis runs over, the one named last changes fastest.
Arguments:
- v_panels: float32 [4096, 4096], P('row', 'col')
- t_factors: float32 [64, 64, 64], P('col')
- z_vecs: float32 [4096, 4096], P(None, ('row', 'col'))
Outputs:
- output: float32 [4096, 4096], P(None, ('row', 'col'))
All inputs are finite; a program needn't handle non-finite values.
Results may differ from the reference program's by a relative error of at most 0.001.
Values sent between devices are 32-bit elements.
A program may use at most 1 GiB of HBM per device.

```python
import jax
import jax.numpy as jnp
from jax import lax

N = 4096
BLOCK = 64
K_DEV = 512
ROW_DEV = 4
COL_DEV = 2

NPANEL = N // BLOCK
M_LOC = NPANEL // COL_DEV
K_COLS = K_DEV * ROW_DEV * COL_DEV


def build_inputs(raw_vals, z_vecs):
    row_nat = jnp.arange(N)[:, None, None]
    diag_row = (jnp.arange(NPANEL) * BLOCK)[None, :, None] + jnp.arange(BLOCK)[None, None, :]
    v_nat = jnp.where(row_nat > diag_row, raw_vals, jnp.where(row_nat == diag_row, 1.0, 0.0)).astype(raw_vals.dtype)
    gram = jnp.einsum("nmb,nmc->mbc", v_nat, v_nat, precision=lax.Precision.HIGHEST)
    half_diag = 0.5 * jnp.diagonal(gram, axis1=1, axis2=2)
    t_inverse = jnp.triu(gram, 1) + jnp.eye(BLOCK, dtype=raw_vals.dtype) * half_diag[:, None, :]
    t_nat = jnp.triu(jnp.linalg.inv(t_inverse))
    v_cols = v_nat.reshape(N, M_LOC, COL_DEV, BLOCK).transpose(0, 2, 1, 3).reshape(N, N)
    v_store = v_cols.reshape(NPANEL // ROW_DEV, ROW_DEV, BLOCK, N).transpose(1, 0, 2, 3).reshape(N, N)
    t_store = t_nat.reshape(M_LOC, COL_DEV, BLOCK, BLOCK).transpose(1, 0, 2, 3).reshape(NPANEL, BLOCK, BLOCK)
    return {"v_panels": v_store, "t_factors": t_store, "z_vecs": z_vecs}


def setup_inputs(seed: int = 0) -> dict:
    base_key = jax.random.key(seed)
    key_v, key_z = jax.random.split(base_key)
    raw_vals = jax.random.normal(key_v, (N, NPANEL, BLOCK), jnp.float32)
    z_vecs = jax.random.normal(key_z, (N, K_COLS), jnp.float32)
    return build_inputs(raw_vals, z_vecs)


def reference(v_panels, t_factors, z_vecs):
    def apply_panel(x_cur, panel_idx):
        store_slot = (panel_idx % COL_DEV) * M_LOC + panel_idx // COL_DEV
        v_blk = lax.dynamic_slice_in_dim(v_panels, store_slot * BLOCK, BLOCK, axis=1)
        t_blk = lax.dynamic_index_in_dim(t_factors, store_slot, axis=0, keepdims=False)
        w_blk = jnp.dot(v_blk.T, x_cur, precision=lax.Precision.HIGHEST, preferred_element_type=jnp.float32)
        y_blk = jnp.dot(t_blk, w_blk, precision=lax.Precision.HIGHEST, preferred_element_type=jnp.float32)
        x_new = x_cur - jnp.dot(v_blk, y_blk, precision=lax.Precision.HIGHEST, preferred_element_type=jnp.float32)
        return x_new, None

    x_out, _ = lax.scan(apply_panel, z_vecs, jnp.arange(NPANEL - 1, -1, -1))
    return x_out
```

```python
import functools

import jax
import jax.numpy as jnp
from jax import lax
from jax.experimental import pallas as pl
from jax.experimental.pallas import tpu as pltpu
from jax.sharding import PartitionSpec as P

MESH = pl.DeviceIdType.MESH
F32 = jnp.float32
BF16 = jnp.bfloat16

NU = 16
NCH = NU * (NU + 1) // 2
L0, L1, L2 = 12, 7, 3
EXTRA = 24


def split3(x):
    h = x.astype(BF16)
    rem = x - h.astype(F32)
    m = rem.astype(BF16)
    l = (rem - m.astype(F32)).astype(BF16)
    return h, m, l


def dot(a, b):
    return jnp.dot(a, b, preferred_element_type=F32)


def mm6(a, b):
    ah, am, al = a
    bh, bm, bl = b
    return (dot(al, bh) + dot(ah, bl) + dot(am, bm)) + (dot(am, bh) + dot(ah, bm)) + dot(ah, bh)


def mm_f32(a, b):
    return mm6(split3(a), split3(b))


def kernel(
    v_hbm, d_hbm, z_hbm, out_hbm,
    vbuf, xbuf, dbuf, vt3, vn3, x3, y3, wacc, s1acc, s2acc, tmat,
    r1_sem, r2_sem, rd_sem, rp_sem, loc_sem, send_sem, z_sem, d_sem, o_sem,
):
    r = lax.axis_index("row")
    q = lax.axis_index("col")
    ry, rx = r // 2, r % 2
    row_x = ry * 2 + (1 - rx)
    row_y = (1 - ry) * 2 + rx
    n1 = row_x * (1 - q) + row_y * q
    n2 = row_y * (1 - q) + row_x * q
    nd = 3 - r
    dev1, dev2, devp = (n1, q), (n2, q), (r, 1 - q)
    cols = pl.ds(pl.multiple_of(q * 128, 128), 128)

    def piece(c, rr):
        return vbuf.at[c, pl.ds(pl.multiple_of(rr * 64, 64), 64), cols]

    def remote(src, dst, k, rsem, dev):
        return pltpu.make_async_remote_copy(
            src_ref=src, dst_ref=dst, send_sem=send_sem.at[k], recv_sem=rsem,
            device_id=dev, device_id_type=MESH,
        )

    def own_src(s, u):
        return v_hbm.at[u, :, pl.ds(pl.multiple_of(s * 128, 128), 128)]

    def stage0(c, s, u):
        src = own_src(s, u)
        remote(src, piece(c, r), 0, r1_sem.at[c], dev1).start()
        remote(src, piece(c, r), 1, r2_sem.at[c], dev2).start()
        pltpu.make_async_copy(src, piece(c, r), loc_sem.at[c]).start()

    def stage1(c):
        p = piece(c, n1)
        remote(p, p, 0, r1_sem.at[c], dev1).wait_recv()
        remote(p, p, 2, rd_sem.at[c], dev2).start()

    def stage2(c):
        p = piece(c, n2)
        remote(p, p, 1, r2_sem.at[c], dev2).wait_recv()
        p = piece(c, nd)
        remote(p, p, 2, rd_sem.at[c], dev2).wait_recv()
        p = piece(c, r)
        pltpu.make_async_copy(p, p, loc_sem.at[c]).wait()
        p = vbuf.at[c, :, cols]
        remote(p, p, 3, rp_sem.at[c], devp).start()

    def stage3(c):
        p = vbuf.at[c, :, pl.ds(pl.multiple_of((1 - q) * 128, 128), 128)]
        remote(p, p, 3, rp_sem.at[c], devp).wait_recv()

    def comm_tick(n, su):
        s, u = su

        @pl.when(n + L0 < NCH)
        def _():
            stage0(n + L0, s, u)

        @pl.when(jnp.logical_and(n + L1 >= 0, n + L1 < NCH))
        def _():
            stage1(n + L1)

        @pl.when(jnp.logical_and(n + L2 >= 0, n + L2 < NCH))
        def _():
            stage2(n + L2)

        last = u == NU - 1
        s2 = jnp.where(last, jnp.maximum(s - 1, 0), s)
        u2 = jnp.where(last, s2, u + 1)
        return s2, u2

    def tick(c, carry):
        n, s, u = carry
        count = jnp.where(c < EXTRA, 2, 1)
        s, u = lax.fori_loop(0, count, lambda i, su: comm_tick(n + i, su), (s, u))
        stage3(c)
        return n + count, s, u

    barrier = pltpu.get_barrier_semaphore()
    for dev in (dev1, dev2, devp):
        pl.semaphore_signal(barrier, inc=1, device_id=dev, device_id_type=MESH)
    pl.semaphore_wait(barrier, 3)

    d_own = dbuf.at[q]
    d_send = pltpu.make_async_remote_copy(
        src_ref=d_hbm, dst_ref=d_own, send_sem=d_sem.at[0], recv_sem=d_sem.at[1],
        device_id=devp, device_id_type=MESH,
    )
    d_send.start()
    d_loc = pltpu.make_async_copy(d_hbm, d_own, d_sem.at[2])
    d_loc.start()

    def z_copy(u):
        return pltpu.make_async_copy(z_hbm.at[:, u], xbuf.at[u], z_sem.at[u])

    s0, u0 = lax.fori_loop(-L0, 0, comm_tick, (jnp.int32(NU - 1), jnp.int32(NU - 1)))
    lax.fori_loop(0, NU, lambda i, _: (z_copy(NU - 1 - i).start(), 0)[1], 0)
    d_send.wait()
    d_loc.wait()

    def do_a(c, u):
        v = vbuf[c]
        th, tm, tl = split3(v.T)
        vt3[0], vt3[1], vt3[2] = th, tm, tl
        nh, nm, nl = split3(v)
        vn3[0], vn3[1], vn3[2] = nh, nm, nl
        xh, xm, xl = split3(xbuf[u].reshape(256, 512))
        x3[0], x3[1], x3[2] = xh, xm, xl
        wacc[...] += mm6((vt3[0], vt3[1], vt3[2]), (x3[0], x3[1], x3[2]))
        s1acc[...] += dot(vt3[1], vn3[1]) + dot(vt3[0], vn3[0])
        s2acc[...] += dot(vt3[0], vn3[2]) + dot(vt3[0], vn3[1])

    def do_c(c, u):
        upd = mm6(split3(vbuf[c]), (y3[0], y3[1], y3[2]))
        xbuf[u] = xbuf[u] - upd.reshape(4, 64, 512)

    lane = lax.broadcasted_iota(jnp.int32, (64, 128), 1)
    low = lane < 64

    def roll(x):
        return pltpu.roll(x, 64, 1)

    def merge_t(s):
        s2 = s2acc[...]
        g = s1acc[...] + s2 + s2.T
        da, db = dbuf[0, s], dbuf[1, s]
        gab = g[:128, 128:]
        u1 = jnp.concatenate([jnp.where(low, gab[:64], 0.0), jnp.where(low, 0.0, gab[64:])], axis=0)
        e = -mm_f32(da, mm_f32(u1, db))
        t01 = jnp.concatenate([da[:64] + roll(e[:64]), roll(db[:64])], axis=0)
        t23 = jnp.concatenate([roll(da[64:]) + e[64:], db[64:]], axis=0)
        u2 = jnp.concatenate(
            [
                jnp.where(low, roll(g[:64, :128]), g[:64, 128:]),
                jnp.where(low, roll(g[128:192, :128]), g[128:192, 128:]),
            ],
            axis=0,
        )
        f = -mm_f32(t01, mm_f32(u2, t23))
        zero = jnp.zeros((64, 128), F32)
        tmat[0:64, 0:128] = da[:64] + jnp.where(low, 0.0, roll(f[:64]))
        tmat[0:64, 128:256] = e[:64] + jnp.where(low, 0.0, f[:64])
        tmat[64:128, 0:128] = da[64:]
        tmat[64:128, 128:256] = e[64:]
        tmat[128:192, 0:128] = jnp.where(low, 0.0, roll(f[64:]))
        tmat[128:192, 128:256] = db[:64] + jnp.where(low, 0.0, f[64:])
        tmat[192:256, 0:128] = zero
        tmat[192:256, 128:256] = db[64:]

    def offset(s):
        return (NU - 1 - s) * (NU - s) // 2

    def outer(k, carry):
        s = NU - k
        sa = s - 1
        z_copy(sa).wait()
        wacc[...] = jnp.zeros_like(wacc)
        s1acc[...] = jnp.zeros_like(s1acc)
        s2acc[...] = jnp.zeros_like(s2acc)
        off_a = offset(sa)
        off_c = off_a - k

        def inner(u, carry):
            i = u - s
            carry = tick(off_a + i, carry)
            do_a(off_a + i, u - 1)
            do_c(off_c + i, u)
            return carry

        carry = lax.fori_loop(s, NU, inner, carry)
        carry = tick(off_a + k, carry)
        do_a(off_a + k, NU - 1)
        merge_t(sa)
        yh, ym, yl = split3(mm_f32(tmat[...], wacc[...]))
        y3[0], y3[1], y3[2] = yh, ym, yl
        return carry

    lax.fori_loop(0, NU, outer, (jnp.int32(0), s0, u0))

    def o_copy(u):
        return pltpu.make_async_copy(xbuf.at[u], out_hbm.at[:, u], o_sem.at[u])

    def final(u, _):
        do_c(NCH - NU + u, u)
        o_copy(u).start()
        return 0

    lax.fori_loop(0, NU, final, 0)
    lax.fori_loop(0, NU, lambda u, _: (o_copy(u).wait(), 0)[1], 0)
    sent = vbuf.at[:, pl.ds(0, 64), pl.ds(0, 128)]
    for k in range(3):
        remote(sent, sent, k, rp_sem.at[0], dev1).wait_send()
    sent = vbuf.at[:, :, pl.ds(0, 128)]
    remote(sent, sent, 3, rp_sem.at[0], devp).wait_send()


def solution(mesh):
    def local_apply(v_loc, t_loc, z_loc):
        t4 = t_loc.reshape(NU, 2, 64, 64)
        zero = jnp.zeros((NU, 64, 64), F32)
        d_loc = jnp.concatenate(
            [jnp.concatenate([t4[:, 0], zero], axis=2), jnp.concatenate([zero, t4[:, 1]], axis=2)], axis=1
        )
        dma = pltpu.SemaphoreType.DMA
        out = pl.pallas_call(
            kernel,
            out_shape=jax.ShapeDtypeStruct((4, NU, 64, 512), F32),
            in_specs=[pl.BlockSpec(memory_space=pl.ANY)] * 3,
            out_specs=pl.BlockSpec(memory_space=pl.ANY),
            scratch_shapes=[
                pltpu.VMEM((NCH, 256, 256), F32),
                pltpu.VMEM((NU, 4, 64, 512), F32),
                pltpu.VMEM((2, NU, 128, 128), F32),
                pltpu.VMEM((3, 256, 256), BF16),
                pltpu.VMEM((3, 256, 256), BF16),
                pltpu.VMEM((3, 256, 512), BF16),
                pltpu.VMEM((3, 256, 512), BF16),
                pltpu.VMEM((256, 512), F32),
                pltpu.VMEM((256, 256), F32),
                pltpu.VMEM((256, 256), F32),
                pltpu.VMEM((256, 256), F32),
                dma((NCH,)), dma((NCH,)), dma((NCH,)), dma((NCH,)), dma((NCH,)),
                dma((4,)), dma((NU,)), dma((3,)), dma((NU,)),
            ],
            compiler_params=pltpu.CompilerParams(
                collective_id=0, has_side_effects=True, vmem_limit_bytes=67_043_328
            ),
            cost_estimate=pl.CostEstimate(flops=116_000_000_000, bytes_accessed=60_000_000, transcendentals=0),
        )(v_loc.reshape(NU, 64, 2048), d_loc, z_loc.reshape(4, NU, 64, 512))
        return out.reshape(4096, 512)

    return jax.shard_map(
        local_apply,
        mesh=mesh,
        in_specs=(P("row", "col"), P("col", None, None), P(None, ("row", "col"))),
        out_specs=P(None, ("row", "col")),
        check_vma=False,
    )
```

```python
import functools

import jax
import jax.numpy as jnp
from jax import lax
from jax.experimental import pallas as pl
from jax.experimental.pallas import tpu as pltpu
from jax.sharding import PartitionSpec as P

MESH = pl.DeviceIdType.MESH
F32 = jnp.float32
BF16 = jnp.bfloat16

NU = 16
NCH = NU * (NU + 1) // 2
L0, L1, L2 = 12, 7, 3
EXTRA = 24


def split3(x):
    h = x.astype(BF16)
    rem = x - h.astype(F32)
    m = rem.astype(BF16)
    l = (rem - m.astype(F32)).astype(BF16)
    return h, m, l


def dot(a, b):
    return jnp.dot(a, b, preferred_element_type=F32)


def mm6(a, b):
    ah, am, al = a
    bh, bm, bl = b
    return (dot(al, bh) + dot(ah, bl) + dot(am, bm)) + (dot(am, bh) + dot(ah, bm)) + dot(ah, bh)


def mm_f32(a, b):
    return mm6(split3(a), split3(b))


def mm_k128(a, b):
    ah, am, al = split3(a)
    bh, bm, bl = split3(b)

    def part(a0, a1, b0, b1):
        return dot(jnp.concatenate([a0, a1], axis=1), jnp.concatenate([b0, b1], axis=0))

    return (part(am, ah, bm, bl) + part(al, ah, bh, bm)) + part(am, ah, bh, bh)


def kernel(
    v_hbm, d_hbm, z_hbm, out_hbm,
    vbuf, xbuf, dbuf, vt3, vn3, x3, y3, wacc, s1acc, s2acc, tmat,
    r1_sem, r2_sem, rd_sem, rp_sem, loc_sem, send_sem, z_sem, d_sem, o_sem,
):
    r = lax.axis_index("row")
    q = lax.axis_index("col")
    ry, rx = r // 2, r % 2
    row_x = ry * 2 + (1 - rx)
    row_y = (1 - ry) * 2 + rx
    n1 = row_x * (1 - q) + row_y * q
    n2 = row_y * (1 - q) + row_x * q
    nd = 3 - r
    dev1, dev2, devp = (n1, q), (n2, q), (r, 1 - q)
    cols = pl.ds(pl.multiple_of(q * 128, 128), 128)

    def piece(c, rr):
        return vbuf.at[c, pl.ds(pl.multiple_of(rr * 64, 64), 64), cols]

    def remote(src, dst, k, rsem, dev):
        return pltpu.make_async_remote_copy(
            src_ref=src, dst_ref=dst, send_sem=send_sem.at[k], recv_sem=rsem,
            device_id=dev, device_id_type=MESH,
        )

    def own_src(s, u):
        return v_hbm.at[u, :, pl.ds(pl.multiple_of(s * 128, 128), 128)]

    def stage0(c, s, u):
        src = own_src(s, u)
        remote(src, piece(c, r), 0, r1_sem.at[c], dev1).start()
        remote(src, piece(c, r), 1, r2_sem.at[c], dev2).start()
        pltpu.make_async_copy(src, piece(c, r), loc_sem.at[c]).start()

    def stage1(c):
        p = piece(c, n1)
        remote(p, p, 0, r1_sem.at[c], dev1).wait_recv()
        remote(p, p, 2, rd_sem.at[c], dev2).start()

    def stage2(c):
        p = piece(c, n2)
        remote(p, p, 1, r2_sem.at[c], dev2).wait_recv()
        p = piece(c, nd)
        remote(p, p, 2, rd_sem.at[c], dev2).wait_recv()
        p = piece(c, r)
        pltpu.make_async_copy(p, p, loc_sem.at[c]).wait()
        p = vbuf.at[c, :, cols]
        remote(p, p, 3, rp_sem.at[c], devp).start()

    def stage3(c):
        p = vbuf.at[c, :, pl.ds(pl.multiple_of((1 - q) * 128, 128), 128)]
        remote(p, p, 3, rp_sem.at[c], devp).wait_recv()

    def comm_tick(n, su):
        s, u = su

        @pl.when(n + L0 < NCH)
        def _():
            stage0(n + L0, s, u)

        @pl.when(jnp.logical_and(n + L1 >= 0, n + L1 < NCH))
        def _():
            stage1(n + L1)

        @pl.when(jnp.logical_and(n + L2 >= 0, n + L2 < NCH))
        def _():
            stage2(n + L2)

        last = u == NU - 1
        s2 = jnp.where(last, jnp.maximum(s - 1, 0), s)
        u2 = jnp.where(last, s2, u + 1)
        return s2, u2

    def tick(c, carry):
        n, s, u = carry
        count = jnp.where(c < EXTRA, 2, 1)
        s, u = lax.fori_loop(0, count, lambda i, su: comm_tick(n + i, su), (s, u))

        @pl.when(c < NCH)
        def _():
            stage3(c)

        return n + count, s, u

    barrier = pltpu.get_barrier_semaphore()
    for dev in (dev1, dev2, devp):
        pl.semaphore_signal(barrier, inc=1, device_id=dev, device_id_type=MESH)
    pl.semaphore_wait(barrier, 3)

    d_own = dbuf.at[:, :, pl.ds(pl.multiple_of(q * 64, 64), 64), :]
    d_send = pltpu.make_async_remote_copy(
        src_ref=d_hbm, dst_ref=d_own, send_sem=d_sem.at[0], recv_sem=d_sem.at[1],
        device_id=devp, device_id_type=MESH,
    )
    d_send.start()
    d_loc = pltpu.make_async_copy(d_hbm, d_own, d_sem.at[2])
    d_loc.start()

    def z_copy(u):
        return pltpu.make_async_copy(z_hbm.at[:, u], xbuf.at[u], z_sem.at[u])

    s0, u0 = lax.fori_loop(-L0, 0, comm_tick, (jnp.int32(NU - 1), jnp.int32(NU - 1)))
    lax.fori_loop(0, NU, lambda i, _: (z_copy(NU - 1 - i).start(), 0)[1], 0)
    d_send.wait()
    d_loc.wait()

    def store3(ref, x):
        ref[0], ref[1], ref[2] = split3(x)

    def load3(ref):
        return ref[0], ref[1], ref[2]

    def do_a():
        wacc[...] += mm6(load3(vt3), load3(x3))

    def do_c(c, u):
        x = xbuf[u].reshape(256, 512) - mm6(split3(vbuf[c]), load3(y3))
        xbuf[u] = x.reshape(4, 64, 512)
        return x

    def do_g(c):
        v = vbuf[c]
        store3(vn3, v)
        store3(vt3, v.T)
        g1 = dot(vt3[1], vn3[1]) + dot(vt3[0], vn3[0])
        g2 = dot(vt3[0], vn3[2]) + dot(vt3[0], vn3[1])
        return g1, g2

    low = lax.broadcasted_iota(jnp.int32, (64, 128), 1) < 64

    def roll(x):
        return pltpu.roll(x, 64, 1)

    def merge_t(s):
        s2 = s2acc[...]
        g = s1acc[...] + s2 + s2.T
        zero = jnp.zeros((64, 128), F32)
        d01, d23 = dbuf[s, 0], dbuf[s, 1]
        u01 = jnp.concatenate([jnp.where(low, 0.0, roll(g[:64, 128:])), zero], axis=0)
        u23 = jnp.concatenate([jnp.where(low, 0.0, g[64:128, 128:]), zero], axis=0)
        u2 = jnp.concatenate(
            [
                jnp.where(low, roll(g[:64, :128]), g[:64, 128:]),
                jnp.where(low, roll(g[128:192, :128]), g[128:192, 128:]),
            ],
            axis=0,
        )
        nm = mm_k128(d01, jnp.concatenate([u01, u2], axis=1))
        z = mm_k128(u23, d23)
        el = mm_k128(nm[:, :128], jnp.concatenate([d01, nm[:, 128:]], axis=1))
        t01 = d01 - el[:, :128]
        t23 = d23 - mm_k128(d23, z)
        f = -mm_k128(nm[:, 128:] - el[:, 128:], t23)
        tmat[0:64, 0:128] = jnp.where(low, t01[:64], roll(f[:64]))
        tmat[0:64, 128:256] = jnp.where(low, roll(t01[:64]), f[:64])
        tmat[64:128, 0:128] = jnp.where(low, 0.0, roll(t23[:64]))
        tmat[64:128, 128:256] = jnp.where(low, 0.0, t23[:64])
        tmat[128:192, 0:128] = jnp.where(low, 0.0, roll(f[64:]))
        tmat[128:192, 128:256] = jnp.where(low, roll(t01[64:]), f[64:])
        tmat[192:256, 0:128] = zero
        tmat[192:256, 128:256] = t23[64:]

    def offset(s):
        return (NU - 1 - s) * (NU - s) // 2

    carry = tick(0, (jnp.int32(0), s0, u0))
    z_copy(NU - 1).wait()
    wacc[...] = jnp.zeros_like(wacc)
    s1acc[...], s2acc[...] = do_g(0)
    store3(x3, xbuf[NU - 1].reshape(256, 512))

    def outer(k, carry):
        s = NU - k
        sa = s - 1
        off_a = offset(sa)
        off_c = off_a - k

        def step(u):
            i = u - s
            do_a()
            x = do_c(off_c + i, u)
            g1, g2 = do_g(off_a + i + 1)
            s1acc[...] += g1
            s2acc[...] += g2
            store3(x3, x)

        def step1(u, carry):
            carry = tick(off_a + u - s + 1, carry)
            step(u)
            return carry

        def step2(j, carry):
            u = s + 2 * j
            carry = tick(off_a + u - s + 1, carry)
            carry = tick(off_a + u - s + 2, carry)
            step(u)
            step(u + 1)
            return carry

        carry = lax.fori_loop(0, k // 2, step2, carry)
        carry = lax.fori_loop(NU - k % 2, NU, step1, carry)
        more = k < NU - 1
        carry = tick(off_a + k + 1, carry)

        @pl.when(more)
        def _():
            z_copy(jnp.maximum(sa - 1, 0)).wait()

        do_a()
        merge_t(sa)
        s1acc[...], s2acc[...] = do_g(jnp.minimum(off_a + k + 1, NCH - 1))
        store3(x3, xbuf[jnp.maximum(sa - 1, 0)].reshape(256, 512))
        store3(y3, mm_f32(tmat[...], wacc[...]))
        wacc[...] = jnp.zeros_like(wacc)
        return carry

    lax.fori_loop(0, NU, outer, carry)

    def o_copy(u):
        return pltpu.make_async_copy(xbuf.at[u], out_hbm.at[:, u], o_sem.at[u])

    def final(u, _):
        do_c(NCH - NU + u, u)
        o_copy(u).start()
        return 0

    lax.fori_loop(0, NU, final, 0)
    lax.fori_loop(0, NU, lambda u, _: (o_copy(u).wait(), 0)[1], 0)
    sent = vbuf.at[:, pl.ds(0, 64), pl.ds(0, 128)]
    for k in range(3):
        remote(sent, sent, k, rp_sem.at[0], dev1).wait_send()
    sent = vbuf.at[:, :, pl.ds(0, 128)]
    remote(sent, sent, 3, rp_sem.at[0], devp).wait_send()


def solution(mesh):
    def local_apply(v_loc, t_loc, z_loc):
        t4 = t_loc.reshape(NU, 2, 64, 64)
        zero = jnp.zeros_like(t4)
        first = lax.axis_index("col") == 0
        d_loc = jnp.concatenate([jnp.where(first, t4, zero), jnp.where(first, zero, t4)], axis=3)
        dma = pltpu.SemaphoreType.DMA
        out = pl.pallas_call(
            kernel,
            out_shape=jax.ShapeDtypeStruct((4, NU, 64, 512), F32),
            in_specs=[pl.BlockSpec(memory_space=pl.ANY)] * 3,
            out_specs=pl.BlockSpec(memory_space=pl.ANY),
            scratch_shapes=[
                pltpu.VMEM((NCH, 256, 256), F32),
                pltpu.VMEM((NU, 4, 64, 512), F32),
                pltpu.VMEM((NU, 2, 128, 128), F32),
                pltpu.VMEM((3, 256, 256), BF16),
                pltpu.VMEM((3, 256, 256), BF16),
                pltpu.VMEM((3, 256, 512), BF16),
                pltpu.VMEM((3, 256, 512), BF16),
                pltpu.VMEM((256, 512), F32),
                pltpu.VMEM((256, 256), F32),
                pltpu.VMEM((256, 256), F32),
                pltpu.VMEM((256, 256), F32),
                dma((NCH,)), dma((NCH,)), dma((NCH,)), dma((NCH,)), dma((NCH,)),
                dma((4,)), dma((NU,)), dma((3,)), dma((NU,)),
            ],
            compiler_params=pltpu.CompilerParams(
                collective_id=0, has_side_effects=True, vmem_limit_bytes=67_043_328
            ),
            cost_estimate=pl.CostEstimate(flops=116_000_000_000, bytes_accessed=60_000_000, transcendentals=0),
        )(v_loc.reshape(NU, 64, 2048), d_loc, z_loc.reshape(4, NU, 64, 512))
        return out.reshape(4096, 512)

    return jax.shard_map(
        local_apply,
        mesh=mesh,
        in_specs=(P("row", "col"), P("col", None, None), P(None, ("row", "col"))),
        out_specs=P(None, ("row", "col")),
        check_vma=False,
    )
```

```python
import functools

import jax
import jax.numpy as jnp
from jax import lax
from jax.experimental import pallas as pl
from jax.experimental.pallas import tpu as pltpu
from jax.sharding import PartitionSpec as P

MESH = pl.DeviceIdType.MESH
F32 = jnp.float32
BF16 = jnp.bfloat16

NU = 16
NCH = NU * (NU + 1) // 2
LEAD0, LEAD1, LEAD2 = 9, 3, 1
ZAHEAD = 4


def split3(x):
    h = x.astype(BF16)
    rem = x - h.astype(F32)
    m = rem.astype(BF16)
    l = (rem - m.astype(F32)).astype(BF16)
    return h, m, l


def dot(a, b):
    return jnp.dot(a, b, preferred_element_type=F32)


def mm6(a, b):
    ah, am, al = a
    bh, bm, bl = b
    return (dot(al, bh) + dot(ah, bl) + dot(am, bm)) + (dot(am, bh) + dot(ah, bm)) + dot(ah, bh)


def mm_f32(a, b):
    return mm6(split3(a), split3(b))


def mm_k128(a, b):
    ah, am, al = split3(a)
    bh, bm, bl = split3(b)

    def part(a0, a1, b0, b1):
        return dot(jnp.concatenate([a0, a1], axis=1), jnp.concatenate([b0, b1], axis=0))

    return (part(am, ah, bm, bl) + part(al, ah, bh, bm)) + part(am, ah, bh, bh)


def kernel(
    v_hbm, d_hbm, z_hbm, out_hbm,
    vbuf, xbuf, dbuf, vt3, vn3, x3, y3, wacc, s1acc, s2acc, tmat,
    r1_sem, r2_sem, rd_sem, rp_sem, loc_sem, send_sem, z_sem, d_sem, o_sem,
):
    r = lax.axis_index("row")
    q = lax.axis_index("col")
    ry, rx = r // 2, r % 2
    row_x = ry * 2 + (1 - rx)
    row_y = (1 - ry) * 2 + rx
    n1 = row_x * (1 - q) + row_y * q
    n2 = row_y * (1 - q) + row_x * q
    nd = 3 - r
    dev1, dev2, devp = (n1, q), (n2, q), (r, 1 - q)
    cols = pl.ds(pl.multiple_of(q * 128, 128), 128)

    def piece(c, rr):
        return vbuf.at[c, pl.ds(pl.multiple_of(rr * 64, 64), 64), cols]

    def remote(src, dst, k, rsem, dev):
        return pltpu.make_async_remote_copy(
            src_ref=src, dst_ref=dst, send_sem=send_sem.at[k], recv_sem=rsem,
            device_id=dev, device_id_type=MESH,
        )

    def own_src(s, u):
        return v_hbm.at[u, :, pl.ds(pl.multiple_of(s * 128, 128), 128)]

    def stage0(c, s, u):
        src = own_src(s, u)
        remote(src, piece(c, r), 0, r1_sem.at[c], dev1).start()
        remote(src, piece(c, r), 1, r2_sem.at[c], dev2).start()
        pltpu.make_async_copy(src, piece(c, r), loc_sem.at[c]).start()

    def stage1(c):
        p = piece(c, n1)
        remote(p, p, 0, r1_sem.at[c], dev1).wait_recv()
        remote(p, p, 2, rd_sem.at[c], dev2).start()

    def stage2(c):
        p = piece(c, n2)
        remote(p, p, 1, r2_sem.at[c], dev2).wait_recv()
        p = piece(c, nd)
        remote(p, p, 2, rd_sem.at[c], dev2).wait_recv()
        p = piece(c, r)
        pltpu.make_async_copy(p, p, loc_sem.at[c]).wait()
        p = vbuf.at[c, :, cols]
        remote(p, p, 3, rp_sem.at[c], devp).start()

    def stage3(c):
        p = vbuf.at[c, :, pl.ds(pl.multiple_of((1 - q) * 128, 128), 128)]
        remote(p, p, 3, rp_sem.at[c], devp).wait_recv()

    def next0(carry):
        n0, s, u, n1, n2 = carry

        @pl.when(n0 < NCH)
        def _():
            stage0(n0, s, u)

        last = u == NU - 1
        s2 = jnp.where(last, jnp.maximum(s - 1, 0), s)
        u2 = jnp.where(last, s2, u + 1)
        return n0 + 1, s2, u2, n1, n2

    def next1(carry):
        n0, s, u, n1, n2 = carry

        @pl.when(n1 < NCH)
        def _():
            stage1(n1)

        return n0, s, u, n1 + 1, n2

    def next2(carry):
        n0, s, u, n1, n2 = carry

        @pl.when(n2 < NCH)
        def _():
            stage2(n2)

        return n0, s, u, n1, n2 + 1

    def repeat(count, fn, carry):
        return lax.fori_loop(0, count, lambda i, c: fn(c), carry)

    def advance(carry):
        return next2(next1(next0(carry)))

    def tick(c, carry):
        carry = advance(carry)

        @pl.when(c < NCH)
        def _():
            stage3(c)

        return carry

    barrier = pltpu.get_barrier_semaphore()
    for dev in (dev1, dev2, devp):
        pl.semaphore_signal(barrier, inc=1, device_id=dev, device_id_type=MESH)
    pl.semaphore_wait(barrier, 3)

    d_own = dbuf.at[:, :, pl.ds(pl.multiple_of(q * 64, 64), 64), :]
    d_send = pltpu.make_async_remote_copy(
        src_ref=d_hbm, dst_ref=d_own, send_sem=d_sem.at[0], recv_sem=d_sem.at[1],
        device_id=devp, device_id_type=MESH,
    )
    d_send.start()
    d_loc = pltpu.make_async_copy(d_hbm, d_own, d_sem.at[2])
    d_loc.start()

    def z_copy(u):
        return pltpu.make_async_copy(z_hbm.at[:, u], xbuf.at[u], z_sem.at[u])

    for i in range(ZAHEAD):
        z_copy(NU - 1 - i).start()
    zero = jnp.int32(0)
    carry = (zero, jnp.int32(NU - 1), jnp.int32(NU - 1), zero, zero)
    carry = repeat(LEAD0, next0, carry)
    carry = repeat(LEAD1, next1, carry)
    carry = repeat(LEAD2, next2, carry)
    d_send.wait()
    d_loc.wait()

    def store3(ref, x):
        ref[0], ref[1], ref[2] = split3(x)

    def load3(ref):
        return ref[0], ref[1], ref[2]

    def do_a():
        wacc[...] += mm6(load3(vt3), load3(x3))

    def do_c(c, u):
        x = xbuf[u].reshape(256, 512) - mm6(split3(vbuf[c]), load3(y3))
        xbuf[u] = x.reshape(4, 64, 512)
        return x

    def do_g(c):
        v = vbuf[c]
        store3(vn3, v)
        store3(vt3, v.T)
        g1 = dot(vt3[1], vn3[1]) + dot(vt3[0], vn3[0])
        g2 = dot(vt3[0], vn3[2]) + dot(vt3[0], vn3[1])
        return g1, g2

    low = lax.broadcasted_iota(jnp.int32, (64, 128), 1) < 64

    def roll(x):
        return pltpu.roll(x, 64, 1)

    def merge_t(s):
        s2 = s2acc[...]
        g = s1acc[...] + s2 + s2.T
        zero = jnp.zeros((64, 128), F32)
        d01, d23 = dbuf[s, 0], dbuf[s, 1]
        u01 = jnp.concatenate([jnp.where(low, 0.0, roll(g[:64, 128:])), zero], axis=0)
        u23 = jnp.concatenate([jnp.where(low, 0.0, g[64:128, 128:]), zero], axis=0)
        u2 = jnp.concatenate(
            [
                jnp.where(low, roll(g[:64, :128]), g[:64, 128:]),
                jnp.where(low, roll(g[128:192, :128]), g[128:192, 128:]),
            ],
            axis=0,
        )
        nm = mm_k128(d01, jnp.concatenate([u01, u2], axis=1))
        z = mm_k128(u23, d23)
        el = mm_k128(nm[:, :128], jnp.concatenate([d01, nm[:, 128:]], axis=1))
        t01 = d01 - el[:, :128]
        t23 = d23 - mm_k128(d23, z)
        f = -mm_k128(nm[:, 128:] - el[:, 128:], t23)
        tmat[0:64, 0:128] = jnp.where(low, t01[:64], roll(f[:64]))
        tmat[0:64, 128:256] = jnp.where(low, roll(t01[:64]), f[:64])
        tmat[64:128, 0:128] = jnp.where(low, 0.0, roll(t23[:64]))
        tmat[64:128, 128:256] = jnp.where(low, 0.0, t23[:64])
        tmat[128:192, 0:128] = jnp.where(low, 0.0, roll(f[64:]))
        tmat[128:192, 128:256] = jnp.where(low, roll(t01[64:]), f[64:])
        tmat[192:256, 0:128] = zero
        tmat[192:256, 128:256] = t23[64:]

    def offset(s):
        return (NU - 1 - s) * (NU - s) // 2

    carry = tick(0, carry)
    z_copy(NU - 1).wait()
    wacc[...] = jnp.zeros_like(wacc)
    s1acc[...], s2acc[...] = do_g(0)
    store3(x3, xbuf[NU - 1].reshape(256, 512))

    def outer(k, carry):
        s = NU - k
        sa = s - 1
        off_a = offset(sa)
        off_c = off_a - k

        def step(u):
            i = u - s
            do_a()
            x = do_c(off_c + i, u)
            g1, g2 = do_g(off_a + i + 1)
            s1acc[...] += g1
            s2acc[...] += g2
            store3(x3, x)

        def step1(u, carry):
            carry = tick(off_a + u - s + 1, carry)
            step(u)
            return carry

        def step2(j, carry):
            u = s + 2 * j
            carry = tick(off_a + u - s + 1, carry)
            carry = tick(off_a + u - s + 2, carry)
            step(u)
            step(u + 1)
            return carry

        carry = lax.fori_loop(0, k // 2, step2, carry)
        carry = lax.fori_loop(NU - k % 2, NU, step1, carry)
        carry = repeat(k % 2, advance, carry)
        carry = tick(off_a + k + 1, carry)

        @pl.when(sa >= ZAHEAD)
        def _():
            z_copy(sa - ZAHEAD).start()

        @pl.when(sa >= 1)
        def _():
            z_copy(sa - 1).wait()

        do_a()
        merge_t(sa)
        s1acc[...], s2acc[...] = do_g(jnp.minimum(off_a + k + 1, NCH - 1))
        store3(x3, xbuf[jnp.maximum(sa - 1, 0)].reshape(256, 512))
        store3(y3, mm_f32(tmat[...], wacc[...]))
        wacc[...] = jnp.zeros_like(wacc)
        return carry

    lax.fori_loop(0, NU, outer, carry)

    def o_copy(u):
        return pltpu.make_async_copy(xbuf.at[u], out_hbm.at[:, u], o_sem.at[u])

    def final(u, _):
        do_c(NCH - NU + u, u)
        o_copy(u).start()
        return 0

    lax.fori_loop(0, NU, final, 0)
    lax.fori_loop(0, NU, lambda u, _: (o_copy(u).wait(), 0)[1], 0)
    sent = vbuf.at[:, pl.ds(0, 64), pl.ds(0, 128)]
    for k in range(3):
        remote(sent, sent, k, rp_sem.at[0], dev1).wait_send()
    sent = vbuf.at[:, :, pl.ds(0, 128)]
    remote(sent, sent, 3, rp_sem.at[0], devp).wait_send()


def solution(mesh):
    def local_apply(v_loc, t_loc, z_loc):
        t4 = t_loc.reshape(NU, 2, 64, 64)
        zero = jnp.zeros_like(t4)
        first = lax.axis_index("col") == 0
        d_loc = jnp.concatenate([jnp.where(first, t4, zero), jnp.where(first, zero, t4)], axis=3)
        dma = pltpu.SemaphoreType.DMA
        out = pl.pallas_call(
            kernel,
            out_shape=jax.ShapeDtypeStruct((4, NU, 64, 512), F32),
            in_specs=[pl.BlockSpec(memory_space=pl.ANY)] * 3,
            out_specs=pl.BlockSpec(memory_space=pl.ANY),
            scratch_shapes=[
                pltpu.VMEM((NCH, 256, 256), F32),
                pltpu.VMEM((NU, 4, 64, 512), F32),
                pltpu.VMEM((NU, 2, 128, 128), F32),
                pltpu.VMEM((3, 256, 256), BF16),
                pltpu.VMEM((3, 256, 256), BF16),
                pltpu.VMEM((3, 256, 512), BF16),
                pltpu.VMEM((3, 256, 512), BF16),
                pltpu.VMEM((256, 512), F32),
                pltpu.VMEM((256, 256), F32),
                pltpu.VMEM((256, 256), F32),
                pltpu.VMEM((256, 256), F32),
                dma((NCH,)), dma((NCH,)), dma((NCH,)), dma((NCH,)), dma((NCH,)),
                dma((4,)), dma((NU,)), dma((3,)), dma((NU,)),
            ],
            compiler_params=pltpu.CompilerParams(
                collective_id=0, has_side_effects=True, vmem_limit_bytes=67_043_328
            ),
            cost_estimate=pl.CostEstimate(flops=116_000_000_000, bytes_accessed=60_000_000, transcendentals=0),
        )(v_loc.reshape(NU, 64, 2048), d_loc, z_loc.reshape(4, NU, 64, 512))
        return out.reshape(4096, 512)

    return jax.shard_map(
        local_apply,
        mesh=mesh,
        in_specs=(P("row", "col"), P("col", None, None), P(None, ("row", "col"))),
        out_specs=P(None, ("row", "col")),
        check_vma=False,
    )
```

```python
import functools

import jax
import jax.numpy as jnp
from jax import lax
from jax.experimental import pallas as pl
from jax.experimental.pallas import tpu as pltpu
from jax.sharding import PartitionSpec as P

MESH = pl.DeviceIdType.MESH
F32 = jnp.float32
BF16 = jnp.bfloat16

NU = 16
NCH = NU * (NU + 1) // 2
LEAD, GROW, LEAD_MAX = (8, 4, 1), (12, 8, 16), (14, 8, 2)
ZAHEAD = 4


def split3(x):
    h = x.astype(BF16)
    rem = x - h.astype(F32)
    m = rem.astype(BF16)
    l = (rem - m.astype(F32)).astype(BF16)
    return h, m, l


def dot(a, b):
    return jnp.dot(a, b, preferred_element_type=F32)


def mm6(a, b):
    ah, am, al = a
    bh, bm, bl = b
    return (dot(al, bh) + dot(ah, bl) + dot(am, bm)) + (dot(am, bh) + dot(ah, bm)) + dot(ah, bh)


def mm_f32(a, b):
    return mm6(split3(a), split3(b))


def mm_k128(a, b):
    ah, am, al = split3(a)
    bh, bm, bl = split3(b)

    def part(a0, a1, b0, b1):
        return dot(jnp.concatenate([a0, a1], axis=1), jnp.concatenate([b0, b1], axis=0))

    return (part(am, ah, bm, bl) + part(al, ah, bh, bm)) + part(am, ah, bh, bh)


def kernel(
    v_hbm, d_hbm, z_hbm, out_hbm,
    vbuf, xbuf, dbuf, vt3, vn3, x3, y3, wacc, s1acc, s2acc, tmat,
    r1_sem, r2_sem, rd_sem, rp_sem, loc_sem, send_sem, z_sem, d_sem, o_sem,
):
    r = lax.axis_index("row")
    q = lax.axis_index("col")
    ry, rx = r // 2, r % 2
    row_x = ry * 2 + (1 - rx)
    row_y = (1 - ry) * 2 + rx
    n1 = row_x * (1 - q) + row_y * q
    n2 = row_y * (1 - q) + row_x * q
    nd = 3 - r
    dev1, dev2, devp = (n1, q), (n2, q), (r, 1 - q)
    cols = pl.ds(pl.multiple_of(q * 128, 128), 128)

    def piece(c, rr):
        return vbuf.at[c, pl.ds(pl.multiple_of(rr * 64, 64), 64), cols]

    def remote(src, dst, k, rsem, dev):
        return pltpu.make_async_remote_copy(
            src_ref=src, dst_ref=dst, send_sem=send_sem.at[k], recv_sem=rsem,
            device_id=dev, device_id_type=MESH,
        )

    def own_src(s, u):
        return v_hbm.at[u, :, pl.ds(pl.multiple_of(s * 128, 128), 128)]

    def stage0(c, s, u):
        src = own_src(s, u)
        remote(src, piece(c, r), 0, r1_sem.at[c], dev1).start()
        remote(src, piece(c, r), 1, r2_sem.at[c], dev2).start()
        pltpu.make_async_copy(src, piece(c, r), loc_sem.at[c]).start()

    def stage1(c):
        p = piece(c, n1)
        remote(p, p, 0, r1_sem.at[c], dev1).wait_recv()
        remote(p, p, 2, rd_sem.at[c], dev2).start()

    def stage2(c):
        p = piece(c, n2)
        remote(p, p, 1, r2_sem.at[c], dev2).wait_recv()
        p = piece(c, nd)
        remote(p, p, 2, rd_sem.at[c], dev2).wait_recv()
        p = piece(c, r)
        pltpu.make_async_copy(p, p, loc_sem.at[c]).wait()
        p = vbuf.at[c, :, cols]
        remote(p, p, 3, rp_sem.at[c], devp).start()

    def stage3(c):
        p = vbuf.at[c, :, pl.ds(pl.multiple_of((1 - q) * 128, 128), 128)]
        remote(p, p, 3, rp_sem.at[c], devp).wait_recv()

    def target(i, c):
        ahead = jnp.minimum(LEAD[i] + c * GROW[i] // 16, LEAD_MAX[i])
        return jnp.minimum(c + ahead, NCH)

    def run0(lo, hi, su):
        def body(n, su):
            s, u = su
            stage0(n, s, u)
            last = u == NU - 1
            s2 = jnp.where(last, jnp.maximum(s - 1, 0), s)
            return s2, jnp.where(last, s2, u + 1)

        return lax.fori_loop(lo, hi, body, su)

    def run(i, lo, hi):
        def body(n, _):
            (None, stage1, stage2)[i](n)
            return 0

        lax.fori_loop(lo, hi, body, 0)

    def tick(c, su):
        for i in (1, 2):
            run(i, target(i, c), target(i, c + 1))
        su = run0(target(0, c), target(0, c + 1), su)

        @pl.when(c < NCH)
        def _():
            stage3(c)

        return su

    barrier = pltpu.get_barrier_semaphore()
    for dev in (dev1, dev2, devp):
        pl.semaphore_signal(barrier, inc=1, device_id=dev, device_id_type=MESH)
    pl.semaphore_wait(barrier, 3)

    d_own = dbuf.at[:, :, pl.ds(pl.multiple_of(q * 64, 64), 64), :]
    d_send = pltpu.make_async_remote_copy(
        src_ref=d_hbm, dst_ref=d_own, send_sem=d_sem.at[0], recv_sem=d_sem.at[1],
        device_id=devp, device_id_type=MESH,
    )
    d_send.start()
    d_loc = pltpu.make_async_copy(d_hbm, d_own, d_sem.at[2])
    d_loc.start()

    def z_copy(u):
        return pltpu.make_async_copy(z_hbm.at[:, u], xbuf.at[u], z_sem.at[u])

    for i in range(ZAHEAD):
        z_copy(NU - 1 - i).start()
    carry = run0(0, target(0, 0), (jnp.int32(NU - 1), jnp.int32(NU - 1)))
    for i in (1, 2):
        run(i, 0, target(i, 0))
    d_send.wait()
    d_loc.wait()

    def store3(ref, x):
        ref[0], ref[1], ref[2] = split3(x)

    def load3(ref):
        return ref[0], ref[1], ref[2]

    def do_a():
        wacc[...] += mm6(load3(vt3), load3(x3))

    def do_c(c, u):
        x = xbuf[u].reshape(256, 512) - mm6(split3(vbuf[c]), load3(y3))
        xbuf[u] = x.reshape(4, 64, 512)
        return x

    def do_g(c):
        v = vbuf[c]
        store3(vn3, v)
        store3(vt3, v.T)
        g1 = dot(vt3[1], vn3[1]) + dot(vt3[0], vn3[0])
        g2 = dot(vt3[0], vn3[2]) + dot(vt3[0], vn3[1])
        return g1, g2

    low = lax.broadcasted_iota(jnp.int32, (64, 128), 1) < 64

    def roll(x):
        return pltpu.roll(x, 64, 1)

    def merge_t(s):
        s2 = s2acc[...]
        g = s1acc[...] + s2 + s2.T
        zero = jnp.zeros((64, 128), F32)
        d01, d23 = dbuf[s, 0], dbuf[s, 1]
        u01 = jnp.concatenate([jnp.where(low, 0.0, roll(g[:64, 128:])), zero], axis=0)
        u23 = jnp.concatenate([jnp.where(low, 0.0, g[64:128, 128:]), zero], axis=0)
        u2 = jnp.concatenate(
            [
                jnp.where(low, roll(g[:64, :128]), g[:64, 128:]),
                jnp.where(low, roll(g[128:192, :128]), g[128:192, 128:]),
            ],
            axis=0,
        )
        nm = mm_k128(d01, jnp.concatenate([u01, u2], axis=1))
        z = mm_k128(u23, d23)
        el = mm_k128(nm[:, :128], jnp.concatenate([d01, nm[:, 128:]], axis=1))
        t01 = d01 - el[:, :128]
        t23 = d23 - mm_k128(d23, z)
        f = -mm_k128(nm[:, 128:] - el[:, 128:], t23)
        tmat[0:64, 0:128] = jnp.where(low, t01[:64], roll(f[:64]))
        tmat[0:64, 128:256] = jnp.where(low, roll(t01[:64]), f[:64])
        tmat[64:128, 0:128] = jnp.where(low, 0.0, roll(t23[:64]))
        tmat[64:128, 128:256] = jnp.where(low, 0.0, t23[:64])
        tmat[128:192, 0:128] = jnp.where(low, 0.0, roll(f[64:]))
        tmat[128:192, 128:256] = jnp.where(low, roll(t01[64:]), f[64:])
        tmat[192:256, 0:128] = zero
        tmat[192:256, 128:256] = t23[64:]

    def offset(s):
        return (NU - 1 - s) * (NU - s) // 2

    carry = tick(0, carry)
    z_copy(NU - 1).wait()
    wacc[...] = jnp.zeros_like(wacc)
    s1acc[...], s2acc[...] = do_g(0)
    store3(x3, xbuf[NU - 1].reshape(256, 512))

    def outer(k, carry):
        s = NU - k
        sa = s - 1
        off_a = offset(sa)
        off_c = off_a - k

        def step(u):
            i = u - s
            do_a()
            x = do_c(off_c + i, u)
            g1, g2 = do_g(off_a + i + 1)
            s1acc[...] += g1
            s2acc[...] += g2
            store3(x3, x)

        def step1(u, carry):
            carry = tick(off_a + u - s + 1, carry)
            step(u)
            return carry

        def step2(j, carry):
            u = s + 2 * j
            carry = tick(off_a + u - s + 1, carry)
            carry = tick(off_a + u - s + 2, carry)
            step(u)
            step(u + 1)
            return carry

        carry = lax.fori_loop(0, k // 2, step2, carry)
        carry = lax.fori_loop(NU - k % 2, NU, step1, carry)
        carry = tick(off_a + k + 1, carry)

        @pl.when(sa >= ZAHEAD)
        def _():
            z_copy(sa - ZAHEAD).start()

        @pl.when(sa >= 1)
        def _():
            z_copy(sa - 1).wait()

        do_a()
        merge_t(sa)
        s1acc[...], s2acc[...] = do_g(jnp.minimum(off_a + k + 1, NCH - 1))
        store3(x3, xbuf[jnp.maximum(sa - 1, 0)].reshape(256, 512))
        store3(y3, mm_f32(tmat[...], wacc[...]))
        wacc[...] = jnp.zeros_like(wacc)
        return carry

    lax.fori_loop(0, NU, outer, carry)

    def o_copy(u):
        return pltpu.make_async_copy(xbuf.at[u], out_hbm.at[:, u], o_sem.at[u])

    def final(u, _):
        do_c(NCH - NU + u, u)
        o_copy(u).start()
        return 0

    lax.fori_loop(0, NU, final, 0)
    lax.fori_loop(0, NU, lambda u, _: (o_copy(u).wait(), 0)[1], 0)
    sent = vbuf.at[:, pl.ds(0, 64), pl.ds(0, 128)]
    for k in range(3):
        remote(sent, sent, k, rp_sem.at[0], dev1).wait_send()
    sent = vbuf.at[:, :, pl.ds(0, 128)]
    remote(sent, sent, 3, rp_sem.at[0], devp).wait_send()


def solution(mesh):
    def local_apply(v_loc, t_loc, z_loc):
        t4 = t_loc.reshape(NU, 2, 64, 64)
        zero = jnp.zeros_like(t4)
        first = lax.axis_index("col") == 0
        d_loc = jnp.concatenate([jnp.where(first, t4, zero), jnp.where(first, zero, t4)], axis=3)
        dma = pltpu.SemaphoreType.DMA
        out = pl.pallas_call(
            kernel,
            out_shape=jax.ShapeDtypeStruct((4, NU, 64, 512), F32),
            in_specs=[pl.BlockSpec(memory_space=pl.ANY)] * 3,
            out_specs=pl.BlockSpec(memory_space=pl.ANY),
            scratch_shapes=[
                pltpu.VMEM((NCH, 256, 256), F32),
                pltpu.VMEM((NU, 4, 64, 512), F32),
                pltpu.VMEM((NU, 2, 128, 128), F32),
                pltpu.VMEM((3, 256, 256), BF16),
                pltpu.VMEM((3, 256, 256), BF16),
                pltpu.VMEM((3, 256, 512), BF16),
                pltpu.VMEM((3, 256, 512), BF16),
                pltpu.VMEM((256, 512), F32),
                pltpu.VMEM((256, 256), F32),
                pltpu.VMEM((256, 256), F32),
                pltpu.VMEM((256, 256), F32),
                dma((NCH,)), dma((NCH,)), dma((NCH,)), dma((NCH,)), dma((NCH,)),
                dma((4,)), dma((NU,)), dma((3,)), dma((NU,)),
            ],
            compiler_params=pltpu.CompilerParams(
                collective_id=0, has_side_effects=True, vmem_limit_bytes=67_043_328
            ),
            cost_estimate=pl.CostEstimate(flops=116_000_000_000, bytes_accessed=60_000_000, transcendentals=0),
        )(v_loc.reshape(NU, 64, 2048), d_loc, z_loc.reshape(4, NU, 64, 512))
        return out.reshape(4096, 512)

    return jax.shard_map(
        local_apply,
        mesh=mesh,
        in_specs=(P("row", "col"), P("col", None, None), P(None, ("row", "col"))),
        out_specs=P(None, ("row", "col")),
        check_vma=False,
    )
```

```python
import functools

import jax
import jax.numpy as jnp
from jax import lax
from jax.experimental import pallas as pl
from jax.experimental.pallas import tpu as pltpu
from jax.sharding import PartitionSpec as P

MESH = pl.DeviceIdType.MESH
F32 = jnp.float32
BF16 = jnp.bfloat16

NU = 16
NCH = NU * (NU + 1) // 2
LEAD, GROW, LEAD_MAX = (8, 4, 1), (12, 8, 16), (14, 8, 2)
ZAHEAD = 4


def split3(x):
    h = x.astype(BF16)
    rem = x - h.astype(F32)
    m = rem.astype(BF16)
    l = (rem - m.astype(F32)).astype(BF16)
    return h, m, l


def dot(a, b):
    return jnp.dot(a, b, preferred_element_type=F32)


def mm6(a, b):
    ah, am, al = a
    bh, bm, bl = b
    return (dot(al, bh) + dot(ah, bl) + dot(am, bm)) + (dot(am, bh) + dot(ah, bm)) + dot(ah, bh)


def mm_f32(a, b):
    return mm6(split3(a), split3(b))


def mm_k128(a, b):
    ah, am, al = split3(a)
    bh, bm, bl = split3(b)

    def part(a0, a1, b0, b1):
        return dot(jnp.concatenate([a0, a1], axis=1), jnp.concatenate([b0, b1], axis=0))

    return (part(am, ah, bm, bl) + part(al, ah, bh, bm)) + part(am, ah, bh, bh)


def kernel(
    v_hbm, d_hbm, z_hbm, out_hbm,
    vbuf, xbuf, dbuf, vt3, vt3b, vn3, x3, x3b, y3, wacc, s1acc, s2acc, tmat,
    r1_sem, r2_sem, rd_sem, rp_sem, loc_sem, send_sem, z_sem, d_sem, o_sem,
):
    r = lax.axis_index("row")
    q = lax.axis_index("col")
    ry, rx = r // 2, r % 2
    row_x = ry * 2 + (1 - rx)
    row_y = (1 - ry) * 2 + rx
    n1 = row_x * (1 - q) + row_y * q
    n2 = row_y * (1 - q) + row_x * q
    nd = 3 - r
    dev1, dev2, devp = (n1, q), (n2, q), (r, 1 - q)
    cols = pl.ds(pl.multiple_of(q * 128, 128), 128)

    def piece(c, rr):
        return vbuf.at[c, pl.ds(pl.multiple_of(rr * 64, 64), 64), cols]

    def remote(src, dst, k, rsem, dev):
        return pltpu.make_async_remote_copy(
            src_ref=src, dst_ref=dst, send_sem=send_sem.at[k], recv_sem=rsem,
            device_id=dev, device_id_type=MESH,
        )

    def own_src(s, u):
        return v_hbm.at[u, :, pl.ds(pl.multiple_of(s * 128, 128), 128)]

    def stage0(c, s, u):
        src = own_src(s, u)
        remote(src, piece(c, r), 0, r1_sem.at[c], dev1).start()
        remote(src, piece(c, r), 1, r2_sem.at[c], dev2).start()
        pltpu.make_async_copy(src, piece(c, r), loc_sem.at[c]).start()

    def stage1(c):
        p = piece(c, n1)
        remote(p, p, 0, r1_sem.at[c], dev1).wait_recv()
        remote(p, p, 2, rd_sem.at[c], dev2).start()

    def stage2(c):
        p = piece(c, n2)
        remote(p, p, 1, r2_sem.at[c], dev2).wait_recv()
        p = piece(c, nd)
        remote(p, p, 2, rd_sem.at[c], dev2).wait_recv()
        p = piece(c, r)
        pltpu.make_async_copy(p, p, loc_sem.at[c]).wait()
        p = vbuf.at[c, :, cols]
        remote(p, p, 3, rp_sem.at[c], devp).start()

    def stage3(c):
        p = vbuf.at[c, :, pl.ds(pl.multiple_of((1 - q) * 128, 128), 128)]
        remote(p, p, 3, rp_sem.at[c], devp).wait_recv()

    def target(i, c):
        ahead = jnp.minimum(LEAD[i] + c * GROW[i] // 16, LEAD_MAX[i])
        return jnp.minimum(c + ahead, NCH)

    def run0(lo, hi, su):
        def body(n, su):
            s, u = su
            stage0(n, s, u)
            last = u == NU - 1
            s2 = jnp.where(last, jnp.maximum(s - 1, 0), s)
            return s2, jnp.where(last, s2, u + 1)

        return lax.fori_loop(lo, hi, body, su)

    def run(i, lo, hi):
        def body(n, _):
            (None, stage1, stage2)[i](n)
            return 0

        lax.fori_loop(lo, hi, body, 0)

    def tick(c, su):
        for i in (1, 2):
            run(i, target(i, c), target(i, c + 1))
        su = run0(target(0, c), target(0, c + 1), su)

        @pl.when(c < NCH)
        def _():
            stage3(c)

        return su

    barrier = pltpu.get_barrier_semaphore()
    for dev in (dev1, dev2, devp):
        pl.semaphore_signal(barrier, inc=1, device_id=dev, device_id_type=MESH)
    pl.semaphore_wait(barrier, 3)

    d_own = dbuf.at[:, :, pl.ds(pl.multiple_of(q * 64, 64), 64), :]
    d_send = pltpu.make_async_remote_copy(
        src_ref=d_hbm, dst_ref=d_own, send_sem=d_sem.at[0], recv_sem=d_sem.at[1],
        device_id=devp, device_id_type=MESH,
    )
    d_send.start()
    d_loc = pltpu.make_async_copy(d_hbm, d_own, d_sem.at[2])
    d_loc.start()

    def z_copy(u):
        return pltpu.make_async_copy(z_hbm.at[:, u], xbuf.at[u], z_sem.at[u])

    for i in range(ZAHEAD):
        z_copy(NU - 1 - i).start()
    carry = run0(0, target(0, 0), (jnp.int32(NU - 1), jnp.int32(NU - 1)))
    for i in (1, 2):
        run(i, 0, target(i, 0))
    d_send.wait()
    d_loc.wait()

    def store3(ref, x):
        ref[0], ref[1], ref[2] = split3(x)

    def load3(ref):
        return ref[0], ref[1], ref[2]

    def do_a(vt, x):
        return mm6(load3(vt), load3(x))

    def do_c(c, u):
        x = xbuf[u].reshape(256, 512) - mm6(split3(vbuf[c]), load3(y3))
        xbuf[u] = x.reshape(4, 64, 512)
        return x

    def do_g(c, vt):
        v = vbuf[c]
        store3(vn3, v)
        store3(vt, v.T)
        g1 = dot(vt[1], vn3[1]) + dot(vt[0], vn3[0])
        g2 = dot(vt[0], vn3[2]) + dot(vt[0], vn3[1])
        return g1, g2

    low = lax.broadcasted_iota(jnp.int32, (64, 128), 1) < 64

    def roll(x):
        return pltpu.roll(x, 64, 1)

    def merge_1(s, s1, s2):
        g = s1 + s2 + s2.T
        zero = jnp.zeros((64, 128), F32)
        d01, d23 = dbuf[s, 0], dbuf[s, 1]
        u01 = jnp.concatenate([jnp.where(low, 0.0, roll(g[:64, 128:])), zero], axis=0)
        u23 = jnp.concatenate([jnp.where(low, 0.0, g[64:128, 128:]), zero], axis=0)
        u2 = jnp.concatenate(
            [
                jnp.where(low, roll(g[:64, :128]), g[:64, 128:]),
                jnp.where(low, roll(g[128:192, :128]), g[128:192, 128:]),
            ],
            axis=0,
        )
        nm = mm_k128(d01, jnp.concatenate([u01, u2], axis=1))
        z = mm_k128(u23, d23)
        return nm, z

    def merge_2(s, nm, z):
        d01, d23 = dbuf[s, 0], dbuf[s, 1]
        el = mm_k128(nm[:, :128], jnp.concatenate([d01, nm[:, 128:]], axis=1))
        t23 = d23 - mm_k128(d23, z)
        return d01 - el[:, :128], nm[:, 128:] - el[:, 128:], t23

    def merge_3(t01, lm, t23):
        f = -mm_k128(lm, t23)
        tmat[0:64, 0:128] = jnp.where(low, t01[:64], roll(f[:64]))
        tmat[0:64, 128:256] = jnp.where(low, roll(t01[:64]), f[:64])
        tmat[64:128, 0:128] = jnp.where(low, 0.0, roll(t23[:64]))
        tmat[64:128, 128:256] = jnp.where(low, 0.0, t23[:64])
        tmat[128:192, 0:128] = jnp.where(low, 0.0, roll(f[64:]))
        tmat[128:192, 128:256] = jnp.where(low, roll(t01[64:]), f[64:])
        tmat[192:256, 0:128] = jnp.zeros((64, 128), F32)
        tmat[192:256, 128:256] = t23[64:]

    def offset(s):
        return (NU - 1 - s) * (NU - s) // 2

    carry = tick(0, carry)
    z_copy(NU - 1).wait()
    wacc[...] = jnp.zeros_like(wacc)
    s1acc[...], s2acc[...] = do_g(0, vt3)
    store3(x3, xbuf[NU - 1].reshape(256, 512))

    def step(c_a, c_c, u):
        wacc[...] += do_a(vt3, x3)
        x = do_c(c_c, u)
        g1, g2 = do_g(c_a + 1, vt3)
        s1acc[...] += g1
        s2acc[...] += g2
        store3(x3, x)

    def first_g(c):
        s1acc[...], s2acc[...] = do_g(jnp.minimum(c, NCH - 1), vt3)

    def finish(sa, w):
        store3(x3, xbuf[jnp.maximum(sa - 1, 0)].reshape(256, 512))
        store3(y3, mm_f32(tmat[...], w))
        wacc[...] = jnp.zeros_like(wacc)

    def next_z(sa):
        @pl.when(sa >= ZAHEAD)
        def _():
            z_copy(sa - ZAHEAD).start()

        @pl.when(sa >= 1)
        def _():
            z_copy(sa - 1).wait()

    carry = tick(1, carry)
    next_z(NU - 1)
    vt3b[...] = vt3[...]
    x3b[...] = x3[...]
    merge_3(*merge_2(NU - 1, *merge_1(NU - 1, s1acc[...], s2acc[...])))
    first_g(1)
    finish(NU - 1, do_a(vt3b, x3b))

    def outer(k, carry):
        s = NU - k
        sa = s - 1
        off_a = offset(sa)
        off_c = off_a - k

        def step1(u, carry):
            i = u - s
            carry = tick(off_a + i + 1, carry)
            step(off_a + i, off_c + i, u)
            return carry

        def step2(j, carry):
            i = 2 * j
            carry = tick(off_a + i + 1, carry)
            carry = tick(off_a + i + 2, carry)
            step(off_a + i, off_c + i, s + i)
            step(off_a + i + 1, off_c + i + 1, s + i + 1)
            return carry

        pairs = (k - 1) // 2
        carry = lax.fori_loop(0, pairs, step2, carry)
        carry = lax.fori_loop(s + 2 * pairs, NU - 1, step1, carry)

        carry = tick(off_a + k, carry)
        carry = tick(off_a + k + 1, carry)
        next_z(sa)
        store3(x3b, do_c(off_c + k - 1, NU - 1))
        g1, g2 = do_g(off_a + k, vt3b)
        w = wacc[...] + do_a(vt3, x3)
        part = merge_1(sa, s1acc[...] + g1, s2acc[...] + g2)
        w = w + do_a(vt3b, x3b)
        part = merge_2(sa, *part)
        first_g(off_a + k + 1)
        merge_3(*part)
        finish(sa, w)
        return carry

    lax.fori_loop(1, NU, outer, carry)

    def o_copy(u):
        return pltpu.make_async_copy(xbuf.at[u], out_hbm.at[:, u], o_sem.at[u])

    def final(u, _):
        do_c(NCH - NU + u, u)
        o_copy(u).start()
        return 0

    lax.fori_loop(0, NU, final, 0)
    lax.fori_loop(0, NU, lambda u, _: (o_copy(u).wait(), 0)[1], 0)
    sent = vbuf.at[:, pl.ds(0, 64), pl.ds(0, 128)]
    for k in range(3):
        remote(sent, sent, k, rp_sem.at[0], dev1).wait_send()
    sent = vbuf.at[:, :, pl.ds(0, 128)]
    remote(sent, sent, 3, rp_sem.at[0], devp).wait_send()


def solution(mesh):
    def local_apply(v_loc, t_loc, z_loc):
        t4 = t_loc.reshape(NU, 2, 64, 64)
        zero = jnp.zeros_like(t4)
        first = lax.axis_index("col") == 0
        d_loc = jnp.concatenate([jnp.where(first, t4, zero), jnp.where(first, zero, t4)], axis=3)
        dma = pltpu.SemaphoreType.DMA
        out = pl.pallas_call(
            kernel,
            out_shape=jax.ShapeDtypeStruct((4, NU, 64, 512), F32),
            in_specs=[pl.BlockSpec(memory_space=pl.ANY)] * 3,
            out_specs=pl.BlockSpec(memory_space=pl.ANY),
            scratch_shapes=[
                pltpu.VMEM((NCH, 256, 256), F32),
                pltpu.VMEM((NU, 4, 64, 512), F32),
                pltpu.VMEM((NU, 2, 128, 128), F32),
                pltpu.VMEM((3, 256, 256), BF16),
                pltpu.VMEM((3, 256, 256), BF16),
                pltpu.VMEM((3, 256, 256), BF16),
                pltpu.VMEM((3, 256, 512), BF16),
                pltpu.VMEM((3, 256, 512), BF16),
                pltpu.VMEM((3, 256, 512), BF16),
                pltpu.VMEM((256, 512), F32),
                pltpu.VMEM((256, 256), F32),
                pltpu.VMEM((256, 256), F32),
                pltpu.VMEM((256, 256), F32),
                dma((NCH,)), dma((NCH,)), dma((NCH,)), dma((NCH,)), dma((NCH,)),
                dma((4,)), dma((NU,)), dma((3,)), dma((NU,)),
            ],
            compiler_params=pltpu.CompilerParams(
                collective_id=0, has_side_effects=True, vmem_limit_bytes=67_043_328
            ),
            cost_estimate=pl.CostEstimate(flops=116_000_000_000, bytes_accessed=60_000_000, transcendentals=0),
        )(v_loc.reshape(NU, 64, 2048), d_loc, z_loc.reshape(4, NU, 64, 512))
        return out.reshape(4096, 512)

    return jax.shard_map(
        local_apply,
        mesh=mesh,
        in_specs=(P("row", "col"), P("col", None, None), P(None, ("row", "col"))),
        out_specs=P(None, ("row", "col")),
        check_vma=False,
    )
```

```python
import functools

import jax
import jax.numpy as jnp
from jax import lax
from jax.experimental import pallas as pl
from jax.experimental.pallas import tpu as pltpu
from jax.sharding import PartitionSpec as P

MESH = pl.DeviceIdType.MESH
F32 = jnp.float32
BF16 = jnp.bfloat16

NU = 16
NCH = NU * (NU + 1) // 2
NP = NCH // 2
LEAD, GROW, LEAD_MAX = (5, 3, 1), (4, 2, 8), (9, 5, 1)
ZAHEAD = 4


def split3(x):
    h = x.astype(BF16)
    rem = x - h.astype(F32)
    m = rem.astype(BF16)
    l = (rem - m.astype(F32)).astype(BF16)
    return h, m, l


def dot(a, b):
    return jnp.dot(a, b, preferred_element_type=F32)


def mm6(a, b):
    ah, am, al = a
    bh, bm, bl = b
    return (dot(al, bh) + dot(ah, bl) + dot(am, bm)) + (dot(am, bh) + dot(ah, bm)) + dot(ah, bh)


def mm_f32(a, b):
    return mm6(split3(a), split3(b))


def mm_k128(a, b):
    ah, am, al = split3(a)
    bh, bm, bl = split3(b)

    def part(a0, a1, b0, b1):
        return dot(jnp.concatenate([a0, a1], axis=1), jnp.concatenate([b0, b1], axis=0))

    return (part(am, ah, bm, bl) + part(al, ah, bh, bm)) + part(am, ah, bh, bh)


def kernel(
    v_hbm, d_hbm, z_hbm, out_hbm,
    vbuf, xbuf, dbuf, vt3, vt3b, vn3, x3, x3b, y3, wacc, s1acc, s2acc, tmat,
    r1_sem, r2_sem, rp_sem, send_sem, z_sem, d_sem, o_sem,
):
    r = lax.axis_index("row")
    q = lax.axis_index("col")
    ry, rx = r // 2, r % 2
    row_x = ry * 2 + (1 - rx)
    row_y = (1 - ry) * 2 + rx
    n1 = row_x * (1 - q) + row_y * q
    n2 = row_y * (1 - q) + row_x * q
    dev1, dev2, devp = (n1, q), (n2, q), (r, 1 - q)
    cols = pl.ds(pl.multiple_of(q * 128, 128), 128)

    def piece(c, n, rr):
        return vbuf.at[pl.ds(c, n), pl.ds(pl.multiple_of(rr * 64, 64), 64), cols]

    def remote(src, dst, k, rsem, dev):
        return pltpu.make_async_remote_copy(
            src_ref=src, dst_ref=dst, send_sem=send_sem.at[k], recv_sem=rsem,
            device_id=dev, device_id_type=MESH,
        )

    def stage0(p, c, s, u):
        src = v_hbm.at[pl.ds(u, 1), :, pl.ds(pl.multiple_of(s * 128, 128), 128)]
        dst = piece(c, 1, r)
        remote(src, dst, 0, r1_sem.at[p], dev1).start()
        remote(src, dst, 1, r2_sem.at[p], dev2).start()
        pltpu.make_async_copy(src, dst, r2_sem.at[p]).start()

    def stage1(p):
        x = piece(2 * p, 2, n1)
        remote(x, x, 0, r1_sem.at[p], dev1).wait_recv()
        remote(x, x, 2, r2_sem.at[p], dev2).start()

    def stage2(p):
        x = vbuf.at[pl.ds(2 * p, 2), pl.ds(0, 192), cols]
        remote(x, x, 1, r2_sem.at[p], dev2).wait_recv()
        x = vbuf.at[pl.ds(2 * p, 2), :, cols]
        remote(x, x, 3, rp_sem.at[p], devp).start()

    def stage3(p):
        x = vbuf.at[pl.ds(2 * p, 2), :, pl.ds(pl.multiple_of((1 - q) * 128, 128), 128)]
        remote(x, x, 3, rp_sem.at[p], devp).wait_recv()

    def target(i, p):
        ahead = jnp.minimum(LEAD[i] + p * GROW[i] // 16, LEAD_MAX[i])
        return jnp.minimum(p + ahead, NP)

    def run0(lo, hi, su):
        def body(p, su):
            s, u = su
            for i in range(2):
                stage0(p, 2 * p + i, s, u)
                last = u == NU - 1
                s2 = jnp.where(last, jnp.maximum(s - 1, 0), s)
                s, u = s2, jnp.where(last, s2, u + 1)
            return s, u

        return lax.fori_loop(lo, hi, body, su)

    def run(i, lo, hi):
        def body(n, _):
            (None, stage1, stage2)[i](n)
            return 0

        lax.fori_loop(lo, hi, body, 0)

    def tick(p, su):
        for i in (1, 2):
            run(i, target(i, p), target(i, p + 1))
        su = run0(target(0, p), target(0, p + 1), su)

        @pl.when(p < NP)
        def _():
            stage3(p)

        return su

    barrier = pltpu.get_barrier_semaphore()
    for dev in (dev1, dev2, devp):
        pl.semaphore_signal(barrier, inc=1, device_id=dev, device_id_type=MESH)
    pl.semaphore_wait(barrier, 3)

    d_own = dbuf.at[q]
    d_send = pltpu.make_async_remote_copy(
        src_ref=d_hbm, dst_ref=d_own, send_sem=d_sem.at[0], recv_sem=d_sem.at[1],
        device_id=devp, device_id_type=MESH,
    )
    d_send.start()
    d_loc = pltpu.make_async_copy(d_hbm, d_own, d_sem.at[2])
    d_loc.start()

    def z_copy(u):
        return pltpu.make_async_copy(z_hbm.at[:, u], xbuf.at[u], z_sem.at[u])

    for i in range(ZAHEAD):
        z_copy(NU - 1 - i).start()
    carry = run0(0, target(0, 0), (jnp.int32(NU - 1), jnp.int32(NU - 1)))
    for i in (1, 2):
        run(i, 0, target(i, 0))
    d_send.wait()
    d_loc.wait()

    def store3(ref, x):
        ref[0], ref[1], ref[2] = split3(x)

    def load3(ref):
        return ref[0], ref[1], ref[2]

    def do_a(vt, x):
        return mm6(load3(vt), load3(x))

    def do_c(c, u):
        x = xbuf[u].reshape(256, 512) - mm6(split3(vbuf[c]), load3(y3))
        xbuf[u] = x.reshape(4, 64, 512)
        return x

    def do_g(c, vt):
        v = vbuf[c]
        store3(vn3, v)
        store3(vt, v.T)
        g1 = dot(vt[1], vn3[1]) + dot(vt[0], vn3[0])
        g2 = dot(vt[0], vn3[2]) + dot(vt[0], vn3[1])
        return g1, g2

    low = lax.broadcasted_iota(jnp.int32, (64, 128), 1) < 64

    def roll(x):
        return pltpu.roll(x, 64, 1)

    def diag(s, i):
        zero = jnp.zeros((64, 64), F32)
        return jnp.concatenate(
            [
                jnp.concatenate([dbuf[0, s, i], zero], axis=1),
                jnp.concatenate([zero, dbuf[1, s, i]], axis=1),
            ],
            axis=0,
        )

    def merge_1(s, s1, s2):
        g = s1 + s2 + s2.T
        zero = jnp.zeros((64, 128), F32)
        d01, d23 = diag(s, 0), diag(s, 1)
        u01 = jnp.concatenate([jnp.where(low, 0.0, roll(g[:64, 128:])), zero], axis=0)
        u23 = jnp.concatenate([jnp.where(low, 0.0, g[64:128, 128:]), zero], axis=0)
        u2 = jnp.concatenate(
            [
                jnp.where(low, roll(g[:64, :128]), g[:64, 128:]),
                jnp.where(low, roll(g[128:192, :128]), g[128:192, 128:]),
            ],
            axis=0,
        )
        nm = mm_k128(d01, jnp.concatenate([u01, u2], axis=1))
        z = mm_k128(u23, d23)
        return nm, z

    def merge_2(s, nm, z):
        d01, d23 = diag(s, 0), diag(s, 1)
        el = mm_k128(nm[:, :128], jnp.concatenate([d01, nm[:, 128:]], axis=1))
        t23 = d23 - mm_k128(d23, z)
        return d01 - el[:, :128], nm[:, 128:] - el[:, 128:], t23

    def merge_3(t01, lm, t23):
        f = -mm_k128(lm, t23)
        tmat[0:64, 0:128] = jnp.where(low, t01[:64], roll(f[:64]))
        tmat[0:64, 128:256] = jnp.where(low, roll(t01[:64]), f[:64])
        tmat[64:128, 0:128] = jnp.where(low, 0.0, roll(t23[:64]))
        tmat[64:128, 128:256] = jnp.where(low, 0.0, t23[:64])
        tmat[128:192, 0:128] = jnp.where(low, 0.0, roll(f[64:]))
        tmat[128:192, 128:256] = jnp.where(low, roll(t01[64:]), f[64:])
        tmat[192:256, 0:128] = jnp.zeros((64, 128), F32)
        tmat[192:256, 128:256] = t23[64:]

    def offset(s):
        return (NU - 1 - s) * (NU - s) // 2

    carry = tick(0, carry)
    z_copy(NU - 1).wait()
    wacc[...] = jnp.zeros_like(wacc)
    s1acc[...], s2acc[...] = do_g(0, vt3)
    store3(x3, xbuf[NU - 1].reshape(256, 512))

    def step(c_a, c_c, u):
        wacc[...] += do_a(vt3, x3)
        x = do_c(c_c, u)
        g1, g2 = do_g(c_a + 1, vt3)
        s1acc[...] += g1
        s2acc[...] += g2
        store3(x3, x)

    def first_g(c):
        s1acc[...], s2acc[...] = do_g(jnp.minimum(c, NCH - 1), vt3)

    def finish(sa, w):
        store3(x3, xbuf[jnp.maximum(sa - 1, 0)].reshape(256, 512))
        store3(y3, mm_f32(tmat[...], w))
        wacc[...] = jnp.zeros_like(wacc)

    def next_z(sa):
        @pl.when(sa >= ZAHEAD)
        def _():
            z_copy(sa - ZAHEAD).start()

        @pl.when(sa >= 1)
        def _():
            z_copy(sa - 1).wait()

    next_z(NU - 1)
    vt3b[...] = vt3[...]
    x3b[...] = x3[...]
    merge_3(*merge_2(NU - 1, *merge_1(NU - 1, s1acc[...], s2acc[...])))
    first_g(1)
    finish(NU - 1, do_a(vt3b, x3b))

    def outer(k, carry):
        s = NU - k
        sa = s - 1
        off_a = offset(sa)
        off_c = off_a - k

        def step1(u, carry):
            i = u - s
            c = off_a + i + 1
            carry = lax.cond(c % 2 == 0, lambda su: tick(c // 2, su), lambda su: su, carry)
            step(off_a + i, off_c + i, u)
            return carry

        def step2(j, carry):
            i = 2 * j
            carry = tick((off_a + i + 2) // 2, carry)
            step(off_a + i, off_c + i, s + i)
            step(off_a + i + 1, off_c + i + 1, s + i + 1)
            return carry

        pairs = (k - 1) // 2
        carry = lax.fori_loop(0, pairs, step2, carry)
        carry = lax.fori_loop(s + 2 * pairs, NU - 1, step1, carry)

        carry = tick((off_a + k + 1) // 2, carry)
        next_z(sa)
        store3(x3b, do_c(off_c + k - 1, NU - 1))
        g1, g2 = do_g(off_a + k, vt3b)
        w = wacc[...] + do_a(vt3, x3)
        part = merge_1(sa, s1acc[...] + g1, s2acc[...] + g2)
        w = w + do_a(vt3b, x3b)
        part = merge_2(sa, *part)
        first_g(off_a + k + 1)
        merge_3(*part)
        finish(sa, w)
        return carry

    lax.fori_loop(1, NU, outer, carry)

    def o_copy(u):
        return pltpu.make_async_copy(xbuf.at[u], out_hbm.at[:, u], o_sem.at[u])

    def final(u, _):
        do_c(NCH - NU + u, u)
        o_copy(u).start()
        return 0

    lax.fori_loop(0, NU, final, 0)
    lax.fori_loop(0, NU, lambda u, _: (o_copy(u).wait(), 0)[1], 0)
    sent = vbuf.at[:, pl.ds(0, 64), pl.ds(0, 128)]
    for k in range(3):
        remote(sent, sent, k, rp_sem.at[0], dev1).wait_send()
    sent = vbuf.at[:, :, pl.ds(0, 128)]
    remote(sent, sent, 3, rp_sem.at[0], devp).wait_send()


def solution(mesh):
    def local_apply(v_loc, t_loc, z_loc):
        dma = pltpu.SemaphoreType.DMA
        out = pl.pallas_call(
            kernel,
            out_shape=jax.ShapeDtypeStruct((4, NU, 64, 512), F32),
            in_specs=[pl.BlockSpec(memory_space=pl.ANY)] * 3,
            out_specs=pl.BlockSpec(memory_space=pl.ANY),
            scratch_shapes=[
                pltpu.VMEM((NCH, 256, 256), F32),
                pltpu.VMEM((NU, 4, 64, 512), F32),
                pltpu.VMEM((2, NU, 2, 64, 64), F32),
                pltpu.VMEM((3, 256, 256), BF16),
                pltpu.VMEM((3, 256, 256), BF16),
                pltpu.VMEM((3, 256, 256), BF16),
                pltpu.VMEM((3, 256, 512), BF16),
                pltpu.VMEM((3, 256, 512), BF16),
                pltpu.VMEM((3, 256, 512), BF16),
                pltpu.VMEM((256, 512), F32),
                pltpu.VMEM((256, 256), F32),
                pltpu.VMEM((256, 256), F32),
                pltpu.VMEM((256, 256), F32),
                dma((NP,)), dma((NP,)), dma((NP,)),
                dma((4,)), dma((NU,)), dma((3,)), dma((NU,)),
            ],
            compiler_params=pltpu.CompilerParams(
                collective_id=0, has_side_effects=True, vmem_limit_bytes=67_043_328
            ),
            cost_estimate=pl.CostEstimate(flops=116_000_000_000, bytes_accessed=60_000_000, transcendentals=0),
        )(v_loc.reshape(NU, 64, 2048), t_loc.reshape(NU, 2, 64, 64), z_loc.reshape(4, NU, 64, 512))
        return out.reshape(4096, 512)

    return jax.shard_map(
        local_apply,
        mesh=mesh,
        in_specs=(P("row", "col"), P("col", None, None), P(None, ("row", "col"))),
        out_specs=P(None, ("row", "col")),
        check_vma=False,
    )
```

```python
import functools

import jax
import jax.numpy as jnp
from jax import lax
from jax.experimental import pallas as pl
from jax.experimental.pallas import tpu as pltpu
from jax.sharding import PartitionSpec as P

MESH = pl.DeviceIdType.MESH
F32 = jnp.float32
BF16 = jnp.bfloat16

NU = 16
NCH = NU * (NU + 1) // 2
NP = NCH // 2
LEAD, GROW, LEAD_MAX = (5, 3, 1), (4, 2, 8), (9, 5, 1)
ZAHEAD = 4
LAST = 2


def split3(x):
    h = x.astype(BF16)
    rem = x - h.astype(F32)
    m = rem.astype(BF16)
    l = (rem - m.astype(F32)).astype(BF16)
    return h, m, l


def dot(a, b):
    return jnp.dot(a, b, preferred_element_type=F32)


def mm6(a, b):
    ah, am, al = a
    bh, bm, bl = b
    return (dot(al, bh) + dot(ah, bl) + dot(am, bm)) + (dot(am, bh) + dot(ah, bm)) + dot(ah, bh)


def mm_f32(a, b):
    return mm6(split3(a), split3(b))


def mm_k128(a, b):
    ah, am, al = split3(a)
    bh, bm, bl = split3(b)

    def part(a0, a1, b0, b1):
        return dot(jnp.concatenate([a0, a1], axis=1), jnp.concatenate([b0, b1], axis=0))

    return (part(am, ah, bm, bl) + part(al, ah, bh, bm)) + part(am, ah, bh, bh)


def kernel(
    v_hbm, d_hbm, z_hbm, x_hbm, v0_hbm, y_hbm,
    vbuf, xbuf, dbuf, vt3, vt3b, vn3, x3, x3b, y3, wacc, s1acc, s2acc, tmat,
    r1_sem, r2_sem, rp_sem, send_sem, z_sem, d_sem, o_sem,
):
    r = lax.axis_index("row")
    q = lax.axis_index("col")
    ry, rx = r // 2, r % 2
    row_x = ry * 2 + (1 - rx)
    row_y = (1 - ry) * 2 + rx
    n1 = row_x * (1 - q) + row_y * q
    n2 = row_y * (1 - q) + row_x * q
    dev1, dev2, devp = (n1, q), (n2, q), (r, 1 - q)
    cols = pl.ds(pl.multiple_of(q * 128, 128), 128)

    def piece(c, n, rr):
        return vbuf.at[pl.ds(c, n), pl.ds(pl.multiple_of(rr * 64, 64), 64), cols]

    def remote(src, dst, k, rsem, dev):
        return pltpu.make_async_remote_copy(
            src_ref=src, dst_ref=dst, send_sem=send_sem.at[k], recv_sem=rsem,
            device_id=dev, device_id_type=MESH,
        )

    def stage0(p, c, s, u):
        src = v_hbm.at[pl.ds(u, 1), :, pl.ds(pl.multiple_of(s * 128, 128), 128)]
        dst = piece(c, 1, r)
        remote(src, dst, 0, r1_sem.at[p], dev1).start()
        remote(src, dst, 1, r2_sem.at[p], dev2).start()
        pltpu.make_async_copy(src, dst, r2_sem.at[p]).start()

    def stage1(p):
        x = piece(2 * p, 2, n1)
        remote(x, x, 0, r1_sem.at[p], dev1).wait_recv()
        remote(x, x, 2, r2_sem.at[p], dev2).start()

    def stage2(p):
        x = vbuf.at[pl.ds(2 * p, 2), pl.ds(0, 192), cols]
        remote(x, x, 1, r2_sem.at[p], dev2).wait_recv()
        x = vbuf.at[pl.ds(2 * p, 2), :, cols]
        remote(x, x, 3, rp_sem.at[p], devp).start()

    def stage3(p):
        x = vbuf.at[pl.ds(2 * p, 2), :, pl.ds(pl.multiple_of((1 - q) * 128, 128), 128)]
        remote(x, x, 3, rp_sem.at[p], devp).wait_recv()

    def target(i, p):
        ahead = jnp.minimum(LEAD[i] + p * GROW[i] // 16, LEAD_MAX[i])
        return jnp.minimum(p + ahead, NP)

    def run0(lo, hi, su):
        def body(p, su):
            s, u = su
            for i in range(2):
                stage0(p, 2 * p + i, s, u)
                last = u == NU - 1
                s2 = jnp.where(last, jnp.maximum(s - 1, 0), s)
                s, u = s2, jnp.where(last, s2, u + 1)
            return s, u

        return lax.fori_loop(lo, hi, body, su)

    def run(i, lo, hi):
        def body(n, _):
            (None, stage1, stage2)[i](n)
            return 0

        lax.fori_loop(lo, hi, body, 0)

    def tick(p, su):
        for i in (1, 2):
            run(i, target(i, p), target(i, p + 1))
        su = run0(target(0, p), target(0, p + 1), su)

        @pl.when(p < NP)
        def _():
            stage3(p)

        return su

    barrier = pltpu.get_barrier_semaphore()
    for dev in (dev1, dev2, devp):
        pl.semaphore_signal(barrier, inc=1, device_id=dev, device_id_type=MESH)
    pl.semaphore_wait(barrier, 3)

    d_own = dbuf.at[q]
    d_send = pltpu.make_async_remote_copy(
        src_ref=d_hbm, dst_ref=d_own, send_sem=d_sem.at[0], recv_sem=d_sem.at[1],
        device_id=devp, device_id_type=MESH,
    )
    d_send.start()
    d_loc = pltpu.make_async_copy(d_hbm, d_own, d_sem.at[2])
    d_loc.start()

    def z_copy(u):
        return pltpu.make_async_copy(z_hbm.at[:, u], xbuf.at[u], z_sem.at[u])

    for i in range(ZAHEAD):
        z_copy(NU - 1 - i).start()
    carry = run0(0, target(0, 0), (jnp.int32(NU - 1), jnp.int32(NU - 1)))
    for i in (1, 2):
        run(i, 0, target(i, 0))
    d_send.wait()
    d_loc.wait()

    def store3(ref, x):
        ref[0], ref[1], ref[2] = split3(x)

    def load3(ref):
        return ref[0], ref[1], ref[2]

    def do_a(vt, x):
        return mm6(load3(vt), load3(x))

    def do_c(c, u):
        x = xbuf[u].reshape(256, 512) - mm6(split3(vbuf[c]), load3(y3))
        xbuf[u] = x.reshape(4, 64, 512)
        return x

    def do_g(c, vt):
        v = vbuf[c]
        store3(vn3, v)
        store3(vt, v.T)
        g1 = dot(vt[1, :192], vn3[1]) + dot(vt[0, :192], vn3[0])
        g2 = dot(vt[0], vn3[2]) + dot(vt[0], vn3[1])
        return g1, g2

    low = lax.broadcasted_iota(jnp.int32, (64, 128), 1) < 64

    def roll(x):
        return pltpu.roll(x, 64, 1)

    def diag(s, i):
        zero = jnp.zeros((64, 64), F32)
        return jnp.concatenate(
            [
                jnp.concatenate([dbuf[0, s, i], zero], axis=1),
                jnp.concatenate([zero, dbuf[1, s, i]], axis=1),
            ],
            axis=0,
        )

    def merge_1(s, s1, s2):
        g = s1 + s2[:192] + s2.T[:192]
        zero = jnp.zeros((64, 128), F32)
        d01, d23 = diag(s, 0), diag(s, 1)
        u01 = jnp.concatenate([jnp.where(low, 0.0, roll(g[:64, 128:])), zero], axis=0)
        u23 = jnp.concatenate([jnp.where(low, 0.0, g[64:128, 128:]), zero], axis=0)
        u2 = jnp.concatenate(
            [
                jnp.where(low, roll(g[:64, :128]), g[:64, 128:]),
                jnp.where(low, roll(g[128:192, :128]), g[128:192, 128:]),
            ],
            axis=0,
        )
        nm = mm_k128(d01, jnp.concatenate([u01, u2], axis=1))
        z = mm_k128(u23, d23)
        return nm, z

    def merge_2(s, nm, z):
        d01, d23 = diag(s, 0), diag(s, 1)
        el = mm_k128(nm[:, :128], jnp.concatenate([d01, nm[:, 128:]], axis=1))
        t23 = d23 - mm_k128(d23, z)
        return d01 - el[:, :128], nm[:, 128:] - el[:, 128:], t23

    def merge_3(t01, lm, t23):
        f = -mm_k128(lm, t23)
        tmat[0:64, 0:128] = jnp.where(low, t01[:64], roll(f[:64]))
        tmat[0:64, 128:256] = jnp.where(low, roll(t01[:64]), f[:64])
        tmat[64:128, 0:128] = jnp.where(low, 0.0, roll(t23[:64]))
        tmat[64:128, 128:256] = jnp.where(low, 0.0, t23[:64])
        tmat[128:192, 0:128] = jnp.where(low, 0.0, roll(f[64:]))
        tmat[128:192, 128:256] = jnp.where(low, roll(t01[64:]), f[64:])
        tmat[192:256, 0:128] = jnp.zeros((64, 128), F32)
        tmat[192:256, 128:256] = t23[64:]

    def offset(s):
        return (NU - 1 - s) * (NU - s) // 2

    carry = tick(0, carry)
    z_copy(NU - 1).wait()
    wacc[...] = jnp.zeros_like(wacc)
    s1acc[...], s2acc[...] = do_g(0, vt3)
    store3(x3, xbuf[NU - 1].reshape(256, 512))

    def step(c_a, c_c, u):
        wacc[...] += do_a(vt3, x3)
        x = do_c(c_c, u)
        g1, g2 = do_g(c_a + 1, vt3)
        s1acc[...] += g1
        s2acc[...] += g2
        store3(x3, x)

    def first_g(c):
        s1acc[...], s2acc[...] = do_g(jnp.minimum(c, NCH - 1), vt3)

    def finish(sa, w):
        store3(x3, xbuf[jnp.maximum(sa - 1, 0)].reshape(256, 512))
        store3(y3, mm_f32(tmat[...], w))
        wacc[...] = jnp.zeros_like(wacc)

    def next_z(sa):
        @pl.when(sa >= ZAHEAD)
        def _():
            z_copy(sa - ZAHEAD).start()

        @pl.when(sa >= 1)
        def _():
            z_copy(sa - 1).wait()

    next_z(NU - 1)
    vt3b[...] = vt3[...]
    x3b[...] = x3[...]
    merge_3(*merge_2(NU - 1, *merge_1(NU - 1, s1acc[...], s2acc[...])))
    first_g(1)
    finish(NU - 1, do_a(vt3b, x3b))

    def x_copy(u):
        return pltpu.make_async_copy(xbuf.at[u], x_hbm.at[:, u], o_sem.at[u])

    def v_copy(u):
        return pltpu.make_async_copy(vbuf.at[NCH - NU + u], v0_hbm.at[u], o_sem.at[NU + u])

    def write_out(sa, lo, n):
        @pl.when(sa == 0)
        def _():
            for u in range(n):
                x_copy(lo + u).start()
                v_copy(lo + u).start()

    def outer(k, carry):
        s = NU - k
        sa = s - 1
        off_a = offset(sa)
        off_c = off_a - k

        def step1(u, carry):
            i = u - s
            c = off_a + i + 1
            carry = lax.cond(c % 2 == 0, lambda su: tick(c // 2, su), lambda su: su, carry)
            step(off_a + i, off_c + i, u)
            write_out(sa, u - 1, 1)
            return carry

        def step2(j, carry):
            i = 2 * j
            carry = tick((off_a + i + 2) // 2, carry)
            step(off_a + i, off_c + i, s + i)
            step(off_a + i + 1, off_c + i + 1, s + i + 1)
            write_out(sa, s + i - 1, 2)
            return carry

        pairs = (k - 1) // 2
        carry = lax.fori_loop(0, pairs, step2, carry)
        carry = lax.fori_loop(s + 2 * pairs, NU - 1, step1, carry)

        carry = tick((off_a + k + 1) // 2, carry)
        next_z(sa)
        write_out(sa, NU - 2, 1)

        @pl.when(sa == 0)
        def _():
            v_copy(NU - 1).start()

        store3(x3b, do_c(off_c + k - 1, NU - 1))
        g1, g2 = do_g(off_a + k, vt3b)
        w = wacc[...] + do_a(vt3, x3)
        part = merge_1(sa, s1acc[...] + g1, s2acc[...] + g2)
        w = w + do_a(vt3b, x3b)
        part = merge_2(sa, *part)
        first_g(off_a + k + 1)
        merge_3(*part)
        finish(sa, w)
        return carry

    lax.fori_loop(1, NU, outer, carry)

    y_copy = pltpu.make_async_copy(y3, y_hbm, o_sem.at[2 * NU])
    y_copy.start()
    x_copy(NU - 1).start()
    lax.fori_loop(0, NU, lambda u, _: (x_copy(u).wait(), v_copy(u).wait(), 0)[2], 0)
    y_copy.wait()
    sent = vbuf.at[:, pl.ds(0, 64), pl.ds(0, 128)]
    for k in range(3):
        remote(sent, sent, k, rp_sem.at[0], dev1).wait_send()
    sent = vbuf.at[:, :, pl.ds(0, 128)]
    remote(sent, sent, 3, rp_sem.at[0], devp).wait_send()


def last_update(x_ref, v_ref, y_ref, out_ref):
    for i in range(LAST):
        upd = mm6(split3(v_ref[i]), (y_ref[0], y_ref[1], y_ref[2]))
        out_ref[:, i] = x_ref[:, i] - upd.reshape(4, 64, 512)


def solution(mesh):
    def local_apply(v_loc, t_loc, z_loc):
        dma = pltpu.SemaphoreType.DMA
        x, v0, y = pl.pallas_call(
            kernel,
            out_shape=(
                jax.ShapeDtypeStruct((4, NU, 64, 512), F32),
                jax.ShapeDtypeStruct((NU, 256, 256), F32),
                jax.ShapeDtypeStruct((3, 256, 512), BF16),
            ),
            in_specs=[pl.BlockSpec(memory_space=pl.ANY)] * 3,
            out_specs=(pl.BlockSpec(memory_space=pl.ANY),) * 3,
            scratch_shapes=[
                pltpu.VMEM((NCH, 256, 256), F32),
                pltpu.VMEM((NU, 4, 64, 512), F32),
                pltpu.VMEM((2, NU, 2, 64, 64), F32),
                pltpu.VMEM((3, 256, 256), BF16),
                pltpu.VMEM((3, 256, 256), BF16),
                pltpu.VMEM((3, 256, 256), BF16),
                pltpu.VMEM((3, 256, 512), BF16),
                pltpu.VMEM((3, 256, 512), BF16),
                pltpu.VMEM((3, 256, 512), BF16),
                pltpu.VMEM((256, 512), F32),
                pltpu.VMEM((192, 256), F32),
                pltpu.VMEM((256, 256), F32),
                pltpu.VMEM((256, 256), F32),
                dma((NP,)), dma((NP,)), dma((NP,)),
                dma((4,)), dma((NU,)), dma((3,)), dma((2 * NU + 1,)),
            ],
            compiler_params=pltpu.CompilerParams(
                collective_id=0, has_side_effects=True, vmem_limit_bytes=67_043_328
            ),
            cost_estimate=pl.CostEstimate(flops=116_000_000_000, bytes_accessed=60_000_000, transcendentals=0),
        )(v_loc.reshape(NU, 64, 2048), t_loc.reshape(NU, 2, 64, 64), z_loc.reshape(4, NU, 64, 512))
        x_spec = pl.BlockSpec((4, LAST, 64, 512), lambda i: (0, i, 0, 0))
        out = pl.pallas_call(
            last_update,
            out_shape=jax.ShapeDtypeStruct((4, NU, 64, 512), F32),
            grid=(NU // LAST,),
            in_specs=[
                x_spec,
                pl.BlockSpec((LAST, 256, 256), lambda i: (i, 0, 0)),
                pl.BlockSpec((3, 256, 512), lambda i: (0, 0, 0)),
            ],
            out_specs=x_spec,
            compiler_params=pltpu.CompilerParams(
                dimension_semantics=("arbitrary",), vmem_limit_bytes=67_043_328
            ),
            cost_estimate=pl.CostEstimate(flops=6_500_000_000, bytes_accessed=22_000_000, transcendentals=0),
        )(x, v0, y)
        return out.reshape(4096, 512)

    return jax.shard_map(
        local_apply,
        mesh=mesh,
        in_specs=(P("row", "col"), P("col", None, None), P(None, ("row", "col"))),
        out_specs=P(None, ("row", "col")),
        check_vma=False,
    )
```

```python
import functools

import jax
import jax.numpy as jnp
from jax import lax
from jax.experimental import pallas as pl
from jax.experimental.pallas import tpu as pltpu
from jax.sharding import PartitionSpec as P

MESH = pl.DeviceIdType.MESH
F32 = jnp.float32
BF16 = jnp.bfloat16

NU = 16
NCH = NU * (NU + 1) // 2
NP = NCH // 2
LEAD = (7, 4, 1)
ZAHEAD = 4
LAST = 2


def split3(x):
    h = x.astype(BF16)
    rem = x - h.astype(F32)
    m = rem.astype(BF16)
    l = (rem - m.astype(F32)).astype(BF16)
    return h, m, l


def dot(a, b):
    return jnp.dot(a, b, preferred_element_type=F32)


def mm6(a, b):
    ah, am, al = a
    bh, bm, bl = b
    return (dot(al, bh) + dot(ah, bl) + dot(am, bm)) + (dot(am, bh) + dot(ah, bm)) + dot(ah, bh)


def mm_f32(a, b):
    return mm6(split3(a), split3(b))


def mm_k128(a, b):
    ah, am, al = split3(a)
    bh, bm, bl = split3(b)

    def part(a0, a1, b0, b1):
        return dot(jnp.concatenate([a0, a1], axis=1), jnp.concatenate([b0, b1], axis=0))

    return (part(am, ah, bm, bl) + part(al, ah, bh, bm)) + part(am, ah, bh, bh)


def kernel(
    v_hbm, d_hbm, z_hbm, x_hbm, v0_hbm, y_hbm,
    vbuf, xbuf, dbuf, vt3, vt3b, vn3, x3, x3b, y3, wacc, s1acc, s2acc, tmat,
    r1_sem, r2_sem, rp_sem, send_sem, z_sem, d_sem, o_sem,
):
    r = lax.axis_index("row")
    q = lax.axis_index("col")
    ry, rx = r // 2, r % 2
    row_x = ry * 2 + (1 - rx)
    row_y = (1 - ry) * 2 + rx
    n1 = row_x * (1 - q) + row_y * q
    n2 = row_y * (1 - q) + row_x * q
    dev1, dev2, devp = (n1, q), (n2, q), (r, 1 - q)
    cols = pl.ds(pl.multiple_of(q * 128, 128), 128)

    def piece(c, n, rr):
        return vbuf.at[pl.ds(c, n), pl.ds(pl.multiple_of(rr * 64, 64), 64), cols]

    def remote(src, dst, k, rsem, dev):
        return pltpu.make_async_remote_copy(
            src_ref=src, dst_ref=dst, send_sem=send_sem.at[k], recv_sem=rsem,
            device_id=dev, device_id_type=MESH,
        )

    def stage0(p, c, s, u):
        src = v_hbm.at[pl.ds(u, 1), :, pl.ds(pl.multiple_of(s * 128, 128), 128)]
        dst = piece(c, 1, r)
        remote(src, dst, 0, r1_sem.at[p], dev1).start()
        remote(src, dst, 1, r2_sem.at[p], dev2).start()
        pltpu.make_async_copy(src, dst, r2_sem.at[p]).start()

    def stage1(p):
        x = piece(2 * p, 2, n1)
        remote(x, x, 0, r1_sem.at[p], dev1).wait_recv()
        remote(x, x, 2, r2_sem.at[p], dev2).start()

    def stage2(p):
        x = vbuf.at[pl.ds(2 * p, 2), pl.ds(0, 192), cols]
        remote(x, x, 1, r2_sem.at[p], dev2).wait_recv()
        x = vbuf.at[pl.ds(2 * p, 2), :, cols]
        remote(x, x, 3, rp_sem.at[p], devp).start()

    def stage3(p):
        x = vbuf.at[pl.ds(2 * p, 2), :, pl.ds(pl.multiple_of((1 - q) * 128, 128), 128)]
        remote(x, x, 3, rp_sem.at[p], devp).wait_recv()

    def send_own(p, su):
        s, u = su
        for i in range(2):

            @pl.when(p < NP)
            def _():
                stage0(p, 2 * p + i, s, u)

            last = u == NU - 1
            s2 = jnp.where(last, jnp.maximum(s - 1, 0), s)
            s, u = s2, jnp.where(last, s2, u + 1)
        return s, u

    def tick(p, su):
        @pl.when(p + LEAD[1] < NP)
        def _():
            stage1(p + LEAD[1])

        @pl.when(p + LEAD[2] < NP)
        def _():
            stage2(p + LEAD[2])

        @pl.when(p < NP)
        def _():
            stage3(p)

        return send_own(p + LEAD[0], su)

    barrier = pltpu.get_barrier_semaphore()
    for dev in (dev1, dev2, devp):
        pl.semaphore_signal(barrier, inc=1, device_id=dev, device_id_type=MESH)
    pl.semaphore_wait(barrier, 3)

    d_own = dbuf.at[q]
    d_send = pltpu.make_async_remote_copy(
        src_ref=d_hbm, dst_ref=d_own, send_sem=d_sem.at[0], recv_sem=d_sem.at[1],
        device_id=devp, device_id_type=MESH,
    )
    d_send.start()
    d_loc = pltpu.make_async_copy(d_hbm, d_own, d_sem.at[2])
    d_loc.start()

    def z_copy(u):
        return pltpu.make_async_copy(z_hbm.at[:, u], xbuf.at[u], z_sem.at[u])

    for i in range(ZAHEAD):
        z_copy(NU - 1 - i).start()
    carry = lax.fori_loop(0, LEAD[0], send_own, (jnp.int32(NU - 1), jnp.int32(NU - 1)))
    lax.fori_loop(0, LEAD[1], lambda p, _: (stage1(p), 0)[1], 0)
    lax.fori_loop(0, LEAD[2], lambda p, _: (stage2(p), 0)[1], 0)
    d_send.wait()
    d_loc.wait()

    def store3(ref, x):
        ref[0], ref[1], ref[2] = split3(x)

    def load3(ref):
        return ref[0], ref[1], ref[2]

    def do_a(vt, x):
        return mm6(load3(vt), load3(x))

    def do_c(c, u):
        x = xbuf[u].reshape(256, 512) - mm6(split3(vbuf[c]), load3(y3))
        xbuf[u] = x.reshape(4, 64, 512)
        return x

    def do_g(c, vt):
        v = vbuf[c]
        store3(vn3, v)
        store3(vt, v.T)
        g1 = dot(vt[1, :192], vn3[1]) + dot(vt[0, :192], vn3[0])
        g2 = dot(vt[0], vn3[2]) + dot(vt[0], vn3[1])
        return g1, g2

    low = lax.broadcasted_iota(jnp.int32, (64, 128), 1) < 64

    def roll(x):
        return pltpu.roll(x, 64, 1)

    def diag(s, i):
        zero = jnp.zeros((64, 64), F32)
        return jnp.concatenate(
            [
                jnp.concatenate([dbuf[0, s, i], zero], axis=1),
                jnp.concatenate([zero, dbuf[1, s, i]], axis=1),
            ],
            axis=0,
        )

    def merge_1(s, s1, s2):
        g = s1 + s2[:192] + s2.T[:192]
        zero = jnp.zeros((64, 128), F32)
        d01, d23 = diag(s, 0), diag(s, 1)
        u01 = jnp.concatenate([jnp.where(low, 0.0, roll(g[:64, 128:])), zero], axis=0)
        u23 = jnp.concatenate([jnp.where(low, 0.0, g[64:128, 128:]), zero], axis=0)
        u2 = jnp.concatenate(
            [
                jnp.where(low, roll(g[:64, :128]), g[:64, 128:]),
                jnp.where(low, roll(g[128:192, :128]), g[128:192, 128:]),
            ],
            axis=0,
        )
        nm = mm_k128(d01, jnp.concatenate([u01, u2], axis=1))
        z = mm_k128(u23, d23)
        return nm, z

    def merge_2(s, nm, z):
        d01, d23 = diag(s, 0), diag(s, 1)
        el = mm_k128(nm[:, :128], jnp.concatenate([d01, nm[:, 128:]], axis=1))
        t23 = d23 - mm_k128(d23, z)
        return d01 - el[:, :128], nm[:, 128:] - el[:, 128:], t23

    def merge_3(t01, lm, t23):
        f = -mm_k128(lm, t23)
        tmat[0:64, 0:128] = jnp.where(low, t01[:64], roll(f[:64]))
        tmat[0:64, 128:256] = jnp.where(low, roll(t01[:64]), f[:64])
        tmat[64:128, 0:128] = jnp.where(low, 0.0, roll(t23[:64]))
        tmat[64:128, 128:256] = jnp.where(low, 0.0, t23[:64])
        tmat[128:192, 0:128] = jnp.where(low, 0.0, roll(f[64:]))
        tmat[128:192, 128:256] = jnp.where(low, roll(t01[64:]), f[64:])
        tmat[192:256, 0:128] = jnp.zeros((64, 128), F32)
        tmat[192:256, 128:256] = t23[64:]

    def offset(s):
        return (NU - 1 - s) * (NU - s) // 2

    carry = tick(0, carry)
    z_copy(NU - 1).wait()
    wacc[...] = jnp.zeros_like(wacc)
    s1acc[...], s2acc[...] = do_g(0, vt3)
    store3(x3, xbuf[NU - 1].reshape(256, 512))

    def step(c_a, c_c, u):
        wacc[...] += do_a(vt3, x3)
        x = do_c(c_c, u)
        g1, g2 = do_g(c_a + 1, vt3)
        s1acc[...] += g1
        s2acc[...] += g2
        store3(x3, x)

    def first_g(c):
        s1acc[...], s2acc[...] = do_g(jnp.minimum(c, NCH - 1), vt3)

    def finish(sa, w):
        store3(x3, xbuf[jnp.maximum(sa - 1, 0)].reshape(256, 512))
        store3(y3, mm_f32(tmat[...], w))
        wacc[...] = jnp.zeros_like(wacc)

    def next_z(sa):
        @pl.when(sa >= ZAHEAD)
        def _():
            z_copy(sa - ZAHEAD).start()

        @pl.when(sa >= 1)
        def _():
            z_copy(sa - 1).wait()

    next_z(NU - 1)
    vt3b[...] = vt3[...]
    x3b[...] = x3[...]
    merge_3(*merge_2(NU - 1, *merge_1(NU - 1, s1acc[...], s2acc[...])))
    first_g(1)
    finish(NU - 1, do_a(vt3b, x3b))

    def x_copy(u):
        return pltpu.make_async_copy(xbuf.at[u], x_hbm.at[:, u], o_sem.at[u])

    def v_copy(u):
        return pltpu.make_async_copy(vbuf.at[NCH - NU + u], v0_hbm.at[u], o_sem.at[NU + u])

    def write_out(sa, lo, n):
        @pl.when(sa == 0)
        def _():
            for u in range(n):
                x_copy(lo + u).start()
                v_copy(lo + u).start()

    def outer(k, carry):
        s = NU - k
        sa = s - 1
        off_a = offset(sa)
        off_c = off_a - k

        def step1(u, carry):
            i = u - s
            c = off_a + i + 1
            carry = lax.cond(c % 2 == 0, lambda su: tick(c // 2, su), lambda su: su, carry)
            step(off_a + i, off_c + i, u)
            write_out(sa, u - 1, 1)
            return carry

        def step2(j, carry):
            i = 2 * j
            carry = tick((off_a + i + 2) // 2, carry)
            step(off_a + i, off_c + i, s + i)
            step(off_a + i + 1, off_c + i + 1, s + i + 1)
            write_out(sa, s + i - 1, 2)
            return carry

        pairs = (k - 1) // 2
        carry = lax.fori_loop(0, pairs, step2, carry)
        carry = lax.fori_loop(s + 2 * pairs, NU - 1, step1, carry)

        carry = tick((off_a + k + 1) // 2, carry)
        next_z(sa)
        write_out(sa, NU - 2, 1)

        @pl.when(sa == 0)
        def _():
            v_copy(NU - 1).start()

        store3(x3b, do_c(off_c + k - 1, NU - 1))
        g1, g2 = do_g(off_a + k, vt3b)
        w = wacc[...] + do_a(vt3, x3)
        part = merge_1(sa, s1acc[...] + g1, s2acc[...] + g2)
        w = w + do_a(vt3b, x3b)
        part = merge_2(sa, *part)
        first_g(off_a + k + 1)
        merge_3(*part)
        finish(sa, w)
        return carry

    lax.fori_loop(1, NU, outer, carry)

    y_copy = pltpu.make_async_copy(y3, y_hbm, o_sem.at[2 * NU])
    y_copy.start()
    x_copy(NU - 1).start()
    lax.fori_loop(0, NU, lambda u, _: (x_copy(u).wait(), v_copy(u).wait(), 0)[2], 0)
    y_copy.wait()
    sent = vbuf.at[:, pl.ds(0, 64), pl.ds(0, 128)]
    for k in range(3):
        remote(sent, sent, k, rp_sem.at[0], dev1).wait_send()
    sent = vbuf.at[:, :, pl.ds(0, 128)]
    remote(sent, sent, 3, rp_sem.at[0], devp).wait_send()


def last_update(x_hbm, v_hbm, y_hbm, out_hbm, xb, vb, yb, sem):
    def x_in(u):
        return pltpu.make_async_copy(x_hbm.at[:, u], xb.at[u], sem.at[u])

    def v_in(u):
        return pltpu.make_async_copy(v_hbm.at[u], vb.at[u], sem.at[NU + u])

    def x_out(u):
        return pltpu.make_async_copy(xb.at[u], out_hbm.at[:, u], sem.at[2 * NU + u])

    y_in = pltpu.make_async_copy(y_hbm, yb, sem.at[3 * NU])
    y_in.start()
    lax.fori_loop(0, NU, lambda u, _: (v_in(u).start(), x_in(u).start(), 0)[2], 0)
    y_in.wait()

    def body(j, _):
        for i in range(LAST):
            x_in(LAST * j + i).wait()
            v_in(LAST * j + i).wait()
        for i in range(LAST):
            u = LAST * j + i
            upd = mm6(split3(vb[u]), (yb[0], yb[1], yb[2]))
            xb[u] = xb[u] - upd.reshape(4, 64, 512)
        for i in range(LAST):
            x_out(LAST * j + i).start()
        return 0

    lax.fori_loop(0, NU // LAST, body, 0)
    lax.fori_loop(0, NU, lambda u, _: (x_out(u).wait(), 0)[1], 0)


def solution(mesh):
    def local_apply(v_loc, t_loc, z_loc):
        dma = pltpu.SemaphoreType.DMA
        x, v0, y = pl.pallas_call(
            kernel,
            out_shape=(
                jax.ShapeDtypeStruct((4, NU, 64, 512), F32),
                jax.ShapeDtypeStruct((NU, 256, 256), F32),
                jax.ShapeDtypeStruct((3, 256, 512), BF16),
            ),
            in_specs=[pl.BlockSpec(memory_space=pl.ANY)] * 3,
            out_specs=(pl.BlockSpec(memory_space=pl.ANY),) * 3,
            scratch_shapes=[
                pltpu.VMEM((NCH, 256, 256), F32),
                pltpu.VMEM((NU, 4, 64, 512), F32),
                pltpu.VMEM((2, NU, 2, 64, 64), F32),
                pltpu.VMEM((3, 256, 256), BF16),
                pltpu.VMEM((3, 256, 256), BF16),
                pltpu.VMEM((3, 256, 256), BF16),
                pltpu.VMEM((3, 256, 512), BF16),
                pltpu.VMEM((3, 256, 512), BF16),
                pltpu.VMEM((3, 256, 512), BF16),
                pltpu.VMEM((256, 512), F32),
                pltpu.VMEM((192, 256), F32),
                pltpu.VMEM((256, 256), F32),
                pltpu.VMEM((256, 256), F32),
                dma((NP,)), dma((NP,)), dma((NP,)),
                dma((4,)), dma((NU,)), dma((3,)), dma((2 * NU + 1,)),
            ],
            compiler_params=pltpu.CompilerParams(
                collective_id=0, has_side_effects=True, vmem_limit_bytes=67_043_328
            ),
            cost_estimate=pl.CostEstimate(flops=116_000_000_000, bytes_accessed=60_000_000, transcendentals=0),
        )(v_loc.reshape(NU, 64, 2048), t_loc.reshape(NU, 2, 64, 64), z_loc.reshape(4, NU, 64, 512))
        out = pl.pallas_call(
            last_update,
            out_shape=jax.ShapeDtypeStruct((4, NU, 64, 512), F32),
            in_specs=[pl.BlockSpec(memory_space=pl.ANY)] * 3,
            out_specs=pl.BlockSpec(memory_space=pl.ANY),
            scratch_shapes=[
                pltpu.VMEM((NU, 4, 64, 512), F32),
                pltpu.VMEM((NU, 256, 256), F32),
                pltpu.VMEM((3, 256, 512), BF16),
                dma((3 * NU + 1,)),
            ],
            compiler_params=pltpu.CompilerParams(vmem_limit_bytes=67_043_328),
            cost_estimate=pl.CostEstimate(flops=6_500_000_000, bytes_accessed=22_000_000, transcendentals=0),
        )(x, v0, y)
        return out.reshape(4096, 512)

    return jax.shard_map(
        local_apply,
        mesh=mesh,
        in_specs=(P("row", "col"), P("col", None, None), P(None, ("row", "col"))),
        out_specs=P(None, ("row", "col")),
        check_vma=False,
    )
```

```python
import functools

import jax
import jax.numpy as jnp
from jax import lax
from jax.experimental import pallas as pl
from jax.experimental.pallas import tpu as pltpu
from jax.sharding import PartitionSpec as P

MESH = pl.DeviceIdType.MESH
F32 = jnp.float32
BF16 = jnp.bfloat16

NU = 16
NCH = NU * (NU + 1) // 2
NP = NCH // 2
LEAD = (7, 4, 1)
PROLOGUE = (0, 0, 0, 0, 1, 0, 1, 1, 0, 0, 1, 0, 2, 2), (1,)
ZAHEAD = 4
LAST = 2


def split3(x):
    h = x.astype(BF16)
    rem = x - h.astype(F32)
    m = rem.astype(BF16)
    l = (rem - m.astype(F32)).astype(BF16)
    return h, m, l


def dot(a, b):
    return jnp.dot(a, b, preferred_element_type=F32)


def mm6(a, b):
    ah, am, al = a
    bh, bm, bl = b
    return (dot(al, bh) + dot(ah, bl) + dot(am, bm)) + (dot(am, bh) + dot(ah, bm)) + dot(ah, bh)


def mm_f32(a, b):
    return mm6(split3(a), split3(b))


def mm_k128(a, b):
    ah, am, al = split3(a)
    bh, bm, bl = split3(b)

    def part(a0, a1, b0, b1):
        return dot(jnp.concatenate([a0, a1], axis=1), jnp.concatenate([b0, b1], axis=0))

    return (part(am, ah, bm, bl) + part(al, ah, bh, bm)) + part(am, ah, bh, bh)


def kernel(
    v_hbm, d_hbm, z_hbm, x_hbm, v0_hbm, y_hbm,
    vbuf, xbuf, dbuf, vt3, vt3b, vn3, x3, x3b, y3, wacc, s1acc, s2acc, tmat,
    r1_sem, r2_sem, rp_sem, send_sem, z_sem, d_sem, o_sem,
):
    r = lax.axis_index("row")
    q = lax.axis_index("col")
    ry, rx = r // 2, r % 2
    row_x = ry * 2 + (1 - rx)
    row_y = (1 - ry) * 2 + rx
    n1 = row_x * (1 - q) + row_y * q
    n2 = row_y * (1 - q) + row_x * q
    dev1, dev2, devp = (n1, q), (n2, q), (r, 1 - q)
    cols = pl.ds(pl.multiple_of(q * 128, 128), 128)

    def piece(c, n, rr):
        return vbuf.at[pl.ds(c, n), pl.ds(pl.multiple_of(rr * 64, 64), 64), cols]

    def remote(src, dst, k, rsem, dev):
        return pltpu.make_async_remote_copy(
            src_ref=src, dst_ref=dst, send_sem=send_sem.at[k], recv_sem=rsem,
            device_id=dev, device_id_type=MESH,
        )

    def stage0(p, c, s, u):
        src = v_hbm.at[pl.ds(u, 1), :, pl.ds(pl.multiple_of(s * 128, 128), 128)]
        dst = piece(c, 1, r)
        remote(src, dst, 0, r1_sem.at[p], dev1).start()
        remote(src, dst, 1, r2_sem.at[p], dev2).start()
        pltpu.make_async_copy(src, dst, r2_sem.at[p]).start()

    def stage1(p):
        x = piece(2 * p, 2, n1)
        remote(x, x, 0, r1_sem.at[p], dev1).wait_recv()
        remote(x, x, 2, r2_sem.at[p], dev2).start()

    def stage2(p):
        x = vbuf.at[pl.ds(2 * p, 2), pl.ds(0, 192), cols]
        remote(x, x, 1, r2_sem.at[p], dev2).wait_recv()
        x = vbuf.at[pl.ds(2 * p, 2), :, cols]
        remote(x, x, 3, rp_sem.at[p], devp).start()

    def stage3(p):
        x = vbuf.at[pl.ds(2 * p, 2), :, pl.ds(pl.multiple_of((1 - q) * 128, 128), 128)]
        remote(x, x, 3, rp_sem.at[p], devp).wait_recv()

    def send_own(p, su):
        s, u = su
        for i in range(2):

            @pl.when(p < NP)
            def _():
                stage0(p, 2 * p + i, s, u)

            last = u == NU - 1
            s2 = jnp.where(last, jnp.maximum(s - 1, 0), s)
            s, u = s2, jnp.where(last, s2, u + 1)
        return s, u

    def tick(p):
        @pl.when(p + LEAD[1] < NP)
        def _():
            stage1(p + LEAD[1])

        @pl.when(p + LEAD[2] < NP)
        def _():
            stage2(p + LEAD[2])

        @pl.when(p < NP)
        def _():
            stage3(p)

    barrier = pltpu.get_barrier_semaphore()
    for dev in (dev1, dev2, devp):
        pl.semaphore_signal(barrier, inc=1, device_id=dev, device_id_type=MESH)
    pl.semaphore_wait(barrier, 3)

    d_own = dbuf.at[q]
    d_send = pltpu.make_async_remote_copy(
        src_ref=d_hbm, dst_ref=d_own, send_sem=d_sem.at[0], recv_sem=d_sem.at[1],
        device_id=devp, device_id_type=MESH,
    )
    d_send.start()
    d_loc = pltpu.make_async_copy(d_hbm, d_own, d_sem.at[2])
    d_loc.start()

    def z_copy(u):
        return pltpu.make_async_copy(z_hbm.at[:, u], xbuf.at[u], z_sem.at[u])

    for i in range(ZAHEAD):
        z_copy(NU - 1 - i).start()
    chunks = [(s, u) for s in range(NU - 1, -1, -1) for u in range(s, NU)]
    done = [0, 0, 0]

    def prologue(stages):
        for i in stages:
            p = done[i]
            done[i] += 1
            if i == 0:
                stage0(p, 2 * p, *chunks[2 * p])
                stage0(p, 2 * p + 1, *chunks[2 * p + 1])
            else:
                (stage1 if i == 1 else stage2)(p)

    prologue(PROLOGUE[0])
    d_send.wait()
    d_loc.wait()

    def store3(ref, x):
        ref[0], ref[1], ref[2] = split3(x)

    def load3(ref):
        return ref[0], ref[1], ref[2]

    def do_a(vt, x):
        return mm6(load3(vt), load3(x))

    def do_c(c, u):
        x = xbuf[u].reshape(256, 512) - mm6(split3(vbuf[c]), load3(y3))
        xbuf[u] = x.reshape(4, 64, 512)
        return x

    def do_g(c, vt):
        v = vbuf[c]
        store3(vn3, v)
        store3(vt, v.T)
        g1 = dot(vt[1, :192], vn3[1]) + dot(vt[0, :192], vn3[0])
        g2 = dot(vt[0], vn3[2]) + dot(vt[0], vn3[1])
        return g1, g2

    low = lax.broadcasted_iota(jnp.int32, (64, 128), 1) < 64

    def roll(x):
        return pltpu.roll(x, 64, 1)

    def diag(s, i):
        zero = jnp.zeros((64, 64), F32)
        return jnp.concatenate(
            [
                jnp.concatenate([dbuf[0, s, i], zero], axis=1),
                jnp.concatenate([zero, dbuf[1, s, i]], axis=1),
            ],
            axis=0,
        )

    def merge_1(s, s1, s2):
        g = s1 + s2[:192] + s2.T[:192]
        zero = jnp.zeros((64, 128), F32)
        d01, d23 = diag(s, 0), diag(s, 1)
        u01 = jnp.concatenate([jnp.where(low, 0.0, roll(g[:64, 128:])), zero], axis=0)
        u23 = jnp.concatenate([jnp.where(low, 0.0, g[64:128, 128:]), zero], axis=0)
        u2 = jnp.concatenate(
            [
                jnp.where(low, roll(g[:64, :128]), g[:64, 128:]),
                jnp.where(low, roll(g[128:192, :128]), g[128:192, 128:]),
            ],
            axis=0,
        )
        nm = mm_k128(d01, jnp.concatenate([u01, u2], axis=1))
        z = mm_k128(u23, d23)
        return nm, z

    def merge_2(s, nm, z):
        d01, d23 = diag(s, 0), diag(s, 1)
        el = mm_k128(nm[:, :128], jnp.concatenate([d01, nm[:, 128:]], axis=1))
        t23 = d23 - mm_k128(d23, z)
        return d01 - el[:, :128], nm[:, 128:] - el[:, 128:], t23

    def merge_3(t01, lm, t23):
        f = -mm_k128(lm, t23)
        tmat[0:64, 0:128] = jnp.where(low, t01[:64], roll(f[:64]))
        tmat[0:64, 128:256] = jnp.where(low, roll(t01[:64]), f[:64])
        tmat[64:128, 0:128] = jnp.where(low, 0.0, roll(t23[:64]))
        tmat[64:128, 128:256] = jnp.where(low, 0.0, t23[:64])
        tmat[128:192, 0:128] = jnp.where(low, 0.0, roll(f[64:]))
        tmat[128:192, 128:256] = jnp.where(low, roll(t01[64:]), f[64:])
        tmat[192:256, 0:128] = jnp.zeros((64, 128), F32)
        tmat[192:256, 128:256] = t23[64:]

    def offset(s):
        return (NU - 1 - s) * (NU - s) // 2

    stage3(0)
    z_copy(NU - 1).wait()
    wacc[...] = jnp.zeros_like(wacc)
    s1acc[...], s2acc[...] = do_g(0, vt3)
    store3(x3, xbuf[NU - 1].reshape(256, 512))

    def step(c_a, c_c, u):
        wacc[...] += do_a(vt3, x3)
        x = do_c(c_c, u)
        g1, g2 = do_g(c_a + 1, vt3)
        s1acc[...] += g1
        s2acc[...] += g2
        store3(x3, x)

    def first_g(c):
        s1acc[...], s2acc[...] = do_g(jnp.minimum(c, NCH - 1), vt3)

    def finish(sa, w):
        store3(x3, xbuf[jnp.maximum(sa - 1, 0)].reshape(256, 512))
        store3(y3, mm_f32(tmat[...], w))
        wacc[...] = jnp.zeros_like(wacc)

    def next_z(sa):
        @pl.when(sa >= ZAHEAD)
        def _():
            z_copy(sa - ZAHEAD).start()

        @pl.when(sa >= 1)
        def _():
            z_copy(sa - 1).wait()

    next_z(NU - 1)
    vt3b[...] = vt3[...]
    x3b[...] = x3[...]
    merge_3(*merge_2(NU - 1, *merge_1(NU - 1, s1acc[...], s2acc[...])))
    first_g(1)
    finish(NU - 1, do_a(vt3b, x3b))

    prologue(PROLOGUE[1])
    carry = tuple(jnp.int32(i) for i in chunks[2 * done[0]])

    def x_copy(u):
        return pltpu.make_async_copy(xbuf.at[u], x_hbm.at[:, u], o_sem.at[u])

    def v_copy(u):
        return pltpu.make_async_copy(vbuf.at[NCH - NU + u], v0_hbm.at[u], o_sem.at[NU + u])

    def write_out(sa, lo, n):
        @pl.when(sa == 0)
        def _():
            for u in range(n):
                x_copy(lo + u).start()
                v_copy(lo + u).start()

    def outer(k, carry):
        s = NU - k
        sa = s - 1
        off_a = offset(sa)
        off_c = off_a - k

        def step1(u, carry):
            i = u - s
            c = off_a + i + 1

            def tick_and_send(su):
                tick(c // 2)
                return send_own(c // 2 + LEAD[0], su)

            carry = lax.cond(c % 2 == 0, tick_and_send, lambda su: su, carry)
            step(off_a + i, off_c + i, u)
            write_out(sa, u - 1, 1)
            return carry

        def step2(j, carry):
            i = 2 * j
            p = (off_a + i + 2) // 2
            tick(p)
            carry = send_own(p + LEAD[0], carry)
            step(off_a + i, off_c + i, s + i)
            step(off_a + i + 1, off_c + i + 1, s + i + 1)
            write_out(sa, s + i - 1, 2)
            return carry

        pairs = (k - 1) // 2
        carry = lax.fori_loop(0, pairs, step2, carry)
        carry = lax.fori_loop(s + 2 * pairs, NU - 1, step1, carry)

        p = (off_a + k + 1) // 2
        tick(p)
        carry = send_own(p + LEAD[0], carry)
        next_z(sa)
        write_out(sa, NU - 2, 1)

        @pl.when(sa == 0)
        def _():
            v_copy(NU - 1).start()

        store3(x3b, do_c(off_c + k - 1, NU - 1))
        g1, g2 = do_g(off_a + k, vt3b)
        w = wacc[...] + do_a(vt3, x3)
        part = merge_1(sa, s1acc[...] + g1, s2acc[...] + g2)
        w = w + do_a(vt3b, x3b)
        part = merge_2(sa, *part)
        first_g(off_a + k + 1)
        merge_3(*part)
        finish(sa, w)
        return carry

    lax.fori_loop(1, NU, outer, carry)

    y_copy = pltpu.make_async_copy(y3, y_hbm, o_sem.at[2 * NU])
    y_copy.start()
    x_copy(NU - 1).start()
    lax.fori_loop(0, NU, lambda u, _: (x_copy(u).wait(), v_copy(u).wait(), 0)[2], 0)
    y_copy.wait()
    sent = vbuf.at[:, pl.ds(0, 64), pl.ds(0, 128)]
    for k in range(3):
        remote(sent, sent, k, rp_sem.at[0], dev1).wait_send()
    sent = vbuf.at[:, :, pl.ds(0, 128)]
    remote(sent, sent, 3, rp_sem.at[0], devp).wait_send()


def last_update(x_hbm, v_hbm, y_hbm, out_hbm, xb, vb, yb, sem):
    def x_in(u):
        return pltpu.make_async_copy(x_hbm.at[:, u], xb.at[u], sem.at[u])

    def v_in(u):
        return pltpu.make_async_copy(v_hbm.at[u], vb.at[u], sem.at[NU + u])

    def x_out(u):
        return pltpu.make_async_copy(xb.at[u], out_hbm.at[:, u], sem.at[2 * NU + u])

    y_in = pltpu.make_async_copy(y_hbm, yb, sem.at[3 * NU])
    y_in.start()
    lax.fori_loop(0, NU, lambda u, _: (v_in(u).start(), x_in(u).start(), 0)[2], 0)
    y_in.wait()

    def body(j, _):
        for i in range(LAST):
            x_in(LAST * j + i).wait()
            v_in(LAST * j + i).wait()
        for i in range(LAST):
            u = LAST * j + i
            upd = mm6(split3(vb[u]), (yb[0], yb[1], yb[2]))
            xb[u] = xb[u] - upd.reshape(4, 64, 512)
        for i in range(LAST):
            x_out(LAST * j + i).start()
        return 0

    lax.fori_loop(0, NU // LAST, body, 0)
    lax.fori_loop(0, NU, lambda u, _: (x_out(u).wait(), 0)[1], 0)


def solution(mesh):
    def local_apply(v_loc, t_loc, z_loc):
        dma = pltpu.SemaphoreType.DMA
        x, v0, y = pl.pallas_call(
            kernel,
            out_shape=(
                jax.ShapeDtypeStruct((4, NU, 64, 512), F32),
                jax.ShapeDtypeStruct((NU, 256, 256), F32),
                jax.ShapeDtypeStruct((3, 256, 512), BF16),
            ),
            in_specs=[pl.BlockSpec(memory_space=pl.ANY)] * 3,
            out_specs=(pl.BlockSpec(memory_space=pl.ANY),) * 3,
            scratch_shapes=[
                pltpu.VMEM((NCH, 256, 256), F32),
                pltpu.VMEM((NU, 4, 64, 512), F32),
                pltpu.VMEM((2, NU, 2, 64, 64), F32),
                pltpu.VMEM((3, 256, 256), BF16),
                pltpu.VMEM((3, 256, 256), BF16),
                pltpu.VMEM((3, 256, 256), BF16),
                pltpu.VMEM((3, 256, 512), BF16),
                pltpu.VMEM((3, 256, 512), BF16),
                pltpu.VMEM((3, 256, 512), BF16),
                pltpu.VMEM((256, 512), F32),
                pltpu.VMEM((192, 256), F32),
                pltpu.VMEM((256, 256), F32),
                pltpu.VMEM((256, 256), F32),
                dma((NP,)), dma((NP,)), dma((NP,)),
                dma((4,)), dma((NU,)), dma((3,)), dma((2 * NU + 1,)),
            ],
            compiler_params=pltpu.CompilerParams(
                collective_id=0, has_side_effects=True, vmem_limit_bytes=67_043_328
            ),
            cost_estimate=pl.CostEstimate(flops=116_000_000_000, bytes_accessed=60_000_000, transcendentals=0),
        )(v_loc.reshape(NU, 64, 2048), t_loc.reshape(NU, 2, 64, 64), z_loc.reshape(4, NU, 64, 512))
        out = pl.pallas_call(
            last_update,
            out_shape=jax.ShapeDtypeStruct((4, NU, 64, 512), F32),
            in_specs=[pl.BlockSpec(memory_space=pl.ANY)] * 3,
            out_specs=pl.BlockSpec(memory_space=pl.ANY),
            scratch_shapes=[
                pltpu.VMEM((NU, 4, 64, 512), F32),
                pltpu.VMEM((NU, 256, 256), F32),
                pltpu.VMEM((3, 256, 512), BF16),
                dma((3 * NU + 1,)),
            ],
            compiler_params=pltpu.CompilerParams(vmem_limit_bytes=67_043_328),
            cost_estimate=pl.CostEstimate(flops=6_500_000_000, bytes_accessed=22_000_000, transcendentals=0),
        )(x, v0, y)
        return out.reshape(4096, 512)

    return jax.shard_map(
        local_apply,
        mesh=mesh,
        in_specs=(P("row", "col"), P("col", None, None), P(None, ("row", "col"))),
        out_specs=P(None, ("row", "col")),
        check_vma=False,
    )
```

```python
import functools

import jax
import jax.numpy as jnp
from jax import lax
from jax.experimental import pallas as pl
from jax.experimental.pallas import tpu as pltpu
from jax.sharding import PartitionSpec as P

MESH = pl.DeviceIdType.MESH
F32 = jnp.float32
BF16 = jnp.bfloat16

NU = 16
NCH = NU * (NU + 1) // 2
NP = NCH // 2
LEAD = (8, 5, 1)
PROLOGUE = (0, 0, 0, 0, 1, 0, 1, 1, 0, 0, 1, 0, 2, 2), (1, 0, 1)
ZAHEAD = 4
LAST = 2


def split3(x):
    h = x.astype(BF16)
    rem = x - h.astype(F32)
    m = rem.astype(BF16)
    l = (rem - m.astype(F32)).astype(BF16)
    return h, m, l


def dot(a, b):
    return jnp.dot(a, b, preferred_element_type=F32)


def mm6(a, b):
    ah, am, al = a
    bh, bm, bl = b
    return (dot(al, bh) + dot(ah, bl) + dot(am, bm)) + (dot(am, bh) + dot(ah, bm)) + dot(ah, bh)


def mm_f32(a, b):
    return mm6(split3(a), split3(b))


def mm_k128(a, b):
    ah, am, al = split3(a)
    bh, bm, bl = split3(b)

    def part(a0, a1, b0, b1):
        return dot(jnp.concatenate([a0, a1], axis=1), jnp.concatenate([b0, b1], axis=0))

    return (part(am, ah, bm, bl) + part(al, ah, bh, bm)) + part(am, ah, bh, bh)


def kernel(
    v_hbm, d_hbm, z_hbm, x_hbm, v0_hbm, y_hbm,
    vbuf, xbuf, dbuf, vt3, vt3b, vn3, x3, x3b, y3, wacc, s1acc, s2acc, tmat,
    r1_sem, r2_sem, rp_sem, send_sem, z_sem, d_sem, o_sem,
):
    r = lax.axis_index("row")
    q = lax.axis_index("col")
    ry, rx = r // 2, r % 2
    row_x = ry * 2 + (1 - rx)
    row_y = (1 - ry) * 2 + rx
    n1 = row_x * (1 - q) + row_y * q
    n2 = row_y * (1 - q) + row_x * q
    dev1, dev2, devp = (n1, q), (n2, q), (r, 1 - q)
    cols = pl.ds(pl.multiple_of(q * 128, 128), 128)

    def piece(c, n, rr):
        return vbuf.at[pl.ds(c, n), pl.ds(pl.multiple_of(rr * 64, 64), 64), cols]

    def remote(src, dst, k, rsem, dev):
        return pltpu.make_async_remote_copy(
            src_ref=src, dst_ref=dst, send_sem=send_sem.at[k], recv_sem=rsem,
            device_id=dev, device_id_type=MESH,
        )

    def stage0(p, c, s, u):
        src = v_hbm.at[pl.ds(u, 1), :, pl.ds(pl.multiple_of(s * 128, 128), 128)]
        dst = piece(c, 1, r)
        remote(src, dst, 0, r1_sem.at[p], dev1).start()
        remote(src, dst, 1, r2_sem.at[p], dev2).start()
        pltpu.make_async_copy(src, dst, r2_sem.at[p]).start()

    def stage1(p):
        x = piece(2 * p, 2, n1)
        remote(x, x, 0, r1_sem.at[p], dev1).wait_recv()
        remote(x, x, 2, r2_sem.at[p], dev2).start()

    def stage2(p):
        x = vbuf.at[pl.ds(2 * p, 2), pl.ds(0, 192), cols]
        remote(x, x, 1, r2_sem.at[p], dev2).wait_recv()
        x = vbuf.at[pl.ds(2 * p, 2), :, cols]
        remote(x, x, 3, rp_sem.at[p], devp).start()

    def stage3(p):
        x = vbuf.at[pl.ds(2 * p, 2), :, pl.ds(pl.multiple_of((1 - q) * 128, 128), 128)]
        remote(x, x, 3, rp_sem.at[p], devp).wait_recv()

    def send_own(p, su):
        s, u = su
        for i in range(2):

            @pl.when(p < NP)
            def _():
                stage0(p, 2 * p + i, s, u)

            last = u == NU - 1
            s2 = jnp.where(last, jnp.maximum(s - 1, 0), s)
            s, u = s2, jnp.where(last, s2, u + 1)
        return s, u

    def tick(p):
        @pl.when(p + LEAD[1] < NP)
        def _():
            stage1(p + LEAD[1])

        @pl.when(p + LEAD[2] < NP)
        def _():
            stage2(p + LEAD[2])

        @pl.when(p < NP)
        def _():
            stage3(p)

    barrier = pltpu.get_barrier_semaphore()
    for dev in (dev1, dev2, devp):
        pl.semaphore_signal(barrier, inc=1, device_id=dev, device_id_type=MESH)
    pl.semaphore_wait(barrier, 3)

    d_own = dbuf.at[q]
    d_send = pltpu.make_async_remote_copy(
        src_ref=d_hbm, dst_ref=d_own, send_sem=d_sem.at[0], recv_sem=d_sem.at[1],
        device_id=devp, device_id_type=MESH,
    )
    d_send.start()
    d_loc = pltpu.make_async_copy(d_hbm, d_own, d_sem.at[2])
    d_loc.start()

    def z_copy(u):
        return pltpu.make_async_copy(z_hbm.at[:, u], xbuf.at[u], z_sem.at[u])

    for i in range(ZAHEAD):
        z_copy(NU - 1 - i).start()
    chunks = [(s, u) for s in range(NU - 1, -1, -1) for u in range(s, NU)]
    done = [0, 0, 0]

    def prologue(stages):
        for i in stages:
            p = done[i]
            done[i] += 1
            if i == 0:
                stage0(p, 2 * p, *chunks[2 * p])
                stage0(p, 2 * p + 1, *chunks[2 * p + 1])
            else:
                (stage1 if i == 1 else stage2)(p)

    prologue(PROLOGUE[0])
    d_send.wait()
    d_loc.wait()

    def store3(ref, x):
        ref[0], ref[1], ref[2] = split3(x)

    def load3(ref):
        return ref[0], ref[1], ref[2]

    def do_a(vt, x):
        return mm6(load3(vt), load3(x))

    def do_c(c, u):
        x = xbuf[u].reshape(256, 512) - mm6(split3(vbuf[c]), load3(y3))
        xbuf[u] = x.reshape(4, 64, 512)
        return x

    def do_g(c, vt):
        v = vbuf[c]
        store3(vn3, v)
        store3(vt, v.T)
        g1 = dot(vt[1, :192], vn3[1]) + dot(vt[0, :192], vn3[0])
        g2 = dot(vt[0], vn3[2]) + dot(vt[0], vn3[1])
        return g1, g2

    low = lax.broadcasted_iota(jnp.int32, (64, 128), 1) < 64

    def roll(x):
        return pltpu.roll(x, 64, 1)

    def diag(s, i):
        zero = jnp.zeros((64, 64), F32)
        return jnp.concatenate(
            [
                jnp.concatenate([dbuf[0, s, i], zero], axis=1),
                jnp.concatenate([zero, dbuf[1, s, i]], axis=1),
            ],
            axis=0,
        )

    def merge_1(s, s1, s2):
        g = s1 + s2[:192] + s2.T[:192]
        zero = jnp.zeros((64, 128), F32)
        d01, d23 = diag(s, 0), diag(s, 1)
        u01 = jnp.concatenate([jnp.where(low, 0.0, roll(g[:64, 128:])), zero], axis=0)
        u23 = jnp.concatenate([jnp.where(low, 0.0, g[64:128, 128:]), zero], axis=0)
        u2 = jnp.concatenate(
            [
                jnp.where(low, roll(g[:64, :128]), g[:64, 128:]),
                jnp.where(low, roll(g[128:192, :128]), g[128:192, 128:]),
            ],
            axis=0,
        )
        nm = mm_k128(d01, jnp.concatenate([u01, u2], axis=1))
        z = mm_k128(u23, d23)
        return nm, z

    def merge_2(s, nm, z):
        d01, d23 = diag(s, 0), diag(s, 1)
        el = mm_k128(nm[:, :128], jnp.concatenate([d01, nm[:, 128:]], axis=1))
        t23 = d23 - mm_k128(d23, z)
        return d01 - el[:, :128], nm[:, 128:] - el[:, 128:], t23

    def merge_3(t01, lm, t23):
        f = -mm_k128(lm, t23)
        tmat[0:64, 0:128] = jnp.where(low, t01[:64], roll(f[:64]))
        tmat[0:64, 128:256] = jnp.where(low, roll(t01[:64]), f[:64])
        tmat[64:128, 0:128] = jnp.where(low, 0.0, roll(t23[:64]))
        tmat[64:128, 128:256] = jnp.where(low, 0.0, t23[:64])
        tmat[128:192, 0:128] = jnp.where(low, 0.0, roll(f[64:]))
        tmat[128:192, 128:256] = jnp.where(low, roll(t01[64:]), f[64:])
        tmat[192:256, 0:128] = jnp.zeros((64, 128), F32)
        tmat[192:256, 128:256] = t23[64:]

    def offset(s):
        return (NU - 1 - s) * (NU - s) // 2

    stage3(0)
    z_copy(NU - 1).wait()
    wacc[...] = jnp.zeros_like(wacc)
    s1acc[...], s2acc[...] = do_g(0, vt3)
    store3(x3, xbuf[NU - 1].reshape(256, 512))

    def step(c_a, c_c, u):
        wacc[...] += do_a(vt3, x3)
        x = do_c(c_c, u)
        g1, g2 = do_g(c_a + 1, vt3)
        s1acc[...] += g1
        s2acc[...] += g2
        store3(x3, x)

    def first_g(c):
        s1acc[...], s2acc[...] = do_g(jnp.minimum(c, NCH - 1), vt3)

    def finish(sa, w):
        store3(x3, xbuf[jnp.maximum(sa - 1, 0)].reshape(256, 512))
        store3(y3, mm_f32(tmat[...], w))
        wacc[...] = jnp.zeros_like(wacc)

    def next_z(sa):
        @pl.when(sa >= ZAHEAD)
        def _():
            z_copy(sa - ZAHEAD).start()

        @pl.when(sa >= 1)
        def _():
            z_copy(sa - 1).wait()

    next_z(NU - 1)
    vt3b[...] = vt3[...]
    x3b[...] = x3[...]
    merge_3(*merge_2(NU - 1, *merge_1(NU - 1, s1acc[...], s2acc[...])))
    first_g(1)
    finish(NU - 1, do_a(vt3b, x3b))

    prologue(PROLOGUE[1])
    carry = tuple(jnp.int32(i) for i in chunks[2 * done[0]])

    def x_copy(u):
        return pltpu.make_async_copy(xbuf.at[u], x_hbm.at[:, u], o_sem.at[u])

    def v_copy(u):
        return pltpu.make_async_copy(vbuf.at[NCH - NU + u], v0_hbm.at[u], o_sem.at[NU + u])

    def write_out(sa, lo, n):
        @pl.when(sa == 0)
        def _():
            for u in range(n):
                x_copy(lo + u).start()
                v_copy(lo + u).start()

    def outer(k, carry):
        s = NU - k
        sa = s - 1
        off_a = offset(sa)
        off_c = off_a - k

        def step1(u, carry):
            i = u - s
            c = off_a + i + 1

            def tick_and_send(su):
                tick(c // 2)
                return send_own(c // 2 + LEAD[0], su)

            carry = lax.cond(c % 2 == 0, tick_and_send, lambda su: su, carry)
            step(off_a + i, off_c + i, u)
            write_out(sa, u - 1, 1)
            return carry

        def step2(j, carry):
            i = 2 * j
            p = (off_a + i + 2) // 2
            tick(p)
            carry = send_own(p + LEAD[0], carry)
            step(off_a + i, off_c + i, s + i)
            step(off_a + i + 1, off_c + i + 1, s + i + 1)
            write_out(sa, s + i - 1, 2)
            return carry

        pairs = (k - 1) // 2
        carry = lax.fori_loop(0, pairs, step2, carry)
        carry = lax.fori_loop(s + 2 * pairs, NU - 1, step1, carry)

        p = (off_a + k + 1) // 2
        tick(p)
        carry = send_own(p + LEAD[0], carry)
        next_z(sa)
        write_out(sa, NU - 2, 1)

        @pl.when(sa == 0)
        def _():
            v_copy(NU - 1).start()

        store3(x3b, do_c(off_c + k - 1, NU - 1))
        g1, g2 = do_g(off_a + k, vt3b)
        w = wacc[...] + do_a(vt3, x3)
        part = merge_1(sa, s1acc[...] + g1, s2acc[...] + g2)
        w = w + do_a(vt3b, x3b)
        part = merge_2(sa, *part)
        first_g(off_a + k + 1)
        merge_3(*part)
        finish(sa, w)
        return carry

    lax.fori_loop(1, NU, outer, carry)

    y_copy = pltpu.make_async_copy(y3, y_hbm, o_sem.at[2 * NU])
    y_copy.start()
    x_copy(NU - 1).start()
    lax.fori_loop(0, NU, lambda u, _: (x_copy(u).wait(), v_copy(u).wait(), 0)[2], 0)
    y_copy.wait()
    sent = vbuf.at[:, pl.ds(0, 64), pl.ds(0, 128)]
    for k in range(3):
        remote(sent, sent, k, rp_sem.at[0], dev1).wait_send()
    sent = vbuf.at[:, :, pl.ds(0, 128)]
    remote(sent, sent, 3, rp_sem.at[0], devp).wait_send()


def last_update(x_hbm, v_hbm, y_hbm, out_hbm, xb, vb, yb, sem):
    def x_in(u):
        return pltpu.make_async_copy(x_hbm.at[:, u], xb.at[u], sem.at[u])

    def v_in(u):
        return pltpu.make_async_copy(v_hbm.at[u], vb.at[u], sem.at[NU + u])

    def x_out(u):
        return pltpu.make_async_copy(xb.at[u], out_hbm.at[:, u], sem.at[2 * NU + u])

    y_in = pltpu.make_async_copy(y_hbm, yb, sem.at[3 * NU])
    y_in.start()
    lax.fori_loop(0, NU, lambda u, _: (v_in(u).start(), x_in(u).start(), 0)[2], 0)
    y_in.wait()

    def body(j, _):
        for i in range(LAST):
            x_in(LAST * j + i).wait()
            v_in(LAST * j + i).wait()
        for i in range(LAST):
            u = LAST * j + i
            upd = mm6(split3(vb[u]), (yb[0], yb[1], yb[2]))
            xb[u] = xb[u] - upd.reshape(4, 64, 512)
        for i in range(LAST):
            x_out(LAST * j + i).start()
        return 0

    lax.fori_loop(0, NU // LAST, body, 0)
    lax.fori_loop(0, NU, lambda u, _: (x_out(u).wait(), 0)[1], 0)


def solution(mesh):
    def local_apply(v_loc, t_loc, z_loc):
        dma = pltpu.SemaphoreType.DMA
        x, v0, y = pl.pallas_call(
            kernel,
            out_shape=(
                jax.ShapeDtypeStruct((4, NU, 64, 512), F32),
                jax.ShapeDtypeStruct((NU, 256, 256), F32),
                jax.ShapeDtypeStruct((3, 256, 512), BF16),
            ),
            in_specs=[pl.BlockSpec(memory_space=pl.ANY)] * 3,
            out_specs=(pl.BlockSpec(memory_space=pl.ANY),) * 3,
            scratch_shapes=[
                pltpu.VMEM((NCH, 256, 256), F32),
                pltpu.VMEM((NU, 4, 64, 512), F32),
                pltpu.VMEM((2, NU, 2, 64, 64), F32),
                pltpu.VMEM((3, 256, 256), BF16),
                pltpu.VMEM((3, 256, 256), BF16),
                pltpu.VMEM((3, 256, 256), BF16),
                pltpu.VMEM((3, 256, 512), BF16),
                pltpu.VMEM((3, 256, 512), BF16),
                pltpu.VMEM((3, 256, 512), BF16),
                pltpu.VMEM((256, 512), F32),
                pltpu.VMEM((192, 256), F32),
                pltpu.VMEM((256, 256), F32),
                pltpu.VMEM((256, 256), F32),
                dma((NP,)), dma((NP,)), dma((NP,)),
                dma((4,)), dma((NU,)), dma((3,)), dma((2 * NU + 1,)),
            ],
            compiler_params=pltpu.CompilerParams(
                collective_id=0, has_side_effects=True, vmem_limit_bytes=67_043_328,
            ),
            cost_estimate=pl.CostEstimate(flops=116_000_000_000, bytes_accessed=60_000_000, transcendentals=0),
        )(v_loc.reshape(NU, 64, 2048), t_loc.reshape(NU, 2, 64, 64), z_loc.reshape(4, NU, 64, 512))
        out = pl.pallas_call(
            last_update,
            out_shape=jax.ShapeDtypeStruct((4, NU, 64, 512), F32),
            in_specs=[pl.BlockSpec(memory_space=pl.ANY)] * 3,
            out_specs=pl.BlockSpec(memory_space=pl.ANY),
            scratch_shapes=[
                pltpu.VMEM((NU, 4, 64, 512), F32),
                pltpu.VMEM((NU, 256, 256), F32),
                pltpu.VMEM((3, 256, 512), BF16),
                dma((3 * NU + 1,)),
            ],
            compiler_params=pltpu.CompilerParams(vmem_limit_bytes=67_043_328),
            cost_estimate=pl.CostEstimate(flops=6_500_000_000, bytes_accessed=22_000_000, transcendentals=0),
        )(x, v0, y)
        return out.reshape(4096, 512)

    return jax.shard_map(
        local_apply,
        mesh=mesh,
        in_specs=(P("row", "col"), P("col", None, None), P(None, ("row", "col"))),
        out_specs=P(None, ("row", "col")),
        check_vma=False,
    )
```

```python
import functools

import jax
import jax.numpy as jnp
from jax import lax
from jax.experimental import pallas as pl
from jax.experimental.pallas import tpu as pltpu
from jax.sharding import PartitionSpec as P

MESH = pl.DeviceIdType.MESH
F32 = jnp.float32
BF16 = jnp.bfloat16

NU = 16
NCH = NU * (NU + 1) // 2
NP = NCH // 2
LEAD = (8, 5, 1)
PROLOGUE = (0, 0, 0, 0, 1, 0, 1, 1, 0, 0, 1, 0, 2, 2), (1, 0, 1)
ZAHEAD = 4
LAST = 2


def split3(x):
    h = x.astype(BF16)
    rem = x - h.astype(F32)
    m = rem.astype(BF16)
    l = (rem - m.astype(F32)).astype(BF16)
    return h, m, l


def dot(a, b):
    return jnp.dot(a, b, preferred_element_type=F32)


def mm6(a, b):
    ah, am, al = a
    bh, bm, bl = b
    return (dot(al, bh) + dot(ah, bl) + dot(am, bm)) + (dot(am, bh) + dot(ah, bm)) + dot(ah, bh)


def mm_f32(a, b):
    return mm6(split3(a), split3(b))


def mm_k128(a, b):
    ah, am, al = split3(a)
    bh, bm, bl = split3(b)

    def part(a0, a1, b0, b1):
        return dot(jnp.concatenate([a0, a1], axis=1), jnp.concatenate([b0, b1], axis=0))

    return (part(am, ah, bm, bl) + part(al, ah, bh, bm)) + part(am, ah, bh, bh)


def kernel(
    v_hbm, d_hbm, z_hbm, x_hbm, v0_hbm, y_hbm,
    vbuf, xbuf, dbuf, vt3, vt3b, vn3, x3, x3b, y3, wacc, s1acc, s2acc, tmat,
    r1_sem, r2_sem, rp_sem, send_sem, z_sem, d_sem, o_sem,
):
    r = lax.axis_index("row")
    q = lax.axis_index("col")
    ry, rx = r // 2, r % 2
    row_x = ry * 2 + (1 - rx)
    row_y = (1 - ry) * 2 + rx
    n1 = row_x * (1 - q) + row_y * q
    n2 = row_y * (1 - q) + row_x * q
    dev1, dev2, devp = (n1, q), (n2, q), (r, 1 - q)
    cols = pl.ds(pl.multiple_of(q * 128, 128), 128)

    def piece(c, n, rr):
        return vbuf.at[pl.ds(c, n), pl.ds(pl.multiple_of(rr * 64, 64), 64), cols]

    def remote(src, dst, k, rsem, dev):
        return pltpu.make_async_remote_copy(
            src_ref=src, dst_ref=dst, send_sem=send_sem.at[k], recv_sem=rsem,
            device_id=dev, device_id_type=MESH,
        )

    def stage0(p, c, s, u):
        src = v_hbm.at[pl.ds(u, 1), :, pl.ds(pl.multiple_of(s * 128, 128), 128)]
        dst = piece(c, 1, r)
        remote(src, dst, 0, r1_sem.at[p], dev1).start()
        remote(src, dst, 1, r2_sem.at[p], dev2).start()
        pltpu.make_async_copy(src, dst, r2_sem.at[p]).start()

    def stage1(p):
        x = piece(2 * p, 2, n1)
        remote(x, x, 0, r1_sem.at[p], dev1).wait_recv()
        remote(x, x, 2, r2_sem.at[p], dev2).start()

    def stage2(p):
        x = vbuf.at[pl.ds(2 * p, 2), pl.ds(0, 192), cols]
        remote(x, x, 1, r2_sem.at[p], dev2).wait_recv()
        x = vbuf.at[pl.ds(2 * p, 2), :, cols]
        remote(x, x, 3, rp_sem.at[p], devp).start()

    def stage3(p):
        x = vbuf.at[pl.ds(2 * p, 2), :, pl.ds(pl.multiple_of((1 - q) * 128, 128), 128)]
        remote(x, x, 3, rp_sem.at[p], devp).wait_recv()

    def send_own(p, su):
        s, u = su
        for i in range(2):

            @pl.when(p < NP)
            def _():
                stage0(p, 2 * p + i, s, u)

            last = u == NU - 1
            s2 = jnp.where(last, jnp.maximum(s - 1, 0), s)
            s, u = s2, jnp.where(last, s2, u + 1)
        return s, u

    def tick(p):
        @pl.when(p + LEAD[1] < NP)
        def _():
            stage1(p + LEAD[1])

        @pl.when(p + LEAD[2] < NP)
        def _():
            stage2(p + LEAD[2])

        @pl.when(p < NP)
        def _():
            stage3(p)

    barrier = pltpu.get_barrier_semaphore()
    for dev in (dev1, dev2, devp):
        pl.semaphore_signal(barrier, inc=1, device_id=dev, device_id_type=MESH)
    pl.semaphore_wait(barrier, 3)

    def z_copy(u):
        return pltpu.make_async_copy(z_hbm.at[:, u], xbuf.at[u], z_sem.at[u])

    chunks = [(s, u) for s in range(NU - 1, -1, -1) for u in range(s, NU)]
    done = [0, 0, 0]

    def prologue(stages):
        for i in stages:
            p = done[i]
            done[i] += 1
            if i == 0:
                stage0(p, 2 * p, *chunks[2 * p])
                stage0(p, 2 * p + 1, *chunks[2 * p + 1])
            else:
                (stage1 if i == 1 else stage2)(p)

    prologue(PROLOGUE[0][:4])
    d_own = dbuf.at[q]
    d_send = pltpu.make_async_remote_copy(
        src_ref=d_hbm, dst_ref=d_own, send_sem=d_sem.at[0], recv_sem=d_sem.at[1],
        device_id=devp, device_id_type=MESH,
    )
    d_send.start()
    d_loc = pltpu.make_async_copy(d_hbm, d_own, d_sem.at[2])
    d_loc.start()
    for i in range(ZAHEAD):
        z_copy(NU - 1 - i).start()
    prologue(PROLOGUE[0][4:])
    d_send.wait()
    d_loc.wait()

    def store3(ref, x):
        ref[0], ref[1], ref[2] = split3(x)

    def load3(ref):
        return ref[0], ref[1], ref[2]

    def do_a(vt, x):
        return mm6(load3(vt), load3(x))

    def do_c(c, u):
        x = xbuf[u].reshape(256, 512) - mm6(split3(vbuf[c]), load3(y3))
        xbuf[u] = x.reshape(4, 64, 512)
        return x

    def do_g(c, vt):
        v = vbuf[c]
        store3(vn3, v)
        store3(vt, v.T)
        g1 = dot(vt[1, :192], vn3[1]) + dot(vt[0, :192], vn3[0])
        g2 = dot(vt[0], vn3[2]) + dot(vt[0], vn3[1])
        return g1, g2

    low = lax.broadcasted_iota(jnp.int32, (64, 128), 1) < 64

    def roll(x):
        return pltpu.roll(x, 64, 1)

    def diag(s, i):
        zero = jnp.zeros((64, 64), F32)
        return jnp.concatenate(
            [
                jnp.concatenate([dbuf[0, s, i], zero], axis=1),
                jnp.concatenate([zero, dbuf[1, s, i]], axis=1),
            ],
            axis=0,
        )

    def merge_1(s, s1, s2):
        g = s1 + s2[:192] + s2.T[:192]
        zero = jnp.zeros((64, 128), F32)
        d01, d23 = diag(s, 0), diag(s, 1)
        u01 = jnp.concatenate([jnp.where(low, 0.0, roll(g[:64, 128:])), zero], axis=0)
        u23 = jnp.concatenate([jnp.where(low, 0.0, g[64:128, 128:]), zero], axis=0)
        u2 = jnp.concatenate(
            [
                jnp.where(low, roll(g[:64, :128]), g[:64, 128:]),
                jnp.where(low, roll(g[128:192, :128]), g[128:192, 128:]),
            ],
            axis=0,
        )
        nm = mm_k128(d01, jnp.concatenate([u01, u2], axis=1))
        z = mm_k128(u23, d23)
        return nm, z

    def merge_2(s, nm, z):
        d01, d23 = diag(s, 0), diag(s, 1)
        el = mm_k128(nm[:, :128], jnp.concatenate([d01, nm[:, 128:]], axis=1))
        t23 = d23 - mm_k128(d23, z)
        return d01 - el[:, :128], nm[:, 128:] - el[:, 128:], t23

    def merge_3(t01, lm, t23):
        f = -mm_k128(lm, t23)
        tmat[0:64, 0:128] = jnp.where(low, t01[:64], roll(f[:64]))
        tmat[0:64, 128:256] = jnp.where(low, roll(t01[:64]), f[:64])
        tmat[64:128, 0:128] = jnp.where(low, 0.0, roll(t23[:64]))
        tmat[64:128, 128:256] = jnp.where(low, 0.0, t23[:64])
        tmat[128:192, 0:128] = jnp.where(low, 0.0, roll(f[64:]))
        tmat[128:192, 128:256] = jnp.where(low, roll(t01[64:]), f[64:])
        tmat[192:256, 0:128] = jnp.zeros((64, 128), F32)
        tmat[192:256, 128:256] = t23[64:]

    def offset(s):
        return (NU - 1 - s) * (NU - s) // 2

    stage3(0)
    z_copy(NU - 1).wait()
    wacc[...] = jnp.zeros_like(wacc)
    s1acc[...], s2acc[...] = do_g(0, vt3)
    store3(x3, xbuf[NU - 1].reshape(256, 512))

    def step(c_a, c_c, u, vt_in, x_in, vt_out, x_out):
        wacc[...] += do_a(vt_in, x_in)
        x = do_c(c_c, u)
        g1, g2 = do_g(c_a + 1, vt_out)
        s1acc[...] += g1
        s2acc[...] += g2
        store3(x_out, x)

    def first_g(c):
        s1acc[...], s2acc[...] = do_g(jnp.minimum(c, NCH - 1), vt3)

    def finish(sa, w):
        store3(x3, xbuf[jnp.maximum(sa - 1, 0)].reshape(256, 512))
        store3(y3, mm_f32(tmat[...], w))
        wacc[...] = jnp.zeros_like(wacc)

    def next_z(sa):
        @pl.when(sa >= ZAHEAD)
        def _():
            z_copy(sa - ZAHEAD).start()

        @pl.when(sa >= 1)
        def _():
            z_copy(sa - 1).wait()

    next_z(NU - 1)
    vt3b[...] = vt3[...]
    x3b[...] = x3[...]
    merge_3(*merge_2(NU - 1, *merge_1(NU - 1, s1acc[...], s2acc[...])))
    first_g(1)
    finish(NU - 1, do_a(vt3b, x3b))

    prologue(PROLOGUE[1])
    carry = tuple(jnp.int32(i) for i in chunks[2 * done[0]])

    def x_copy(u):
        return pltpu.make_async_copy(xbuf.at[u], x_hbm.at[:, u], o_sem.at[u])

    def v_copy(u):
        return pltpu.make_async_copy(vbuf.at[NCH - NU + u], v0_hbm.at[u], o_sem.at[NU + u])

    def write_out(sa, lo, n):
        @pl.when(sa == 0)
        def _():
            for u in range(n):
                x_copy(lo + u).start()
                v_copy(lo + u).start()

    def outer(k, carry):
        s = NU - k
        sa = s - 1
        off_a = offset(sa)
        off_c = off_a - k

        def step1(u, carry):
            i = u - s
            c = off_a + i + 1

            def tick_and_send(su):
                tick(c // 2)
                return send_own(c // 2 + LEAD[0], su)

            carry = lax.cond(c % 2 == 0, tick_and_send, lambda su: su, carry)
            step(off_a + i, off_c + i, u, vt3, x3, vt3, x3)
            write_out(sa, u - 1, 1)
            return carry

        def step2(j, carry):
            i = 2 * j
            p = (off_a + i + 2) // 2
            tick(p)
            carry = send_own(p + LEAD[0], carry)
            a = do_a(vt3, x3)
            x = do_c(off_c + i, s + i)
            store3(x3b, x)
            g1, g2 = do_g(off_a + i + 1, vt3b)
            x = do_c(off_c + i + 1, s + i + 1)
            wacc[...] += a + do_a(vt3b, x3b)
            store3(x3, x)
            h1, h2 = do_g(off_a + i + 2, vt3)
            s1acc[...] += g1 + h1
            s2acc[...] += g2 + h2
            write_out(sa, s + i - 1, 2)
            return carry

        pairs = (k - 1) // 2
        carry = lax.fori_loop(0, pairs, step2, carry)
        carry = lax.fori_loop(s + 2 * pairs, NU - 1, step1, carry)

        p = (off_a + k + 1) // 2
        tick(p)
        carry = send_own(p + LEAD[0], carry)
        next_z(sa)
        write_out(sa, NU - 2, 1)

        @pl.when(sa == 0)
        def _():
            v_copy(NU - 1).start()

        store3(x3b, do_c(off_c + k - 1, NU - 1))
        g1, g2 = do_g(off_a + k, vt3b)
        w = wacc[...] + do_a(vt3, x3)
        part = merge_1(sa, s1acc[...] + g1, s2acc[...] + g2)
        w = w + do_a(vt3b, x3b)
        part = merge_2(sa, *part)
        first_g(off_a + k + 1)
        merge_3(*part)
        finish(sa, w)
        return carry

    lax.fori_loop(1, NU, outer, carry)

    y_copy = pltpu.make_async_copy(y3, y_hbm, o_sem.at[2 * NU])
    y_copy.start()
    x_copy(NU - 1).start()
    lax.fori_loop(0, NU, lambda u, _: (x_copy(u).wait(), v_copy(u).wait(), 0)[2], 0)
    y_copy.wait()
    sent = vbuf.at[:, pl.ds(0, 64), pl.ds(0, 128)]
    for k in range(3):
        remote(sent, sent, k, rp_sem.at[0], dev1).wait_send()
    sent = vbuf.at[:, :, pl.ds(0, 128)]
    remote(sent, sent, 3, rp_sem.at[0], devp).wait_send()


def last_update(x_hbm, v_hbm, y_hbm, out_hbm, xb, vb, yb, sem):
    def x_in(u):
        return pltpu.make_async_copy(x_hbm.at[:, u], xb.at[u], sem.at[u])

    def v_in(u):
        return pltpu.make_async_copy(v_hbm.at[u], vb.at[u], sem.at[NU + u])

    def x_out(u):
        return pltpu.make_async_copy(xb.at[u], out_hbm.at[:, u], sem.at[2 * NU + u])

    y_in = pltpu.make_async_copy(y_hbm, yb, sem.at[3 * NU])
    y_in.start()
    lax.fori_loop(0, NU, lambda u, _: (v_in(u).start(), x_in(u).start(), 0)[2], 0)
    y_in.wait()

    def body(j, _):
        for i in range(LAST):
            x_in(LAST * j + i).wait()
            v_in(LAST * j + i).wait()
        for i in range(LAST):
            u = LAST * j + i
            upd = mm6(split3(vb[u]), (yb[0], yb[1], yb[2]))
            xb[u] = xb[u] - upd.reshape(4, 64, 512)
        for i in range(LAST):
            x_out(LAST * j + i).start()
        return 0

    lax.fori_loop(0, NU // LAST, body, 0)
    lax.fori_loop(0, NU, lambda u, _: (x_out(u).wait(), 0)[1], 0)


def solution(mesh):
    def local_apply(v_loc, t_loc, z_loc):
        dma = pltpu.SemaphoreType.DMA
        x, v0, y = pl.pallas_call(
            kernel,
            out_shape=(
                jax.ShapeDtypeStruct((4, NU, 64, 512), F32),
                jax.ShapeDtypeStruct((NU, 256, 256), F32),
                jax.ShapeDtypeStruct((3, 256, 512), BF16),
            ),
            in_specs=[pl.BlockSpec(memory_space=pl.ANY)] * 3,
            out_specs=(pl.BlockSpec(memory_space=pl.ANY),) * 3,
            scratch_shapes=[
                pltpu.VMEM((NCH, 256, 256), F32),
                pltpu.VMEM((NU, 4, 64, 512), F32),
                pltpu.VMEM((2, NU, 2, 64, 64), F32),
                pltpu.VMEM((3, 256, 256), BF16),
                pltpu.VMEM((3, 256, 256), BF16),
                pltpu.VMEM((3, 256, 256), BF16),
                pltpu.VMEM((3, 256, 512), BF16),
                pltpu.VMEM((3, 256, 512), BF16),
                pltpu.VMEM((3, 256, 512), BF16),
                pltpu.VMEM((256, 512), F32),
                pltpu.VMEM((192, 256), F32),
                pltpu.VMEM((256, 256), F32),
                pltpu.VMEM((256, 256), F32),
                dma((NP,)), dma((NP,)), dma((NP,)),
                dma((4,)), dma((NU,)), dma((3,)), dma((2 * NU + 1,)),
            ],
            compiler_params=pltpu.CompilerParams(
                collective_id=0, has_side_effects=True, vmem_limit_bytes=67_043_328,
            ),
            cost_estimate=pl.CostEstimate(flops=116_000_000_000, bytes_accessed=60_000_000, transcendentals=0),
        )(v_loc.reshape(NU, 64, 2048), t_loc.reshape(NU, 2, 64, 64), z_loc.reshape(4, NU, 64, 512))
        out = pl.pallas_call(
            last_update,
            out_shape=jax.ShapeDtypeStruct((4, NU, 64, 512), F32),
            in_specs=[pl.BlockSpec(memory_space=pl.ANY)] * 3,
            out_specs=pl.BlockSpec(memory_space=pl.ANY),
            scratch_shapes=[
                pltpu.VMEM((NU, 4, 64, 512), F32),
                pltpu.VMEM((NU, 256, 256), F32),
                pltpu.VMEM((3, 256, 512), BF16),
                dma((3 * NU + 1,)),
            ],
            compiler_params=pltpu.CompilerParams(vmem_limit_bytes=67_043_328),
            cost_estimate=pl.CostEstimate(flops=6_500_000_000, bytes_accessed=22_000_000, transcendentals=0),
        )(x, v0, y)
        return out.reshape(4096, 512)

    return jax.shard_map(
        local_apply,
        mesh=mesh,
        in_specs=(P("row", "col"), P("col", None, None), P(None, ("row", "col"))),
        out_specs=P(None, ("row", "col")),
        check_vma=False,
    )
```

```python
import functools

import jax
import jax.numpy as jnp
from jax import lax
from jax.experimental import pallas as pl
from jax.experimental.pallas import tpu as pltpu
from jax.sharding import PartitionSpec as P

MESH = pl.DeviceIdType.MESH
F32 = jnp.float32
BF16 = jnp.bfloat16

NU = 16
NCH = NU * (NU + 1) // 2
NP = NCH // 2
LEAD = (8, 5, 1)
PROLOGUE = (0, 0, 0, 0, 1, 0, 1, 1, 0, 0, 1, 0, 2, 2), (1, 0, 1)
ZAHEAD = 4
LAST = 4


def split3(x):
    h = x.astype(BF16)
    rem = x - h.astype(F32)
    m = rem.astype(BF16)
    l = (rem - m.astype(F32)).astype(BF16)
    return h, m, l


def dot(a, b):
    return jnp.dot(a, b, preferred_element_type=F32)


def mm6(a, b):
    ah, am, al = a
    bh, bm, bl = b
    return (dot(al, bh) + dot(ah, bl) + dot(am, bm)) + (dot(am, bh) + dot(ah, bm)) + dot(ah, bh)


def mm_f32(a, b):
    return mm6(split3(a), split3(b))


def mm_k128(a, b):
    ah, am, al = split3(a)
    bh, bm, bl = split3(b)

    def part(a0, a1, b0, b1):
        return dot(jnp.concatenate([a0, a1], axis=1), jnp.concatenate([b0, b1], axis=0))

    return (part(am, ah, bm, bl) + part(al, ah, bh, bm)) + part(am, ah, bh, bh)


def kernel(
    v_hbm, d_hbm, z_hbm, x_hbm, v0_hbm, y_hbm,
    vbuf, xbuf, dbuf, vt3, vt3b, vn3, x3, x3b, y3, wacc, s1acc, s2acc, tmat,
    r1_sem, r2_sem, rp_sem, send_sem, z_sem, d_sem, o_sem,
):
    r = lax.axis_index("row")
    q = lax.axis_index("col")
    ry, rx = r // 2, r % 2
    row_x = ry * 2 + (1 - rx)
    row_y = (1 - ry) * 2 + rx
    n1 = row_x * (1 - q) + row_y * q
    n2 = row_y * (1 - q) + row_x * q
    dev1, dev2, devp = (n1, q), (n2, q), (r, 1 - q)
    cols = pl.ds(pl.multiple_of(q * 128, 128), 128)

    def piece(c, n, rr):
        return vbuf.at[pl.ds(c, n), pl.ds(pl.multiple_of(rr * 64, 64), 64), cols]

    def remote(src, dst, k, rsem, dev):
        return pltpu.make_async_remote_copy(
            src_ref=src, dst_ref=dst, send_sem=send_sem.at[k], recv_sem=rsem,
            device_id=dev, device_id_type=MESH,
        )

    def stage0(p, c, s, u):
        src = v_hbm.at[pl.ds(u, 1), :, pl.ds(pl.multiple_of(s * 128, 128), 128)]
        dst = piece(c, 1, r)
        remote(src, dst, 0, r1_sem.at[p], dev1).start()
        remote(src, dst, 1, r2_sem.at[p], dev2).start()
        pltpu.make_async_copy(src, dst, r2_sem.at[p]).start()

    def stage1(p):
        x = piece(2 * p, 2, n1)
        remote(x, x, 0, r1_sem.at[p], dev1).wait_recv()
        remote(x, x, 2, r2_sem.at[p], dev2).start()

    def stage2(p):
        x = vbuf.at[pl.ds(2 * p, 2), pl.ds(0, 192), cols]
        remote(x, x, 1, r2_sem.at[p], dev2).wait_recv()
        x = vbuf.at[pl.ds(2 * p, 2), :, cols]
        remote(x, x, 3, rp_sem.at[p], devp).start()

    def stage3(p):
        x = vbuf.at[pl.ds(2 * p, 2), :, pl.ds(pl.multiple_of((1 - q) * 128, 128), 128)]
        remote(x, x, 3, rp_sem.at[p], devp).wait_recv()

    def send_own(p, su):
        s, u = su
        for i in range(2):

            @pl.when(p < NP)
            def _():
                stage0(p, 2 * p + i, s, u)

            last = u == NU - 1
            s2 = jnp.where(last, jnp.maximum(s - 1, 0), s)
            s, u = s2, jnp.where(last, s2, u + 1)
        return s, u

    def tick(p):
        @pl.when(p + LEAD[1] < NP)
        def _():
            stage1(p + LEAD[1])

        @pl.when(p + LEAD[2] < NP)
        def _():
            stage2(p + LEAD[2])

        @pl.when(p < NP)
        def _():
            stage3(p)

    barrier = pltpu.get_barrier_semaphore()
    for dev in (dev1, dev2, devp):
        pl.semaphore_signal(barrier, inc=1, device_id=dev, device_id_type=MESH)
    pl.semaphore_wait(barrier, 3)

    def z_copy(u):
        return pltpu.make_async_copy(z_hbm.at[:, u], xbuf.at[u], z_sem.at[u])

    chunks = [(s, u) for s in range(NU - 1, -1, -1) for u in range(s, NU)]
    done = [0, 0, 0]

    def prologue(stages):
        for i in stages:
            p = done[i]
            done[i] += 1
            if i == 0:
                stage0(p, 2 * p, *chunks[2 * p])
                stage0(p, 2 * p + 1, *chunks[2 * p + 1])
            else:
                (stage1 if i == 1 else stage2)(p)

    prologue(PROLOGUE[0][:4])
    d_own = dbuf.at[q]
    d_send = pltpu.make_async_remote_copy(
        src_ref=d_hbm, dst_ref=d_own, send_sem=d_sem.at[0], recv_sem=d_sem.at[1],
        device_id=devp, device_id_type=MESH,
    )
    d_send.start()
    d_loc = pltpu.make_async_copy(d_hbm, d_own, d_sem.at[2])
    d_loc.start()
    for i in range(ZAHEAD):
        z_copy(NU - 1 - i).start()
    prologue(PROLOGUE[0][4:])
    d_send.wait()
    d_loc.wait()

    def store3(ref, x):
        ref[0], ref[1], ref[2] = split3(x)

    def load3(ref):
        return ref[0], ref[1], ref[2]

    def do_a(vt, x):
        return mm6(load3(vt), load3(x))

    def do_c(c, u):
        x = xbuf[u].reshape(256, 512) - mm6(split3(vbuf[c]), load3(y3))
        xbuf[u] = x.reshape(4, 64, 512)
        return x

    def do_g(c, vt):
        v = vbuf[c]
        store3(vn3, v)
        store3(vt, v.T)
        g1 = dot(vt[1, :192], vn3[1]) + dot(vt[0, :192], vn3[0])
        g2 = dot(vt[0], vn3[2]) + dot(vt[0], vn3[1])
        return g1, g2

    low = lax.broadcasted_iota(jnp.int32, (64, 128), 1) < 64

    def roll(x):
        return pltpu.roll(x, 64, 1)

    def diag(s, i):
        zero = jnp.zeros((64, 64), F32)
        return jnp.concatenate(
            [
                jnp.concatenate([dbuf[0, s, i], zero], axis=1),
                jnp.concatenate([zero, dbuf[1, s, i]], axis=1),
            ],
            axis=0,
        )

    def merge_1(s, s1, s2):
        g = s1 + s2[:192] + s2.T[:192]
        zero = jnp.zeros((64, 128), F32)
        d01, d23 = diag(s, 0), diag(s, 1)
        u01 = jnp.concatenate([jnp.where(low, 0.0, roll(g[:64, 128:])), zero], axis=0)
        u23 = jnp.concatenate([jnp.where(low, 0.0, g[64:128, 128:]), zero], axis=0)
        u2 = jnp.concatenate(
            [
                jnp.where(low, roll(g[:64, :128]), g[:64, 128:]),
                jnp.where(low, roll(g[128:192, :128]), g[128:192, 128:]),
            ],
            axis=0,
        )
        nm = mm_k128(d01, jnp.concatenate([u01, u2], axis=1))
        z = mm_k128(u23, d23)
        return nm, z

    def merge_2(s, nm, z):
        d01, d23 = diag(s, 0), diag(s, 1)
        el = mm_k128(nm[:, :128], jnp.concatenate([d01, nm[:, 128:]], axis=1))
        t23 = d23 - mm_k128(d23, z)
        return d01 - el[:, :128], nm[:, 128:] - el[:, 128:], t23

    def merge_3(t01, lm, t23):
        f = -mm_k128(lm, t23)
        tmat[0:64, 0:128] = jnp.where(low, t01[:64], roll(f[:64]))
        tmat[0:64, 128:256] = jnp.where(low, roll(t01[:64]), f[:64])
        tmat[64:128, 0:128] = jnp.where(low, 0.0, roll(t23[:64]))
        tmat[64:128, 128:256] = jnp.where(low, 0.0, t23[:64])
        tmat[128:192, 0:128] = jnp.where(low, 0.0, roll(f[64:]))
        tmat[128:192, 128:256] = jnp.where(low, roll(t01[64:]), f[64:])
        tmat[192:256, 0:128] = jnp.zeros((64, 128), F32)
        tmat[192:256, 128:256] = t23[64:]

    def offset(s):
        return (NU - 1 - s) * (NU - s) // 2

    stage3(0)
    z_copy(NU - 1).wait()
    wacc[...] = jnp.zeros_like(wacc)
    s1acc[...], s2acc[...] = do_g(0, vt3)
    store3(x3, xbuf[NU - 1].reshape(256, 512))

    def step(c_a, c_c, u, vt_in, x_in, vt_out, x_out):
        wacc[...] += do_a(vt_in, x_in)
        x = do_c(c_c, u)
        g1, g2 = do_g(c_a + 1, vt_out)
        s1acc[...] += g1
        s2acc[...] += g2
        store3(x_out, x)

    def first_g(c):
        s1acc[...], s2acc[...] = do_g(jnp.minimum(c, NCH - 1), vt3)

    def finish(sa, w):
        store3(x3, xbuf[jnp.maximum(sa - 1, 0)].reshape(256, 512))
        store3(y3, mm_f32(tmat[...], w))
        wacc[...] = jnp.zeros_like(wacc)

    def next_z(sa):
        @pl.when(sa >= ZAHEAD)
        def _():
            z_copy(sa - ZAHEAD).start()

        @pl.when(sa >= 1)
        def _():
            z_copy(sa - 1).wait()

    next_z(NU - 1)
    vt3b[...] = vt3[...]
    x3b[...] = x3[...]
    merge_3(*merge_2(NU - 1, *merge_1(NU - 1, s1acc[...], s2acc[...])))
    first_g(1)
    finish(NU - 1, do_a(vt3b, x3b))

    prologue(PROLOGUE[1])
    carry = tuple(jnp.int32(i) for i in chunks[2 * done[0]])

    def x_copy(u):
        return pltpu.make_async_copy(xbuf.at[u], x_hbm.at[:, u], o_sem.at[u])

    def v_copy(u):
        return pltpu.make_async_copy(vbuf.at[NCH - NU + u], v0_hbm.at[u], o_sem.at[NU + u])

    def write_out(sa, lo, n):
        @pl.when(sa == 0)
        def _():
            for u in range(n):
                x_copy(lo + u).start()
                v_copy(lo + u).start()

    def outer(k, carry):
        s = NU - k
        sa = s - 1
        off_a = offset(sa)
        off_c = off_a - k

        def step1(u, carry):
            i = u - s
            c = off_a + i + 1

            def tick_and_send(su):
                tick(c // 2)
                return send_own(c // 2 + LEAD[0], su)

            carry = lax.cond(c % 2 == 0, tick_and_send, lambda su: su, carry)
            step(off_a + i, off_c + i, u, vt3, x3, vt3, x3)
            write_out(sa, u - 1, 1)
            return carry

        def step2(j, carry):
            i = 2 * j
            p = (off_a + i + 2) // 2
            tick(p)
            carry = send_own(p + LEAD[0], carry)
            a = do_a(vt3, x3)
            x = do_c(off_c + i, s + i)
            store3(x3b, x)
            g1, g2 = do_g(off_a + i + 1, vt3b)
            x = do_c(off_c + i + 1, s + i + 1)
            wacc[...] += a + do_a(vt3b, x3b)
            store3(x3, x)
            h1, h2 = do_g(off_a + i + 2, vt3)
            s1acc[...] += g1 + h1
            s2acc[...] += g2 + h2
            write_out(sa, s + i - 1, 2)
            return carry

        pairs = (k - 1) // 2
        carry = lax.fori_loop(0, pairs, step2, carry)
        carry = lax.fori_loop(s + 2 * pairs, NU - 1, step1, carry)

        p = (off_a + k + 1) // 2
        tick(p)
        carry = send_own(p + LEAD[0], carry)
        next_z(sa)
        write_out(sa, NU - 2, 1)

        @pl.when(sa == 0)
        def _():
            v_copy(NU - 1).start()

        store3(x3b, do_c(off_c + k - 1, NU - 1))
        g1, g2 = do_g(off_a + k, vt3b)
        w = wacc[...] + do_a(vt3, x3)
        part = merge_1(sa, s1acc[...] + g1, s2acc[...] + g2)
        w = w + do_a(vt3b, x3b)
        part = merge_2(sa, *part)
        first_g(off_a + k + 1)
        merge_3(*part)
        finish(sa, w)
        return carry

    lax.fori_loop(1, NU, outer, carry)

    y_copy = pltpu.make_async_copy(y3, y_hbm, o_sem.at[2 * NU])
    y_copy.start()
    x_copy(NU - 1).start()
    lax.fori_loop(0, NU, lambda u, _: (x_copy(u).wait(), v_copy(u).wait(), 0)[2], 0)
    y_copy.wait()
    sent = vbuf.at[:, pl.ds(0, 64), pl.ds(0, 128)]
    for k in range(3):
        remote(sent, sent, k, rp_sem.at[0], dev1).wait_send()
    sent = vbuf.at[:, :, pl.ds(0, 128)]
    remote(sent, sent, 3, rp_sem.at[0], devp).wait_send()


def last_update(x_hbm, v_hbm, y_hbm, out_hbm, xb, vb, yb, sem):
    def x_in(u):
        return pltpu.make_async_copy(x_hbm.at[:, u], xb.at[u], sem.at[u])

    def v_in(u):
        return pltpu.make_async_copy(v_hbm.at[u], vb.at[u], sem.at[NU + u])

    def x_out(u):
        return pltpu.make_async_copy(xb.at[u], out_hbm.at[:, u], sem.at[2 * NU + u])

    y_in = pltpu.make_async_copy(y_hbm, yb, sem.at[3 * NU])
    y_in.start()
    lax.fori_loop(0, NU, lambda u, _: (v_in(u).start(), x_in(u).start(), 0)[2], 0)
    y_in.wait()

    def body(j, _):
        for i in range(LAST):
            x_in(LAST * j + i).wait()
            v_in(LAST * j + i).wait()
        for i in range(LAST):
            u = LAST * j + i
            upd = mm6(split3(vb[u]), (yb[0], yb[1], yb[2]))
            xb[u] = xb[u] - upd.reshape(4, 64, 512)
        for i in range(LAST):
            x_out(LAST * j + i).start()
        return 0

    lax.fori_loop(0, NU // LAST, body, 0)
    lax.fori_loop(0, NU, lambda u, _: (x_out(u).wait(), 0)[1], 0)


def solution(mesh):
    def local_apply(v_loc, t_loc, z_loc):
        dma = pltpu.SemaphoreType.DMA
        x, v0, y = pl.pallas_call(
            kernel,
            out_shape=(
                jax.ShapeDtypeStruct((4, NU, 64, 512), F32),
                jax.ShapeDtypeStruct((NU, 256, 256), F32),
                jax.ShapeDtypeStruct((3, 256, 512), BF16),
            ),
            in_specs=[pl.BlockSpec(memory_space=pl.ANY)] * 3,
            out_specs=(pl.BlockSpec(memory_space=pl.ANY),) * 3,
            scratch_shapes=[
                pltpu.VMEM((NCH, 256, 256), F32),
                pltpu.VMEM((NU, 4, 64, 512), F32),
                pltpu.VMEM((2, NU, 2, 64, 64), F32),
                pltpu.VMEM((3, 256, 256), BF16),
                pltpu.VMEM((3, 256, 256), BF16),
                pltpu.VMEM((3, 256, 256), BF16),
                pltpu.VMEM((3, 256, 512), BF16),
                pltpu.VMEM((3, 256, 512), BF16),
                pltpu.VMEM((3, 256, 512), BF16),
                pltpu.VMEM((256, 512), F32),
                pltpu.VMEM((192, 256), F32),
                pltpu.VMEM((256, 256), F32),
                pltpu.VMEM((256, 256), F32),
                dma((NP,)), dma((NP,)), dma((NP,)),
                dma((4,)), dma((NU,)), dma((3,)), dma((2 * NU + 1,)),
            ],
            compiler_params=pltpu.CompilerParams(
                collective_id=0, has_side_effects=True, vmem_limit_bytes=67_043_328,
            ),
            cost_estimate=pl.CostEstimate(flops=116_000_000_000, bytes_accessed=60_000_000, transcendentals=0),
        )(v_loc.reshape(NU, 64, 2048), t_loc.reshape(NU, 2, 64, 64), z_loc.reshape(4, NU, 64, 512))
        out = pl.pallas_call(
            last_update,
            out_shape=jax.ShapeDtypeStruct((4, NU, 64, 512), F32),
            in_specs=[pl.BlockSpec(memory_space=pl.ANY)] * 3,
            out_specs=pl.BlockSpec(memory_space=pl.ANY),
            scratch_shapes=[
                pltpu.VMEM((NU, 4, 64, 512), F32),
                pltpu.VMEM((NU, 256, 256), F32),
                pltpu.VMEM((3, 256, 512), BF16),
                dma((3 * NU + 1,)),
            ],
            compiler_params=pltpu.CompilerParams(vmem_limit_bytes=67_043_328),
            cost_estimate=pl.CostEstimate(flops=6_500_000_000, bytes_accessed=22_000_000, transcendentals=0),
        )(x, v0, y)
        return out.reshape(4096, 512)

    return jax.shard_map(
        local_apply,
        mesh=mesh,
        in_specs=(P("row", "col"), P("col", None, None), P(None, ("row", "col"))),
        out_specs=P(None, ("row", "col")),
        check_vma=False,
    )
```

```python
import functools

import jax
import jax.numpy as jnp
from jax import lax
from jax.experimental import pallas as pl
from jax.experimental.pallas import tpu as pltpu
from jax.sharding import PartitionSpec as P

MESH = pl.DeviceIdType.MESH
F32 = jnp.float32
BF16 = jnp.bfloat16

NU = 16
NCH = NU * (NU + 1) // 2
NP = NCH // 2
LEAD = (8, 5, 1)
PROLOGUE = (0, 0, 0, 0, 1, 0, 1, 1, 0, 0, 1, 0, 2, 2), (1, 0, 1)
ZAHEAD = 4
LAST = 2


def split3(x):
    h = x.astype(BF16)
    rem = x - h.astype(F32)
    m = rem.astype(BF16)
    l = (rem - m.astype(F32)).astype(BF16)
    return h, m, l


def dot(a, b):
    return jnp.dot(a, b, preferred_element_type=F32)


def mm6(a, b):
    ah, am, al = a
    bh, bm, bl = b
    return (dot(al, bh) + dot(ah, bl) + dot(am, bm)) + (dot(am, bh) + dot(ah, bm)) + dot(ah, bh)


def mm_f32(a, b):
    return mm6(split3(a), split3(b))


def mm_k128(a, b):
    ah, am, al = split3(a)
    bh, bm, bl = split3(b)

    def part(a0, a1, b0, b1):
        return dot(jnp.concatenate([a0, a1], axis=1), jnp.concatenate([b0, b1], axis=0))

    return (part(am, ah, bm, bl) + part(al, ah, bh, bm)) + part(am, ah, bh, bh)


def kernel(
    v_hbm, d_hbm, z_hbm, x_hbm, v0_hbm, y_hbm,
    vbuf, xbuf, dbuf, vt3, vt3b, vn3, x3, x3b, y3, wacc, s1acc, s2acc, tmat,
    r1_sem, r2_sem, rp_sem, send_sem, z_sem, d_sem, o_sem,
):
    r = lax.axis_index("row")
    q = lax.axis_index("col")
    ry, rx = r // 2, r % 2
    row_x = ry * 2 + (1 - rx)
    row_y = (1 - ry) * 2 + rx
    n1 = row_x * (1 - q) + row_y * q
    n2 = row_y * (1 - q) + row_x * q
    dev1, dev2, devp = (n1, q), (n2, q), (r, 1 - q)
    cols = pl.ds(pl.multiple_of(q * 128, 128), 128)

    def piece(c, n, rr):
        return vbuf.at[pl.ds(c, n), pl.ds(pl.multiple_of(rr * 64, 64), 64), cols]

    def remote(src, dst, k, rsem, dev):
        return pltpu.make_async_remote_copy(
            src_ref=src, dst_ref=dst, send_sem=send_sem.at[k], recv_sem=rsem,
            device_id=dev, device_id_type=MESH,
        )

    def stage0(p, c, s, u):
        src = v_hbm.at[pl.ds(u, 1), :, pl.ds(pl.multiple_of(s * 128, 128), 128)]
        dst = piece(c, 1, r)
        remote(src, dst, 0, r1_sem.at[p], dev1).start()
        remote(src, dst, 1, r2_sem.at[p], dev2).start()
        pltpu.make_async_copy(src, dst, r2_sem.at[p]).start()

    def stage1(p, wait=True, send=True):
        x = piece(2 * p, 2, n1)
        if wait:
            remote(x, x, 0, r1_sem.at[p], dev1).wait_recv()
        if send:
            remote(x, x, 2, r2_sem.at[p], dev2).start()

    def stage2(p, wait=True, send=True):
        if wait:
            x = vbuf.at[pl.ds(2 * p, 2), pl.ds(0, 192), cols]
            remote(x, x, 1, r2_sem.at[p], dev2).wait_recv()
        if send:
            x = vbuf.at[pl.ds(2 * p, 2), :, cols]
            remote(x, x, 3, rp_sem.at[p], devp).start()

    def stage3(p):
        x = vbuf.at[pl.ds(2 * p, 2), :, pl.ds(pl.multiple_of((1 - q) * 128, 128), 128)]
        remote(x, x, 3, rp_sem.at[p], devp).wait_recv()

    def send_own(p, su):
        s, u = su
        for i in range(2):

            @pl.when(p < NP)
            def _():
                stage0(p, 2 * p + i, s, u)

            last = u == NU - 1
            s2 = jnp.where(last, jnp.maximum(s - 1, 0), s)
            s, u = s2, jnp.where(last, s2, u + 1)
        return s, u

    def tick(p):
        @pl.when(p + LEAD[1] < NP)
        def _():
            stage1(p + LEAD[1], True, False)

        @pl.when(p + LEAD[2] < NP)
        def _():
            stage2(p + LEAD[2], True, False)

        @pl.when(p < NP)
        def _():
            stage3(p)

        @pl.when(p + LEAD[1] < NP)
        def _():
            stage1(p + LEAD[1], False, True)

        @pl.when(p + LEAD[2] < NP)
        def _():
            stage2(p + LEAD[2], False, True)

    barrier = pltpu.get_barrier_semaphore()
    for dev in (dev1, dev2, devp):
        pl.semaphore_signal(barrier, inc=1, device_id=dev, device_id_type=MESH)
    pl.semaphore_wait(barrier, 3)

    def z_copy(u):
        return pltpu.make_async_copy(z_hbm.at[:, u], xbuf.at[u], z_sem.at[u])

    chunks = [(s, u) for s in range(NU - 1, -1, -1) for u in range(s, NU)]
    done = [0, 0, 0]

    def prologue(stages):
        for i in stages:
            p = done[i]
            done[i] += 1
            if i == 0:
                stage0(p, 2 * p, *chunks[2 * p])
                stage0(p, 2 * p + 1, *chunks[2 * p + 1])
            else:
                (stage1 if i == 1 else stage2)(p)

    prologue(PROLOGUE[0][:4])
    d_own = dbuf.at[q]
    d_send = pltpu.make_async_remote_copy(
        src_ref=d_hbm, dst_ref=d_own, send_sem=d_sem.at[0], recv_sem=d_sem.at[1],
        device_id=devp, device_id_type=MESH,
    )
    d_send.start()
    d_loc = pltpu.make_async_copy(d_hbm, d_own, d_sem.at[2])
    d_loc.start()
    for i in range(ZAHEAD):
        z_copy(NU - 1 - i).start()
    prologue(PROLOGUE[0][4:])
    d_send.wait()
    d_loc.wait()

    def store3(ref, x):
        ref[0], ref[1], ref[2] = split3(x)

    def load3(ref):
        return ref[0], ref[1], ref[2]

    def do_a(vt, x):
        return mm6(load3(vt), load3(x))

    def do_c(c, u):
        x = xbuf[u].reshape(256, 512) - mm6(split3(vbuf[c]), load3(y3))
        xbuf[u] = x.reshape(4, 64, 512)
        return x

    def do_g(c, vt):
        v = vbuf[c]
        store3(vn3, v)
        store3(vt, v.T)
        g1 = dot(vt[1, :192], vn3[1]) + dot(vt[0, :192], vn3[0])
        g2 = dot(vt[0], vn3[2]) + dot(vt[0], vn3[1])
        return g1, g2

    low = lax.broadcasted_iota(jnp.int32, (64, 128), 1) < 64

    def roll(x):
        return pltpu.roll(x, 64, 1)

    def diag(s, i):
        zero = jnp.zeros((64, 64), F32)
        return jnp.concatenate(
            [
                jnp.concatenate([dbuf[0, s, i], zero], axis=1),
                jnp.concatenate([zero, dbuf[1, s, i]], axis=1),
            ],
            axis=0,
        )

    def merge_1(s, s1, s2):
        g = s1 + s2[:192] + s2.T[:192]
        zero = jnp.zeros((64, 128), F32)
        d01, d23 = diag(s, 0), diag(s, 1)
        u01 = jnp.concatenate([jnp.where(low, 0.0, roll(g[:64, 128:])), zero], axis=0)
        u23 = jnp.concatenate([jnp.where(low, 0.0, g[64:128, 128:]), zero], axis=0)
        u2 = jnp.concatenate(
            [
                jnp.where(low, roll(g[:64, :128]), g[:64, 128:]),
                jnp.where(low, roll(g[128:192, :128]), g[128:192, 128:]),
            ],
            axis=0,
        )
        nm = mm_k128(d01, jnp.concatenate([u01, u2], axis=1))
        z = mm_k128(u23, d23)
        return nm, z

    def merge_2(s, nm, z):
        d01, d23 = diag(s, 0), diag(s, 1)
        el = mm_k128(nm[:, :128], jnp.concatenate([d01, nm[:, 128:]], axis=1))
        t23 = d23 - mm_k128(d23, z)
        return d01 - el[:, :128], nm[:, 128:] - el[:, 128:], t23

    def merge_3(t01, lm, t23):
        f = -mm_k128(lm, t23)
        tmat[0:64, 0:128] = jnp.where(low, t01[:64], roll(f[:64]))
        tmat[0:64, 128:256] = jnp.where(low, roll(t01[:64]), f[:64])
        tmat[64:128, 0:128] = jnp.where(low, 0.0, roll(t23[:64]))
        tmat[64:128, 128:256] = jnp.where(low, 0.0, t23[:64])
        tmat[128:192, 0:128] = jnp.where(low, 0.0, roll(f[64:]))
        tmat[128:192, 128:256] = jnp.where(low, roll(t01[64:]), f[64:])
        tmat[192:256, 0:128] = jnp.zeros((64, 128), F32)
        tmat[192:256, 128:256] = t23[64:]

    def offset(s):
        return (NU - 1 - s) * (NU - s) // 2

    stage3(0)
    z_copy(NU - 1).wait()
    wacc[...] = jnp.zeros_like(wacc)
    s1acc[...], s2acc[...] = do_g(0, vt3)
    store3(x3, xbuf[NU - 1].reshape(256, 512))

    def step(c_a, c_c, u, vt_in, x_in, vt_out, x_out):
        wacc[...] += do_a(vt_in, x_in)
        x = do_c(c_c, u)
        g1, g2 = do_g(c_a + 1, vt_out)
        s1acc[...] += g1
        s2acc[...] += g2
        store3(x_out, x)

    def first_g(c):
        s1acc[...], s2acc[...] = do_g(jnp.minimum(c, NCH - 1), vt3)

    def finish(sa, w):
        store3(x3, xbuf[jnp.maximum(sa - 1, 0)].reshape(256, 512))
        store3(y3, mm_f32(tmat[...], w))
        wacc[...] = jnp.zeros_like(wacc)

    def next_z(sa):
        @pl.when(sa >= ZAHEAD)
        def _():
            z_copy(sa - ZAHEAD).start()

        @pl.when(sa >= 1)
        def _():
            z_copy(sa - 1).wait()

    next_z(NU - 1)
    vt3b[...] = vt3[...]
    x3b[...] = x3[...]
    merge_3(*merge_2(NU - 1, *merge_1(NU - 1, s1acc[...], s2acc[...])))
    first_g(1)
    finish(NU - 1, do_a(vt3b, x3b))

    prologue(PROLOGUE[1])
    carry = tuple(jnp.int32(i) for i in chunks[2 * done[0]])

    def x_copy(u):
        return pltpu.make_async_copy(xbuf.at[u], x_hbm.at[:, u], o_sem.at[u])

    def v_copy(u):
        return pltpu.make_async_copy(vbuf.at[NCH - NU + u], v0_hbm.at[u], o_sem.at[NU + u])

    def write_out(sa, lo, n):
        @pl.when(sa == 0)
        def _():
            for u in range(n):
                x_copy(lo + u).start()
                v_copy(lo + u).start()

    def outer(k, carry):
        s = NU - k
        sa = s - 1
        off_a = offset(sa)
        off_c = off_a - k

        def step1(u, carry):
            i = u - s
            c = off_a + i + 1

            def tick_and_send(su):
                tick(c // 2)
                return send_own(c // 2 + LEAD[0], su)

            carry = lax.cond(c % 2 == 0, tick_and_send, lambda su: su, carry)
            step(off_a + i, off_c + i, u, vt3, x3, vt3, x3)
            write_out(sa, u - 1, 1)
            return carry

        def step2(j, carry):
            i = 2 * j
            p = (off_a + i + 2) // 2
            tick(p)
            carry = send_own(p + LEAD[0], carry)
            a = do_a(vt3, x3)
            x = do_c(off_c + i, s + i)
            store3(x3b, x)
            g1, g2 = do_g(off_a + i + 1, vt3b)
            x = do_c(off_c + i + 1, s + i + 1)
            wacc[...] += a + do_a(vt3b, x3b)
            store3(x3, x)
            h1, h2 = do_g(off_a + i + 2, vt3)
            s1acc[...] += g1 + h1
            s2acc[...] += g2 + h2
            write_out(sa, s + i - 1, 2)
            return carry

        pairs = (k - 1) // 2
        carry = lax.fori_loop(0, pairs, step2, carry)
        carry = lax.fori_loop(s + 2 * pairs, NU - 1, step1, carry)

        p = (off_a + k + 1) // 2
        tick(p)
        carry = send_own(p + LEAD[0], carry)
        next_z(sa)
        write_out(sa, NU - 2, 1)

        @pl.when(sa == 0)
        def _():
            v_copy(NU - 1).start()

        store3(x3b, do_c(off_c + k - 1, NU - 1))
        g1, g2 = do_g(off_a + k, vt3b)
        w = wacc[...] + do_a(vt3, x3)
        part = merge_1(sa, s1acc[...] + g1, s2acc[...] + g2)
        w = w + do_a(vt3b, x3b)
        part = merge_2(sa, *part)
        first_g(off_a + k + 1)
        merge_3(*part)
        finish(sa, w)
        return carry

    lax.fori_loop(1, NU, outer, carry)

    y_copy = pltpu.make_async_copy(y3, y_hbm, o_sem.at[2 * NU])
    y_copy.start()
    x_copy(NU - 1).start()
    lax.fori_loop(0, NU, lambda u, _: (x_copy(u).wait(), v_copy(u).wait(), 0)[2], 0)
    y_copy.wait()
    sent = vbuf.at[:, pl.ds(0, 64), pl.ds(0, 128)]
    for k in range(3):
        remote(sent, sent, k, rp_sem.at[0], dev1).wait_send()
    sent = vbuf.at[:, :, pl.ds(0, 128)]
    remote(sent, sent, 3, rp_sem.at[0], devp).wait_send()


def last_update(x_hbm, v_hbm, y_hbm, out_hbm, xb, vb, yb, sem):
    def x_in(u):
        return pltpu.make_async_copy(x_hbm.at[:, u], xb.at[u], sem.at[u])

    def v_in(u):
        return pltpu.make_async_copy(v_hbm.at[u], vb.at[u], sem.at[NU + u])

    def x_out(u):
        return pltpu.make_async_copy(xb.at[u], out_hbm.at[:, u], sem.at[2 * NU + u])

    y_in = pltpu.make_async_copy(y_hbm, yb, sem.at[3 * NU])
    y_in.start()
    lax.fori_loop(0, NU, lambda u, _: (v_in(u).start(), x_in(u).start(), 0)[2], 0)
    y_in.wait()

    def body(j, _):
        for i in range(LAST):
            x_in(LAST * j + i).wait()
            v_in(LAST * j + i).wait()
        for i in range(LAST):
            u = LAST * j + i
            upd = mm6(split3(vb[u]), (yb[0], yb[1], yb[2]))
            xb[u] = xb[u] - upd.reshape(4, 64, 512)
        for i in range(LAST):
            x_out(LAST * j + i).start()
        return 0

    lax.fori_loop(0, NU // LAST, body, 0)
    lax.fori_loop(0, NU, lambda u, _: (x_out(u).wait(), 0)[1], 0)


def solution(mesh):
    def local_apply(v_loc, t_loc, z_loc):
        dma = pltpu.SemaphoreType.DMA
        x, v0, y = pl.pallas_call(
            kernel,
            out_shape=(
                jax.ShapeDtypeStruct((4, NU, 64, 512), F32),
                jax.ShapeDtypeStruct((NU, 256, 256), F32),
                jax.ShapeDtypeStruct((3, 256, 512), BF16),
            ),
            in_specs=[pl.BlockSpec(memory_space=pl.ANY)] * 3,
            out_specs=(pl.BlockSpec(memory_space=pl.ANY),) * 3,
            scratch_shapes=[
                pltpu.VMEM((NCH, 256, 256), F32),
                pltpu.VMEM((NU, 4, 64, 512), F32),
                pltpu.VMEM((2, NU, 2, 64, 64), F32),
                pltpu.VMEM((3, 256, 256), BF16),
                pltpu.VMEM((3, 256, 256), BF16),
                pltpu.VMEM((3, 256, 256), BF16),
                pltpu.VMEM((3, 256, 512), BF16),
                pltpu.VMEM((3, 256, 512), BF16),
                pltpu.VMEM((3, 256, 512), BF16),
                pltpu.VMEM((256, 512), F32),
                pltpu.VMEM((192, 256), F32),
                pltpu.VMEM((256, 256), F32),
                pltpu.VMEM((256, 256), F32),
                dma((NP,)), dma((NP,)), dma((NP,)),
                dma((4,)), dma((NU,)), dma((3,)), dma((2 * NU + 1,)),
            ],
            compiler_params=pltpu.CompilerParams(
                collective_id=0, has_side_effects=True, vmem_limit_bytes=67_043_328,
            ),
            cost_estimate=pl.CostEstimate(flops=116_000_000_000, bytes_accessed=60_000_000, transcendentals=0),
        )(v_loc.reshape(NU, 64, 2048), t_loc.reshape(NU, 2, 64, 64), z_loc.reshape(4, NU, 64, 512))
        out = pl.pallas_call(
            last_update,
            out_shape=jax.ShapeDtypeStruct((4, NU, 64, 512), F32),
            in_specs=[pl.BlockSpec(memory_space=pl.ANY)] * 3,
            out_specs=pl.BlockSpec(memory_space=pl.ANY),
            scratch_shapes=[
                pltpu.VMEM((NU, 4, 64, 512), F32),
                pltpu.VMEM((NU, 256, 256), F32),
                pltpu.VMEM((3, 256, 512), BF16),
                dma((3 * NU + 1,)),
            ],
            compiler_params=pltpu.CompilerParams(vmem_limit_bytes=67_043_328),
            cost_estimate=pl.CostEstimate(flops=6_500_000_000, bytes_accessed=22_000_000, transcendentals=0),
        )(x, v0, y)
        return out.reshape(4096, 512)

    return jax.shard_map(
        local_apply,
        mesh=mesh,
        in_specs=(P("row", "col"), P("col", None, None), P(None, ("row", "col"))),
        out_specs=P(None, ("row", "col")),
        check_vma=False,
    )
```
